128 devices in a mesh: dp: 1, vp: 16 (over z, y), tp: 8 (over x, core).
Axes of the slice: x: 4, y: 4, z: 4, core: 2. Of those that a mesh axis runs over, the one named last changes fastest.
Arguments:
- hidden: bfloat16 [512, 2048], P('dp', 'tp')
- lnf_gain: float32 [2048], P('tp')
- lnf_bias: float32 [2048], P('tp')
- emb_table: bfloat16 [250880, 2048], P('vp', 'tp')
- next_tok: int32 [512], P('dp')
- eln_gain: float32 [2048], P('tp')
- eln_bias: float32 [2048], P('tp')
Outputs:
- output 1: float32 [512, 250880], P('dp', ('vp', 'tp'))
- output 2: float32 [512], P('dp')
- output 3: bfloat16 [512, 2048], P('dp', 'tp')
All inputs are finite; a program needn't handle non-finite values.
Results may differ from the reference program's by a relative error of at most 0.001.
Values sent between devices are 32-bit elements.
A program may use at most 1 GiB of HBM per device.

```python
import jax
import jax.numpy as jnp

BATCH_ROWS = 512
D = 2048
VOCAB_SIZE = 250880
VP_BLOCKS = 16
HOT_COUNT = min(2, VP_BLOCKS)
NORM_EPS = 1e-5


def draw_tokens(key):
    key_hot, key_pick, key_any, key_sel, key_pos = jax.random.split(key, 5)
    block_len = VOCAB_SIZE // VP_BLOCKS
    hot_blocks = jax.random.permutation(key_hot, VP_BLOCKS)[:HOT_COUNT]
    hot_pick = jax.random.randint(key_pick, (BATCH_ROWS,), 0, HOT_COUNT)
    any_block = jax.random.randint(key_any, (BATCH_ROWS,), 0, VP_BLOCKS)
    use_hot = jax.random.randint(key_sel, (BATCH_ROWS,), 0, 4) < 3
    tok_block = jnp.where(use_hot, hot_blocks[hot_pick], any_block)
    tok_within = jax.random.randint(key_pos, (BATCH_ROWS,), 0, block_len)
    return (tok_block * block_len + tok_within).astype(jnp.int32)


def setup_inputs(seed: int = 0, part: int = 0) -> dict:
    shared_key, part_root = jax.random.split(jax.random.key(seed))
    part_key = jax.random.fold_in(part_root, part)
    key_hid, key_off, key_tok = jax.random.split(part_key, 3)
    key_tab, key_rowm, key_g1, key_b1, key_g2, key_b2 = jax.random.split(shared_key, 6)
    col_pos = jnp.arange(D, dtype=jnp.float32) / D
    hidden = jax.random.normal(key_hid, (BATCH_ROWS, D), jnp.float32) * (0.5 + 1.5 * col_pos)
    hidden = hidden + jax.random.normal(key_off, (BATCH_ROWS, 1), jnp.float32) * (1.0 + 2.0 * col_pos)
    tab_vals = jax.random.normal(key_tab, (VOCAB_SIZE, D), jnp.float32) * (0.5 + col_pos)
    tab_vals = (tab_vals + jax.random.normal(key_rowm, (VOCAB_SIZE, 1), jnp.float32)) * (D ** -0.5)
    return {
        "hidden": hidden.astype(jnp.bfloat16),
        "lnf_gain": 1.5 + 0.5 * jax.random.normal(key_g1, (D,), jnp.float32),
        "lnf_bias": 0.5 * jax.random.normal(key_b1, (D,), jnp.float32),
        "emb_table": tab_vals.astype(jnp.bfloat16),
        "next_tok": draw_tokens(key_tok),
        "eln_gain": 1.0 + 0.3 * jax.random.normal(key_g2, (D,), jnp.float32),
        "eln_bias": 0.5 * jax.random.normal(key_b2, (D,), jnp.float32),
    }


def layer_norm(rows_in, norm_gain, norm_bias):
    rows_f32 = rows_in.astype(jnp.float32)
    row_mean = jnp.mean(rows_f32, axis=-1, keepdims=True)
    row_var = jnp.mean(rows_f32 * rows_f32, axis=-1, keepdims=True) - row_mean * row_mean
    return (rows_f32 - row_mean) / jnp.sqrt(row_var + NORM_EPS) * norm_gain + norm_bias


def reference(hidden, lnf_gain, lnf_bias, emb_table, next_tok, eln_gain, eln_bias):
    normed = layer_norm(hidden, lnf_gain, lnf_bias).astype(jnp.bfloat16)
    logits = jnp.dot(normed, emb_table.T, preferred_element_type=jnp.float32)
    log_sum = jax.nn.logsumexp(logits, axis=-1)
    logprobs = logits - log_sum[:, None]
    tok_rows = jnp.take(emb_table, next_tok, axis=0)
    next_in = layer_norm(tok_rows, eln_gain, eln_bias).astype(jnp.bfloat16)
    return (logprobs, log_sum, next_in)
```

```python
import functools

import jax
import jax.numpy as jnp
from jax import lax
from jax.experimental import pallas as pl
from jax.experimental.pallas import tpu as pltpu
from jax.sharding import PartitionSpec as P

NORM_EPS = 1e-5
MESH = pl.DeviceIdType.MESH
CHUNK = 128
F32 = jnp.float32
BF16 = jnp.bfloat16

OPP, LEFT, RIGHT, OWN = 0, 1, 2, 3
STEP_OF_SLOT = (2, 3, 1, 0)


def head_kernel(n_vp, n_tp, n_block, full_width,
                hid_ref, g_ref, b_ref, emb_ref, tok_ref, eg_ref, eb_ref,
                logits_ref, lse_ref, next_ref,
                e_own, e_oth, e_out, e_in, send_f, recv_f, send_n, recv_l, recv_r,
                hx, xn, m_acc, s_acc, pick, st_ln, st_lse, st_all, rs_buf, row_st, ag_buf,
                own_sem, oth_sem, ex_send, ex_recv, hx_send, hx_recv,
                f_send, f_recv, n_send, r_send, l_recv, r_recv,
                t_send, t_recv, v_send, v_recv):
    vp = lax.axis_index("vp")
    tp = lax.axis_index("tp")
    core = lax.rem(tp, 2)
    chip = tp // 2
    n_chip = n_tp // 2
    rows = hid_ref.shape[0]
    width = hid_ref.shape[1]
    slab = rows // n_vp
    left = {"tp": lax.rem(chip + n_chip - 1, n_chip) * 2 + core}
    right = {"tp": lax.rem(chip + 1, n_chip) * 2 + core}
    partner = {"tp": chip * 2 + 1 - core}
    half = (n_block // 2) // CHUNK
    n_round = half + 1
    small = n_block - 2 * half * CHUNK
    small2 = (small // 16) * 8
    small1 = small - small2
    tail0 = 2 * half * CHUNK

    def piece(h, i):
        if isinstance(i, int) and i == 0:
            return (tail0 + small2, small1) if h == 0 else (tail0, small2)
        off = h * half * CHUNK + (i - 1) * CHUNK
        return (off if isinstance(i, int) else pl.multiple_of(off, CHUNK)), CHUNK

    def load(slot, other):
        blk = lax.rem(chip + STEP_OF_SLOT[slot], n_chip) * 2 + (1 - core if other else core)
        src = emb_ref.at[pl.ds(pl.multiple_of(blk * n_block, 8), n_block), :]
        dst = (e_oth if other else e_own).at[slot]
        return pltpu.make_async_copy(src, dst, (oth_sem if other else own_sem).at[slot])

    for slot in range(4):
        load(slot, True).start()
        load(slot, False).start()

    barrier = pltpu.get_barrier_semaphore()
    for j in range(1, n_tp):
        pl.semaphore_signal(barrier, inc=1, device_id={"tp": lax.rem(tp + j, n_tp)}, device_id_type=MESH)
    for j in range(1, n_vp):
        pl.semaphore_signal(barrier, inc=1, device_id={"vp": lax.rem(vp + j, n_vp)}, device_id_type=MESH)

    h_t = hid_ref[...].astype(F32).T
    hx[0, :, 0:rows] = h_t
    hx[0, :, rows:rows + 128] = jnp.broadcast_to(g_ref[...], (128, width)).T
    hx[0, :, rows + 128:rows + 256] = jnp.broadcast_to(b_ref[...], (128, width)).T
    sub8 = lax.broadcasted_iota(jnp.int32, (8, rows), 0)
    st_ln[tp] = jnp.where(sub8 == 0, jnp.sum(h_t, axis=0, keepdims=True), jnp.sum(h_t * h_t, axis=0, keepdims=True))

    pl.semaphore_wait(barrier, n_tp + n_vp - 2)

    def tp_copy(buf, stage, j):
        peer = lax.rem(tp + j, n_tp)
        return pltpu.make_async_remote_copy(
            src_ref=buf.at[tp], dst_ref=buf.at[tp], send_sem=t_send.at[stage, j], recv_sem=t_recv.at[stage, j],
            device_id={"tp": peer}, device_id_type=MESH)

    def tp_start(buf, stage):
        for j in range(1, n_tp):
            tp_copy(buf, stage, j).start()

    def tp_wait(buf, stage):
        for j in range(1, n_tp):
            src = lax.rem(tp + n_tp - j, n_tp)
            pltpu.make_async_remote_copy(
                src_ref=buf.at[src], dst_ref=buf.at[src], send_sem=t_send.at[stage, j], recv_sem=t_recv.at[stage, j],
                device_id={"tp": src}, device_id_type=MESH).wait_recv()

    def tp_drain(buf, stage):
        for j in range(1, n_tp):
            tp_copy(buf, stage, j).wait_send()

    tp_start(st_ln, 0)

    hx_copy = pltpu.make_async_remote_copy(
        src_ref=hx.at[0], dst_ref=hx.at[1], send_sem=hx_send.at[0], recv_sem=hx_recv.at[0],
        device_id=partner, device_id_type=MESH)
    hx_copy.start()

    parts = ((tail0, small), (0, tail0))

    def ex_copy(slot, q):
        off, n = parts[q]
        return pltpu.make_async_remote_copy(
            src_ref=e_out.at[slot, pl.ds(off, n), :], dst_ref=e_in.at[slot, pl.ds(off, n), :],
            send_sem=ex_send.at[slot, q], recv_sem=ex_recv.at[slot, q], device_id=partner, device_id_type=MESH)

    for slot in range(4):
        load(slot, True).wait()
        for q in range(2):
            off, n = parts[q]
            e_out[slot, off:off + n, :] = e_oth[slot, off:off + n, :].astype(F32)
            ex_copy(slot, q).start()

    tp_wait(st_ln, 0)
    total = st_ln[0]
    for j in range(1, n_tp):
        total = total + st_ln[j]
    mean = total[0:1] / full_width
    rstd = lax.rsqrt(total[1:2] / full_width - mean * mean + NORM_EPS)

    def norm(which):
        gain = hx[which, :, rows:rows + 128]
        bias = hx[which, :, rows + 128:rows + 256]
        for c in range(rows // 128):
            cols = slice(c * 128, c * 128 + 128)
            xn[which, :, cols] = ((hx[which, :, cols] - mean[:, cols]) * rstd[:, cols] * gain + bias).astype(BF16)

    norm(0)
    hx_copy.wait_recv()
    norm(1)

    def part_sum(slot, off, n):
        mine = e_own[slot, pl.ds(off, n), :]
        theirs = e_in[slot, pl.ds(off, n), :].astype(BF16)
        return (jnp.dot(mine, xn[0], preferred_element_type=F32)
                + jnp.dot(theirs, xn[1], preferred_element_type=F32))

    def f_copy(h, i):
        off, n = piece(h, i)
        return pltpu.make_async_remote_copy(
            src_ref=send_f.at[pl.ds(off, n), :], dst_ref=recv_f.at[pl.ds(off, n), :],
            send_sem=f_send.at[h, i], recv_sem=f_recv.at[h, i],
            device_id=left if h == 0 else right, device_id_type=MESH)

    def r_copy(h, i):
        off, n = piece(h, i)
        dst = (recv_r if h == 0 else recv_l).at[pl.ds(off, n), :]
        return pltpu.make_async_remote_copy(
            src_ref=recv_f.at[pl.ds(off, n), :], dst_ref=dst,
            send_sem=r_send.at[h, i], recv_sem=(r_recv if h == 0 else l_recv).at[h, i],
            device_id=left if h == 0 else right, device_id_type=MESH)

    def n_copy(h, i):
        off, n = piece(h, i)
        dst = (recv_l if h == 0 else recv_r).at[pl.ds(off, n), :]
        return pltpu.make_async_remote_copy(
            src_ref=send_n.at[pl.ds(off, n), :], dst_ref=dst,
            send_sem=n_send.at[h, i], recv_sem=(l_recv if h == 0 else r_recv).at[h, i],
            device_id=right if h == 0 else left, device_id_type=MESH)

    def far(i):
        for h in range(2):
            off, n = piece(h, i)
            send_f[pl.ds(off, n), :] = part_sum(OPP, off, n)
            f_copy(h, i).start()

    def near(i):
        for h in range(2):
            off, n = piece(h, i)
            send_n[pl.ds(off, n), :] = part_sum(RIGHT if h == 0 else LEFT, off, n)
            n_copy(h, i).start()

    def relay(i):
        for h in range(2):
            off, n = piece(h, i)
            mine = part_sum(LEFT if h == 0 else RIGHT, off, n)
            f_copy(h, i).wait_recv()
            recv_f[pl.ds(off, n), :] = recv_f[pl.ds(off, n), :] + mine
            r_copy(h, i).start()

    def account(z, first):
        zr = z.reshape(z.shape[0] // 8, 8, rows)
        top = jnp.max(zr, axis=0)
        if first:
            m_acc[...] = top
            s_acc[...] = jnp.sum(jnp.exp(zr - top[None]), axis=0)
        else:
            old = m_acc[...]
            new = jnp.maximum(old, top)
            m_acc[...] = new
            s_acc[...] = s_acc[...] * jnp.exp(old - new) + jnp.sum(jnp.exp(zr - new[None]), axis=0)

    def arrive(h, i):
        (r_copy if h == 0 else n_copy)(h, i).wait_recv()
        (n_copy if h == 0 else r_copy)(h, i).wait_recv()

    def settle(i):
        if isinstance(i, int) and i == 0:
            arrive(0, 0)
            arrive(1, 0)
            for off in range(tail0, n_block, CHUNK):
                n = min(CHUNK, n_block - off)
                z = part_sum(OWN, off, n) + recv_l[off:off + n, :] + recv_r[off:off + n, :]
                account(z, off == tail0)
                logits_ref[off:off + n, :] = z
            return
        for h in range(2):
            off, n = piece(h, i)
            mine = part_sum(OWN, off, n)
            arrive(h, i)
            z = mine + recv_l[pl.ds(off, n), :] + recv_r[pl.ds(off, n), :]
            account(z, False)
            logits_ref[pl.ds(off, n), :] = z

    tok = jnp.broadcast_to(tok_ref[...], (128, rows)).T

    def gather(step):
        for other in range(2):
            blk_chip = lax.rem(chip + jnp.where(step == 0, STEP_OF_SLOT[0], jnp.where(
                step == 1, STEP_OF_SLOT[1], jnp.where(step == 2, STEP_OF_SLOT[2], STEP_OF_SLOT[3]))), n_chip)
            blk = blk_chip * 2 + (1 - core if other else core)
            base = vp * (n_tp * n_block) + blk * n_block
            ref = e_oth if other else e_own
            acc = pick[...]
            for off in range(0, n_block, 512):
                n = min(512, n_block - off)
                for o, k in ((off, n // 128 * 128), (off + n // 128 * 128, n % 128)):
                    if k == 0:
                        continue
                    lane = lax.broadcasted_iota(jnp.int32, (rows, k), 1) + (base + o)
                    if k % 128 == 0:
                        want = jnp.concatenate([tok] * (k // 128), axis=1) if k > 128 else tok
                    else:
                        want = tok[:, :k]
                    hot = jnp.where(want == lane, 1.0, 0.0).astype(BF16)
                    acc = acc + jnp.dot(hot, ref[step, o:o + k, :], preferred_element_type=F32)
            pick[...] = acc

    def v_copy(src_buf, src_idx, dst_buf, stage, j, peer):
        return pltpu.make_async_remote_copy(
            src_ref=src_buf.at[src_idx] if src_idx is not None else src_buf, dst_ref=dst_buf,
            send_sem=v_send.at[stage, j], recv_sem=v_recv.at[stage, j],
            device_id={"vp": peer}, device_id_type=MESH)

    def rs_copy(j):
        peer = lax.rem(vp + j, n_vp)
        return v_copy(pick.at[pl.ds(pl.multiple_of(peer * slab, 8), slab), :], None, rs_buf.at[vp], 0, j, peer)

    def rs_in(j):
        src = lax.rem(vp + n_vp - j, n_vp)
        return v_copy(rs_buf, src, rs_buf.at[src], 0, j, src)

    def vp_copy(buf, stage, j):
        peer = lax.rem(vp + j, n_vp)
        return v_copy(buf, vp, buf.at[vp], stage, j, peer)

    def vp_in(buf, stage, j):
        src = lax.rem(vp + n_vp - j, n_vp)
        return v_copy(buf, src, buf.at[src], stage, j, src)

    def rows_scatter():
        for j in range(1, n_vp):
            rs_copy(j).start()
        rs_buf[vp] = pick[pl.ds(pl.multiple_of(vp * slab, 8), slab), :]

    def rows_stats():
        for j in range(1, n_vp):
            rs_in(j).wait_recv()
        tot = rs_buf[0]
        for j in range(1, n_vp):
            tot = tot + rs_buf[j]
        ag_buf[vp] = tot
        lane = lax.broadcasted_iota(jnp.int32, (slab, 128), 1)
        row_st[tp] = jnp.where(lane == 0, jnp.sum(tot, axis=1, keepdims=True), jnp.sum(tot * tot, axis=1, keepdims=True))
        tp_start(row_st, 1)

    def rows_norm():
        tp_wait(row_st, 1)
        tot = row_st[0]
        for j in range(1, n_tp):
            tot = tot + row_st[j]
        mu = tot[:, 0:1] / full_width
        rs = lax.rsqrt(tot[:, 1:2] / full_width - mu * mu + NORM_EPS)
        out = ((ag_buf[vp] - mu) * rs * eg_ref[...] + eb_ref[...]).astype(BF16)
        ag_buf[vp] = out.astype(F32)
        for j in range(1, n_vp):
            vp_copy(ag_buf, 1, j).start()

    def rows_out():
        for j in range(1, n_vp):
            vp_in(ag_buf, 1, j).wait_recv()
        for j in range(n_vp):
            next_ref[j * slab:(j + 1) * slab, :] = ag_buf[j]

    pick[...] = jnp.zeros_like(pick)

    load(OPP, False).wait()
    for q in range(2):
        ex_copy(OPP, q).wait_recv()
        far(q)
    for slot in (LEFT, RIGHT):
        load(slot, False).wait()
        for q in range(2):
            ex_copy(slot, q).wait_recv()
    near(0)
    far(2)
    relay(0)
    load(OWN, False).wait()
    for q in range(2):
        ex_copy(OWN, q).wait_recv()

    def round_body(i, carry):
        near(i)

        @pl.when(i + 2 < n_round)
        def _():
            far(i + 2)

        relay(i)

        @pl.when(i <= 4)
        def _():
            gather(i - 1)

        @pl.when(i == 5)
        def _():
            rows_scatter()

        @pl.when(i == 6)
        def _():
            rows_stats()

        @pl.when(i == 7)
        def _():
            rows_norm()

        @pl.when(i == 2)
        def _():
            settle(0)

        @pl.when(i >= 3)
        def _():
            settle(i - 2)

        return carry

    lax.fori_loop(1, n_round, round_body, 0)

    rows_out()

    def last_body(i, carry):
        settle(i)
        return carry

    lax.fori_loop(n_round - 2, n_round, last_body, 0)

    def merge(buf, n):
        top = buf[0, 0:1]
        for j in range(1, n):
            top = jnp.maximum(top, buf[j, 0:1])
        tot = buf[0, 1:2] * jnp.exp(buf[0, 0:1] - top)
        for j in range(1, n):
            tot = tot + buf[j, 1:2] * jnp.exp(buf[j, 0:1] - top)
        return top, tot

    m8 = m_acc[...]
    top = jnp.max(m8, axis=0, keepdims=True)
    tot = jnp.sum(s_acc[...] * jnp.exp(m8 - top), axis=0, keepdims=True)
    st_lse[tp] = jnp.where(sub8 == 0, top, tot)
    tp_start(st_lse, 2)
    tp_wait(st_lse, 2)
    top, tot = merge(st_lse, n_tp)
    st_all[vp] = jnp.where(sub8 == 0, top, tot)
    for j in range(1, n_vp):
        vp_copy(st_all, 2, j).start()
    hx_copy.wait_send()
    for slot in range(4):
        for q in range(2):
            ex_copy(slot, q).wait_send()
    for h in range(2):
        f_copy(h, 0).wait_send()
        n_copy(h, 0).wait_send()
        r_copy(h, 0).wait_send()

    def drain(i, carry):
        for h in range(2):
            f_copy(h, i).wait_send()
            n_copy(h, i).wait_send()
            r_copy(h, i).wait_send()
        return carry

    lax.fori_loop(1, n_round, drain, 0)
    tp_drain(st_ln, 0)
    tp_drain(row_st, 1)
    tp_drain(st_lse, 2)
    for j in range(1, n_vp):
        rs_copy(j).wait_send()
        vp_copy(ag_buf, 1, j).wait_send()
    for j in range(1, n_vp):
        vp_in(st_all, 2, j).wait_recv()
    top, tot = merge(st_all, n_vp)
    lse_ref[...] = top + jnp.log(tot)
    for j in range(1, n_vp):
        vp_copy(st_all, 2, j).wait_send()


def solution(mesh):
    n_vp, n_tp = mesh.shape["vp"], mesh.shape["tp"]

    def per_device(hidden, lnf_gain, lnf_bias, emb_table, next_tok, eln_gain, eln_bias):
        rows, width = hidden.shape
        n_block = emb_table.shape[0] // n_tp
        slab = rows // n_vp
        n_round = n_block // 2 // CHUNK + 1
        dma = pltpu.SemaphoreType.DMA
        vmem = pl.BlockSpec(memory_space=pltpu.VMEM)
        logits, lse, next_in = pl.pallas_call(
            functools.partial(head_kernel, n_vp, n_tp, n_block, width * n_tp),
            out_shape=(
                jax.ShapeDtypeStruct((n_block, rows), F32),
                jax.ShapeDtypeStruct((1, rows), F32),
                jax.ShapeDtypeStruct((rows, width), F32),
            ),
            in_specs=[vmem, vmem, vmem, pl.BlockSpec(memory_space=pl.ANY), vmem, vmem, vmem],
            out_specs=(vmem, vmem, vmem),
            scratch_shapes=[
                pltpu.VMEM((4, n_block, width), BF16),
                pltpu.VMEM((4, n_block, width), BF16),
                pltpu.VMEM((4, n_block, width), F32),
                pltpu.VMEM((4, n_block, width), F32),
                pltpu.VMEM((n_block, rows), F32),
                pltpu.VMEM((n_block, rows), F32),
                pltpu.VMEM((n_block, rows), F32),
                pltpu.VMEM((n_block, rows), F32),
                pltpu.VMEM((n_block, rows), F32),
                pltpu.VMEM((2, width, rows + 256), F32),
                pltpu.VMEM((2, width, rows), BF16),
                pltpu.VMEM((8, rows), F32),
                pltpu.VMEM((8, rows), F32),
                pltpu.VMEM((rows, width), F32),
                pltpu.VMEM((n_tp, 8, rows), F32),
                pltpu.VMEM((n_tp, 8, rows), F32),
                pltpu.VMEM((n_vp, 8, rows), F32),
                pltpu.VMEM((n_vp, slab, width), F32),
                pltpu.VMEM((n_tp, slab, 128), F32),
                pltpu.VMEM((n_vp, slab, width), F32),
                dma((4,)), dma((4,)), dma((4, 2)), dma((4, 2)), dma((1,)), dma((1,)),
                dma((2, n_round)), dma((2, n_round)), dma((2, n_round)), dma((2, n_round)), dma((2, n_round)), dma((2, n_round)),
                dma((3, n_tp)), dma((3, n_tp)), dma((3, n_vp)), dma((3, n_vp)),
            ],
            compiler_params=pltpu.CompilerParams(
                collective_id=0, has_side_effects=True, vmem_limit_bytes=62 * 1024 * 1024),
            cost_estimate=pl.CostEstimate(
                flops=4 * rows * n_block * n_tp * width, bytes_accessed=16 * n_block * n_tp * width, transcendentals=rows * n_block),
        )(hidden, lnf_gain[None, :], lnf_bias[None, :], emb_table, next_tok[None, :], eln_gain[None, :], eln_bias[None, :])
        return (logits - lse).T, lse[0], next_in.astype(BF16)

    return jax.shard_map(
        per_device,
        mesh=mesh,
        in_specs=(P("dp", "tp"), P("tp"), P("tp"), P("vp", "tp"), P("dp"), P("tp"), P("tp")),
        out_specs=(P("dp", ("vp", "tp")), P("dp"), P("dp", "tp")),
        check_vma=False,
    )
```

```python
import functools

import jax
import jax.numpy as jnp
from jax import lax
from jax.experimental import pallas as pl
from jax.experimental.pallas import tpu as pltpu
from jax.sharding import PartitionSpec as P

NORM_EPS = 1e-5
MESH = pl.DeviceIdType.MESH
CHUNK = 128
F32 = jnp.float32
BF16 = jnp.bfloat16

OPP, LEFT, RIGHT, OWN = 0, 1, 2, 3
STEP_OF_SLOT = (2, 3, 1, 0)


def head_kernel(n_vp, n_tp, n_block, full_width,
                hid_ref, g_ref, b_ref, emb_ref, tok_ref, eg_ref, eb_ref,
                logits_ref, lse_ref, next_ref,
                e_own, e_oth, e_out, e_in, send_f, recv_f, send_n, recv_l, recv_r,
                hx, xn, m_acc, s_acc, pick, st_ln, st_lse, st_all, rs_buf, row_st, ag_buf,
                own_sem, oth_sem, ex_send, ex_recv, hx_send, hx_recv,
                f_send, f_recv, n_send, r_send, l_recv, r_recv,
                t_send, t_recv, v_send, v_recv):
    vp = lax.axis_index("vp")
    tp = lax.axis_index("tp")
    core = lax.rem(tp, 2)
    chip = tp // 2
    n_chip = n_tp // 2
    rows = hid_ref.shape[0]
    width = hid_ref.shape[1]
    slab = rows // n_vp
    left = {"tp": lax.rem(chip + n_chip - 1, n_chip) * 2 + core}
    right = {"tp": lax.rem(chip + 1, n_chip) * 2 + core}
    partner = {"tp": chip * 2 + 1 - core}
    half = (n_block // 2) // CHUNK
    n_round = half + 1
    small = n_block - 2 * half * CHUNK
    small2 = (small // 16) * 8
    small1 = small - small2
    tail0 = 2 * half * CHUNK

    def piece(h, i):
        if isinstance(i, int) and i == 0:
            return (tail0 + small2, small1) if h == 0 else (tail0, small2)
        off = h * half * CHUNK + (i - 1) * CHUNK
        return (off if isinstance(i, int) else pl.multiple_of(off, CHUNK)), CHUNK

    def load(slot, other):
        blk = lax.rem(chip + STEP_OF_SLOT[slot], n_chip) * 2 + (1 - core if other else core)
        src = emb_ref.at[pl.ds(pl.multiple_of(blk * n_block, 8), n_block), :]
        dst = (e_oth if other else e_own).at[slot]
        return pltpu.make_async_copy(src, dst, (oth_sem if other else own_sem).at[slot])

    for slot in range(4):
        load(slot, True).start()
        load(slot, False).start()

    barrier = pltpu.get_barrier_semaphore()
    for j in range(1, n_tp):
        pl.semaphore_signal(barrier, inc=1, device_id={"tp": lax.rem(tp + j, n_tp)}, device_id_type=MESH)
    for j in range(1, n_vp):
        pl.semaphore_signal(barrier, inc=1, device_id={"vp": lax.rem(vp + j, n_vp)}, device_id_type=MESH)

    h_t = hid_ref[...].astype(F32).T
    hx[0, :, 0:rows] = h_t
    hx[0, :, rows:rows + 128] = jnp.broadcast_to(g_ref[...], (128, width)).T
    hx[0, :, rows + 128:rows + 256] = jnp.broadcast_to(b_ref[...], (128, width)).T
    st_ln[tp, :, 0:rows] = jnp.sum(h_t, axis=0, keepdims=True)
    st_ln[tp, :, rows:2 * rows] = jnp.sum(h_t * h_t, axis=0, keepdims=True)

    pl.semaphore_wait(barrier, n_tp + n_vp - 2)

    def tp_copy(buf, stage, j):
        peer = lax.rem(tp + j, n_tp)
        return pltpu.make_async_remote_copy(
            src_ref=buf.at[tp], dst_ref=buf.at[tp], send_sem=t_send.at[stage, j], recv_sem=t_recv.at[stage, j],
            device_id={"tp": peer}, device_id_type=MESH)

    def tp_start(buf, stage):
        for j in range(1, n_tp):
            tp_copy(buf, stage, j).start()

    def tp_wait(buf, stage):
        for j in range(1, n_tp):
            src = lax.rem(tp + n_tp - j, n_tp)
            pltpu.make_async_remote_copy(
                src_ref=buf.at[src], dst_ref=buf.at[src], send_sem=t_send.at[stage, j], recv_sem=t_recv.at[stage, j],
                device_id={"tp": src}, device_id_type=MESH).wait_recv()

    def tp_drain(buf, stage):
        for j in range(1, n_tp):
            tp_copy(buf, stage, j).wait_send()

    tp_start(st_ln, 0)

    hx_copy = pltpu.make_async_remote_copy(
        src_ref=hx.at[0], dst_ref=hx.at[1], send_sem=hx_send.at[0], recv_sem=hx_recv.at[0],
        device_id=partner, device_id_type=MESH)
    hx_copy.start()

    parts = ((tail0, small), (0, tail0))

    def ex_copy(slot, q):
        off, n = parts[q]
        return pltpu.make_async_remote_copy(
            src_ref=e_out.at[slot, pl.ds(off, n), :], dst_ref=e_in.at[slot, pl.ds(off, n), :],
            send_sem=ex_send.at[slot, q], recv_sem=ex_recv.at[slot, q], device_id=partner, device_id_type=MESH)

    for slot in range(4):
        load(slot, True).wait()
        for q in range(2):
            off, n = parts[q]
            e_out[slot, off:off + n, :] = e_oth[slot, off:off + n, :].astype(F32)
            ex_copy(slot, q).start()

    tp_wait(st_ln, 0)
    total = st_ln[0]
    for j in range(1, n_tp):
        total = total + st_ln[j]
    mean = total[:, 0:rows] / full_width
    rstd = lax.rsqrt(total[:, rows:2 * rows] / full_width - mean * mean + NORM_EPS)

    def norm(which):
        gain = hx[which, :, rows:rows + 128]
        bias = hx[which, :, rows + 128:rows + 256]
        for c in range(rows // 128):
            cols = slice(c * 128, c * 128 + 128)
            xn[which, :, cols] = ((hx[which, :, cols] - mean[:, cols]) * rstd[:, cols] * gain + bias).astype(BF16)

    norm(0)
    hx_copy.wait_recv()
    norm(1)

    def part_sum(slot, off, n):
        mine = e_own[slot, pl.ds(off, n), :]
        theirs = e_in[slot, pl.ds(off, n), :].astype(BF16)
        return (jnp.dot(mine, xn[0], preferred_element_type=F32)
                + jnp.dot(theirs, xn[1], preferred_element_type=F32))

    def f_copy(h, i):
        off, n = piece(h, i)
        return pltpu.make_async_remote_copy(
            src_ref=send_f.at[pl.ds(off, n), :], dst_ref=recv_f.at[pl.ds(off, n), :],
            send_sem=f_send.at[h, i], recv_sem=f_recv.at[h, i],
            device_id=left if h == 0 else right, device_id_type=MESH)

    def r_copy(h, i):
        off, n = piece(h, i)
        dst = (recv_r if h == 0 else recv_l).at[pl.ds(off, n), :]
        return pltpu.make_async_remote_copy(
            src_ref=recv_f.at[pl.ds(off, n), :], dst_ref=dst,
            send_sem=r_send.at[h, i], recv_sem=(r_recv if h == 0 else l_recv).at[h, i],
            device_id=left if h == 0 else right, device_id_type=MESH)

    def n_copy(h, i):
        off, n = piece(h, i)
        dst = (recv_l if h == 0 else recv_r).at[pl.ds(off, n), :]
        return pltpu.make_async_remote_copy(
            src_ref=send_n.at[pl.ds(off, n), :], dst_ref=dst,
            send_sem=n_send.at[h, i], recv_sem=(l_recv if h == 0 else r_recv).at[h, i],
            device_id=right if h == 0 else left, device_id_type=MESH)

    def far(i):
        for h in range(2):
            off, n = piece(h, i)
            send_f[pl.ds(off, n), :] = part_sum(OPP, off, n)
            f_copy(h, i).start()

    def near(i):
        for h in range(2):
            off, n = piece(h, i)
            send_n[pl.ds(off, n), :] = part_sum(RIGHT if h == 0 else LEFT, off, n)
            n_copy(h, i).start()

    def relay(i):
        for h in range(2):
            off, n = piece(h, i)
            mine = part_sum(LEFT if h == 0 else RIGHT, off, n)
            f_copy(h, i).wait_recv()
            recv_f[pl.ds(off, n), :] = recv_f[pl.ds(off, n), :] + mine
            r_copy(h, i).start()

    def account(z, first):
        zr = z.reshape(z.shape[0] // 8, 8, rows)
        top = jnp.max(zr, axis=0)
        if first:
            m_acc[...] = top
            s_acc[...] = jnp.sum(jnp.exp(zr - top[None]), axis=0)
        else:
            old = m_acc[...]
            new = jnp.maximum(old, top)
            m_acc[...] = new
            s_acc[...] = s_acc[...] * jnp.exp(old - new) + jnp.sum(jnp.exp(zr - new[None]), axis=0)

    def arrive(h, i):
        (r_copy if h == 0 else n_copy)(h, i).wait_recv()
        (n_copy if h == 0 else r_copy)(h, i).wait_recv()

    def settle(i):
        if isinstance(i, int) and i == 0:
            arrive(0, 0)
            arrive(1, 0)
            for off in range(tail0, n_block, CHUNK):
                n = min(CHUNK, n_block - off)
                z = part_sum(OWN, off, n) + recv_l[off:off + n, :] + recv_r[off:off + n, :]
                account(z, off == tail0)
                logits_ref[off:off + n, :] = z
            return
        for h in range(2):
            off, n = piece(h, i)
            mine = part_sum(OWN, off, n)
            arrive(h, i)
            z = mine + recv_l[pl.ds(off, n), :] + recv_r[pl.ds(off, n), :]
            account(z, False)
            logits_ref[pl.ds(off, n), :] = z

    tok = jnp.broadcast_to(tok_ref[...], (128, rows)).T

    def gather(step):
        for other in range(2):
            blk_chip = lax.rem(chip + jnp.where(step == 0, STEP_OF_SLOT[0], jnp.where(
                step == 1, STEP_OF_SLOT[1], jnp.where(step == 2, STEP_OF_SLOT[2], STEP_OF_SLOT[3]))), n_chip)
            blk = blk_chip * 2 + (1 - core if other else core)
            base = vp * (n_tp * n_block) + blk * n_block
            ref = e_oth if other else e_own
            acc = pick[...]
            for off in range(0, n_block, 512):
                n = min(512, n_block - off)
                for o, k in ((off, n // 128 * 128), (off + n // 128 * 128, n % 128)):
                    if k == 0:
                        continue
                    lane = lax.broadcasted_iota(jnp.int32, (rows, k), 1) + (base + o)
                    if k % 128 == 0:
                        want = jnp.concatenate([tok] * (k // 128), axis=1) if k > 128 else tok
                    else:
                        want = tok[:, :k]
                    hot = jnp.where(want == lane, 1.0, 0.0).astype(BF16)
                    acc = acc + jnp.dot(hot, ref[step, o:o + k, :], preferred_element_type=F32)
            pick[...] = acc

    def v_copy(src_buf, src_idx, dst_buf, stage, j, peer):
        return pltpu.make_async_remote_copy(
            src_ref=src_buf.at[src_idx] if src_idx is not None else src_buf, dst_ref=dst_buf,
            send_sem=v_send.at[stage, j], recv_sem=v_recv.at[stage, j],
            device_id={"vp": peer}, device_id_type=MESH)

    def rs_copy(j):
        peer = lax.rem(vp + j, n_vp)
        return v_copy(pick.at[pl.ds(pl.multiple_of(peer * slab, 8), slab), :], None, rs_buf.at[vp], 0, j, peer)

    def rs_in(j):
        src = lax.rem(vp + n_vp - j, n_vp)
        return v_copy(rs_buf, src, rs_buf.at[src], 0, j, src)

    def vp_copy(buf, stage, j):
        peer = lax.rem(vp + j, n_vp)
        return v_copy(buf, vp, buf.at[vp], stage, j, peer)

    def vp_in(buf, stage, j):
        src = lax.rem(vp + n_vp - j, n_vp)
        return v_copy(buf, src, buf.at[src], stage, j, src)

    def rows_scatter():
        for j in range(1, n_vp):
            rs_copy(j).start()
        rs_buf[vp] = pick[pl.ds(pl.multiple_of(vp * slab, 8), slab), :]

    def rows_stats():
        for j in range(1, n_vp):
            rs_in(j).wait_recv()
        tot = rs_buf[0]
        for j in range(1, n_vp):
            tot = tot + rs_buf[j]
        ag_buf[vp] = tot
        lane = lax.broadcasted_iota(jnp.int32, (slab, 128), 1)
        row_st[tp] = jnp.where(lane == 0, jnp.sum(tot, axis=1, keepdims=True), jnp.sum(tot * tot, axis=1, keepdims=True))
        tp_start(row_st, 1)

    def rows_norm():
        tp_wait(row_st, 1)
        tot = row_st[0]
        for j in range(1, n_tp):
            tot = tot + row_st[j]
        mu = tot[:, 0:1] / full_width
        rs = lax.rsqrt(tot[:, 1:2] / full_width - mu * mu + NORM_EPS)
        out = ((ag_buf[vp] - mu) * rs * eg_ref[...] + eb_ref[...]).astype(BF16)
        ag_buf[vp] = out.astype(F32)
        for j in range(1, n_vp):
            vp_copy(ag_buf, 1, j).start()

    def rows_out():
        for j in range(1, n_vp):
            vp_in(ag_buf, 1, j).wait_recv()
        for j in range(n_vp):
            next_ref[j * slab:(j + 1) * slab, :] = ag_buf[j]

    pick[...] = jnp.zeros_like(pick)

    load(OPP, False).wait()
    for q in range(2):
        ex_copy(OPP, q).wait_recv()
        far(q)
    for slot in (LEFT, RIGHT):
        load(slot, False).wait()
        for q in range(2):
            ex_copy(slot, q).wait_recv()
    near(0)
    far(2)
    relay(0)
    load(OWN, False).wait()
    for q in range(2):
        ex_copy(OWN, q).wait_recv()

    def round_body(i, carry):
        near(i)

        @pl.when(i + 2 < n_round)
        def _():
            far(i + 2)

        relay(i)

        @pl.when(i <= 2)
        def _():
            gather(2 * i - 2)
            gather(2 * i - 1)

        @pl.when(i == 3)
        def _():
            rows_scatter()

        @pl.when(i == 4)
        def _():
            rows_stats()

        @pl.when(i == 6)
        def _():
            rows_norm()

        @pl.when(i == 2)
        def _():
            settle(0)

        @pl.when(i >= 3)
        def _():
            settle(i - 2)

        return carry

    lax.fori_loop(1, n_round, round_body, 0)

    def last_body(i, carry):
        settle(i)
        return carry

    lax.fori_loop(n_round - 2, n_round, last_body, 0)

    def merge(buf, n):
        top = buf[0]
        for j in range(1, n):
            top = jnp.maximum(top, buf[j])
        tot = jnp.exp(buf[0] - top)
        for j in range(1, n):
            tot = tot + jnp.exp(buf[j] - top)
        return top + jnp.log(tot)

    m8 = m_acc[...]
    top = jnp.max(m8, axis=0, keepdims=True)
    st_lse[tp] = top + jnp.log(jnp.sum(s_acc[...] * jnp.exp(m8 - top), axis=0, keepdims=True))
    tp_start(st_lse, 2)
    tp_wait(st_lse, 2)
    st_all[vp] = merge(st_lse, n_tp)
    for j in range(1, n_vp):
        vp_copy(st_all, 2, j).start()
    rows_out()
    hx_copy.wait_send()
    for slot in range(4):
        for q in range(2):
            ex_copy(slot, q).wait_send()
    for h in range(2):
        f_copy(h, 0).wait_send()
        n_copy(h, 0).wait_send()
        r_copy(h, 0).wait_send()

    def drain(i, carry):
        for h in range(2):
            f_copy(h, i).wait_send()
            n_copy(h, i).wait_send()
            r_copy(h, i).wait_send()
        return carry

    lax.fori_loop(1, n_round, drain, 0)
    tp_drain(st_ln, 0)
    tp_drain(row_st, 1)
    tp_drain(st_lse, 2)
    for j in range(1, n_vp):
        rs_copy(j).wait_send()
        vp_copy(ag_buf, 1, j).wait_send()
    for j in range(1, n_vp):
        vp_in(st_all, 2, j).wait_recv()
    lse_ref[...] = merge(st_all, n_vp)
    for j in range(1, n_vp):
        vp_copy(st_all, 2, j).wait_send()


def finish_kernel(n_piece, z_ref, lse_ref, next_ref, out_ref, sum_ref, row_ref, buf, sems):
    lse = lse_ref[...]
    n = z_ref.shape[0] // n_piece

    def put(j):
        part = pl.ds(j * n, n)
        return pltpu.make_async_copy(buf.at[part, :], out_ref.at[part, :], sems.at[j])

    for j in range(n_piece):
        buf[j * n:(j + 1) * n, :] = z_ref[j * n:(j + 1) * n, :] - lse
        put(j).start()
    sum_ref[...] = lse
    row_ref[...] = next_ref[...].astype(BF16)
    for j in range(n_piece):
        put(j).wait()


def solution(mesh):
    n_vp, n_tp = mesh.shape["vp"], mesh.shape["tp"]

    def per_device(hidden, lnf_gain, lnf_bias, emb_table, next_tok, eln_gain, eln_bias):
        rows, width = hidden.shape
        n_block = emb_table.shape[0] // n_tp
        slab = rows // n_vp
        n_round = n_block // 2 // CHUNK + 1
        dma = pltpu.SemaphoreType.DMA
        vmem = pl.BlockSpec(memory_space=pltpu.VMEM)
        logits, lse, next_in = pl.pallas_call(
            functools.partial(head_kernel, n_vp, n_tp, n_block, width * n_tp),
            out_shape=(
                pltpu.VMEM((n_block, rows), F32),
                pltpu.VMEM((1, rows), F32),
                pltpu.VMEM((rows, width), F32),
            ),
            in_specs=[vmem, vmem, vmem, pl.BlockSpec(memory_space=pl.ANY), vmem, vmem, vmem],
            out_specs=(vmem, vmem, vmem),
            scratch_shapes=[
                pltpu.VMEM((4, n_block, width), BF16),
                pltpu.VMEM((4, n_block, width), BF16),
                pltpu.VMEM((4, n_block, width), F32),
                pltpu.VMEM((4, n_block, width), F32),
                pltpu.VMEM((n_block, rows), F32),
                pltpu.VMEM((n_block, rows), F32),
                pltpu.VMEM((n_block, rows), F32),
                pltpu.VMEM((n_block, rows), F32),
                pltpu.VMEM((n_block, rows), F32),
                pltpu.VMEM((2, width, rows + 256), F32),
                pltpu.VMEM((2, width, rows), BF16),
                pltpu.VMEM((8, rows), F32),
                pltpu.VMEM((8, rows), F32),
                pltpu.VMEM((rows, width), F32),
                pltpu.VMEM((n_tp, 1, 2 * rows), F32),
                pltpu.VMEM((n_tp, 1, rows), F32),
                pltpu.VMEM((n_vp, 1, rows), F32),
                pltpu.VMEM((n_vp, slab, width), F32),
                pltpu.VMEM((n_tp, slab, 128), F32),
                pltpu.VMEM((n_vp, slab, width), F32),
                dma((4,)), dma((4,)), dma((4, 2)), dma((4, 2)), dma((1,)), dma((1,)),
                dma((2, n_round)), dma((2, n_round)), dma((2, n_round)), dma((2, n_round)), dma((2, n_round)), dma((2, n_round)),
                dma((3, n_tp)), dma((3, n_tp)), dma((3, n_vp)), dma((3, n_vp)),
            ],
            compiler_params=pltpu.CompilerParams(
                collective_id=0, has_side_effects=True, vmem_limit_bytes=53 * 1024 * 1024),
            cost_estimate=pl.CostEstimate(
                flops=4 * rows * n_block * n_tp * width, bytes_accessed=16 * n_block * n_tp * width, transcendentals=rows * n_block),
        )(hidden, lnf_gain[None, :], lnf_bias[None, :], emb_table, next_tok[None, :], eln_gain[None, :], eln_bias[None, :])
        n_piece = 5
        logprobs_t, log_sum, next_bf = pl.pallas_call(
            functools.partial(finish_kernel, n_piece),
            out_shape=(
                jax.ShapeDtypeStruct((n_block, rows), F32),
                jax.ShapeDtypeStruct((1, rows), F32),
                jax.ShapeDtypeStruct((rows, width), BF16),
            ),
            in_specs=[vmem, vmem, vmem],
            out_specs=(pl.BlockSpec(memory_space=pl.ANY), vmem, vmem),
            scratch_shapes=[pltpu.VMEM((n_block, rows), F32), dma((n_piece,))],
            compiler_params=pltpu.CompilerParams(vmem_limit_bytes=16 * 1024 * 1024),
        )(logits, lse, next_in)
        return logprobs_t.T, log_sum[0], next_bf

    return jax.shard_map(
        per_device,
        mesh=mesh,
        in_specs=(P("dp", "tp"), P("tp"), P("tp"), P("vp", "tp"), P("dp"), P("tp"), P("tp")),
        out_specs=(P("dp", ("vp", "tp")), P("dp"), P("dp", "tp")),
        check_vma=False,
    )
```

```python
import functools

import jax
import jax.numpy as jnp
from jax import lax
from jax.experimental import pallas as pl
from jax.experimental.pallas import tpu as pltpu
from jax.sharding import PartitionSpec as P

NORM_EPS = 1e-5
MESH = pl.DeviceIdType.MESH
CHUNK = 128
F32 = jnp.float32
BF16 = jnp.bfloat16

OPP, LEFT, RIGHT, OWN = 0, 1, 2, 3
STEP_OF_SLOT = (2, 3, 1, 0)


def head_kernel(n_vp, n_tp, n_block, full_width,
                hid_hbm, g_hbm, b_hbm, emb_ref, tok_hbm, eg_hbm, eb_hbm,
                logits_ref, lse_ref, next_ref,
                e_own, e_oth, e_out, e_in, send_f, recv_f, send_n, recv_l, recv_r,
                hx, xn, m_acc, s_acc, pick, st_ln, st_lse, st_all, rs_buf, row_st, ag_buf,
                own_sem, oth_sem, ex_send, ex_recv, hx_send, hx_recv,
                f_send, f_recv, n_send, r_send, l_recv, r_recv,
                t_send, t_recv, v_send, v_recv,
                hid_ref, g_ref, b_ref, tok_ref, eg_ref, eb_ref, in_sem):
    vp = lax.axis_index("vp")
    tp = lax.axis_index("tp")
    core = lax.rem(tp, 2)
    chip = tp // 2
    n_chip = n_tp // 2
    rows, width = hid_hbm.shape
    slab = rows // n_vp
    left = {"tp": lax.rem(chip + n_chip - 1, n_chip) * 2 + core}
    right = {"tp": lax.rem(chip + 1, n_chip) * 2 + core}
    partner = {"tp": chip * 2 + 1 - core}
    half = (n_block // 2) // CHUNK
    n_round = half + 1
    small = n_block - 2 * half * CHUNK
    small2 = (small // 16) * 8
    small1 = small - small2
    tail0 = 2 * half * CHUNK

    def piece(h, i):
        if isinstance(i, int) and i == 0:
            return (tail0 + small2, small1) if h == 0 else (tail0, small2)
        off = h * half * CHUNK + (i - 1) * CHUNK
        return (off if isinstance(i, int) else pl.multiple_of(off, CHUNK)), CHUNK

    def load(slot, other):
        blk = lax.rem(chip + STEP_OF_SLOT[slot], n_chip) * 2 + (1 - core if other else core)
        src = emb_ref.at[pl.ds(pl.multiple_of(blk * n_block, 8), n_block), :]
        dst = (e_oth if other else e_own).at[slot]
        return pltpu.make_async_copy(src, dst, (oth_sem if other else own_sem).at[slot])

    small_in = [pltpu.make_async_copy(src, dst, in_sem.at[k]) for k, (src, dst) in enumerate((
        (hid_hbm, hid_ref), (g_hbm, g_ref), (b_hbm, b_ref), (tok_hbm, tok_ref), (eg_hbm, eg_ref), (eb_hbm, eb_ref)))]

    barrier = pltpu.get_barrier_semaphore()
    for j in range(1, n_tp):
        pl.semaphore_signal(barrier, inc=1, device_id={"tp": lax.rem(tp + j, n_tp)}, device_id_type=MESH)
    for j in range(1, n_vp):
        pl.semaphore_signal(barrier, inc=1, device_id={"vp": lax.rem(vp + j, n_vp)}, device_id_type=MESH)

    for copy in small_in[:3]:
        copy.start()
    for slot in range(4):
        load(slot, True).start()
        load(slot, False).start()
    for copy in small_in[3:]:
        copy.start()

    for copy in small_in[:3]:
        copy.wait()
    h_t = hid_ref[...].astype(F32).T
    hx[0, :, 0:rows] = h_t
    hx[0, :, rows:rows + 128] = jnp.broadcast_to(g_ref[...], (128, width)).T
    hx[0, :, rows + 128:rows + 256] = jnp.broadcast_to(b_ref[...], (128, width)).T
    st_ln[tp, :, 0:rows] = jnp.sum(h_t, axis=0, keepdims=True)
    st_ln[tp, :, rows:2 * rows] = jnp.sum(h_t * h_t, axis=0, keepdims=True)

    pl.semaphore_wait(barrier, n_tp + n_vp - 2)

    def tp_copy(buf, stage, j):
        peer = lax.rem(tp + j, n_tp)
        return pltpu.make_async_remote_copy(
            src_ref=buf.at[tp], dst_ref=buf.at[tp], send_sem=t_send.at[stage, j], recv_sem=t_recv.at[stage, j],
            device_id={"tp": peer}, device_id_type=MESH)

    def tp_start(buf, stage):
        for j in range(1, n_tp):
            tp_copy(buf, stage, j).start()

    def tp_wait(buf, stage):
        for j in range(1, n_tp):
            src = lax.rem(tp + n_tp - j, n_tp)
            pltpu.make_async_remote_copy(
                src_ref=buf.at[src], dst_ref=buf.at[src], send_sem=t_send.at[stage, j], recv_sem=t_recv.at[stage, j],
                device_id={"tp": src}, device_id_type=MESH).wait_recv()

    def tp_drain(buf, stage):
        for j in range(1, n_tp):
            tp_copy(buf, stage, j).wait_send()

    tp_start(st_ln, 0)

    hx_copy = pltpu.make_async_remote_copy(
        src_ref=hx.at[0], dst_ref=hx.at[1], send_sem=hx_send.at[0], recv_sem=hx_recv.at[0],
        device_id=partner, device_id_type=MESH)
    hx_copy.start()

    parts = ((tail0, small), (0, tail0))

    def ex_copy(slot, q):
        off, n = parts[q]
        return pltpu.make_async_remote_copy(
            src_ref=e_out.at[slot, pl.ds(off, n), :], dst_ref=e_in.at[slot, pl.ds(off, n), :],
            send_sem=ex_send.at[slot, q], recv_sem=ex_recv.at[slot, q], device_id=partner, device_id_type=MESH)

    for slot in range(4):
        load(slot, True).wait()
        for q in range(2):
            off, n = parts[q]
            e_out[slot, off:off + n, :] = e_oth[slot, off:off + n, :].astype(F32)
            ex_copy(slot, q).start()

    tp_wait(st_ln, 0)
    total = st_ln[0]
    for j in range(1, n_tp):
        total = total + st_ln[j]
    mean = total[:, 0:rows] / full_width
    rstd = lax.rsqrt(total[:, rows:2 * rows] / full_width - mean * mean + NORM_EPS)

    def norm(which):
        gain = hx[which, :, rows:rows + 128]
        bias = hx[which, :, rows + 128:rows + 256]
        for c in range(rows // 128):
            cols = slice(c * 128, c * 128 + 128)
            xn[which, :, cols] = ((hx[which, :, cols] - mean[:, cols]) * rstd[:, cols] * gain + bias).astype(BF16)

    norm(0)
    hx_copy.wait_recv()
    norm(1)

    def part_sum(slot, off, n):
        mine = e_own[slot, pl.ds(off, n), :]
        theirs = e_in[slot, pl.ds(off, n), :].astype(BF16)
        return (jnp.dot(mine, xn[0], preferred_element_type=F32)
                + jnp.dot(theirs, xn[1], preferred_element_type=F32))

    def f_copy(h, i):
        off, n = piece(h, i)
        return pltpu.make_async_remote_copy(
            src_ref=send_f.at[pl.ds(off, n), :], dst_ref=recv_f.at[pl.ds(off, n), :],
            send_sem=f_send.at[h, i], recv_sem=f_recv.at[h, i],
            device_id=left if h == 0 else right, device_id_type=MESH)

    def r_copy(h, i):
        off, n = piece(h, i)
        dst = (recv_r if h == 0 else recv_l).at[pl.ds(off, n), :]
        return pltpu.make_async_remote_copy(
            src_ref=recv_f.at[pl.ds(off, n), :], dst_ref=dst,
            send_sem=r_send.at[h, i], recv_sem=(r_recv if h == 0 else l_recv).at[h, i],
            device_id=left if h == 0 else right, device_id_type=MESH)

    def n_copy(h, i):
        off, n = piece(h, i)
        dst = (recv_l if h == 0 else recv_r).at[pl.ds(off, n), :]
        return pltpu.make_async_remote_copy(
            src_ref=send_n.at[pl.ds(off, n), :], dst_ref=dst,
            send_sem=n_send.at[h, i], recv_sem=(l_recv if h == 0 else r_recv).at[h, i],
            device_id=right if h == 0 else left, device_id_type=MESH)

    def far(i):
        for h in range(2):
            off, n = piece(h, i)
            send_f[pl.ds(off, n), :] = part_sum(OPP, off, n)
            f_copy(h, i).start()

    def near(i):
        for h in range(2):
            off, n = piece(h, i)
            send_n[pl.ds(off, n), :] = part_sum(RIGHT if h == 0 else LEFT, off, n)
            n_copy(h, i).start()

    def relay(i):
        for h in range(2):
            off, n = piece(h, i)
            mine = part_sum(LEFT if h == 0 else RIGHT, off, n)
            f_copy(h, i).wait_recv()
            recv_f[pl.ds(off, n), :] = recv_f[pl.ds(off, n), :] + mine
            r_copy(h, i).start()

    def account(z, first):
        zr = z.reshape(z.shape[0] // 8, 8, rows)
        top = jnp.max(zr, axis=0)
        if first:
            m_acc[...] = top
            s_acc[...] = jnp.sum(jnp.exp(zr - top[None]), axis=0)
        else:
            old = m_acc[...]
            new = jnp.maximum(old, top)
            m_acc[...] = new
            s_acc[...] = s_acc[...] * jnp.exp(old - new) + jnp.sum(jnp.exp(zr - new[None]), axis=0)

    def arrive(h, i):
        (r_copy if h == 0 else n_copy)(h, i).wait_recv()
        (n_copy if h == 0 else r_copy)(h, i).wait_recv()

    def settle(i):
        if isinstance(i, int) and i == 0:
            arrive(0, 0)
            arrive(1, 0)
            for off in range(tail0, n_block, CHUNK):
                n = min(CHUNK, n_block - off)
                z = part_sum(OWN, off, n) + recv_l[off:off + n, :] + recv_r[off:off + n, :]
                account(z, off == tail0)
                logits_ref[off:off + n, :] = z
            return
        mine = [part_sum(OWN, *piece(h, i)) for h in range(2)]
        for h in range(2):
            off, n = piece(h, i)
            arrive(h, i)
            z = mine[h] + recv_l[pl.ds(off, n), :] + recv_r[pl.ds(off, n), :]
            account(z, False)
            logits_ref[pl.ds(off, n), :] = z

    for copy in small_in[3:]:
        copy.wait()
    tok = jnp.broadcast_to(tok_ref[...], (128, rows)).T

    def gather(step):
        for other in range(2):
            blk_chip = lax.rem(chip + jnp.where(step == 0, STEP_OF_SLOT[0], jnp.where(
                step == 1, STEP_OF_SLOT[1], jnp.where(step == 2, STEP_OF_SLOT[2], STEP_OF_SLOT[3]))), n_chip)
            blk = blk_chip * 2 + (1 - core if other else core)
            base = vp * (n_tp * n_block) + blk * n_block
            ref = e_oth if other else e_own
            acc = pick[...]
            for off in range(0, n_block, 512):
                n = min(512, n_block - off)
                for o, k in ((off, n // 128 * 128), (off + n // 128 * 128, n % 128)):
                    if k == 0:
                        continue
                    lane = lax.broadcasted_iota(jnp.int32, (rows, k), 1) + (base + o)
                    if k % 128 == 0:
                        want = jnp.concatenate([tok] * (k // 128), axis=1) if k > 128 else tok
                    else:
                        want = tok[:, :k]
                    hot = jnp.where(want == lane, 1.0, 0.0).astype(BF16)
                    acc = acc + jnp.dot(hot, ref[step, o:o + k, :], preferred_element_type=F32)
            pick[...] = acc

    def v_copy(src_buf, src_idx, dst_buf, stage, j, peer):
        return pltpu.make_async_remote_copy(
            src_ref=src_buf.at[src_idx] if src_idx is not None else src_buf, dst_ref=dst_buf,
            send_sem=v_send.at[stage, j], recv_sem=v_recv.at[stage, j],
            device_id={"vp": peer}, device_id_type=MESH)

    def rs_copy(j):
        peer = lax.rem(vp + j, n_vp)
        return v_copy(pick.at[pl.ds(pl.multiple_of(peer * slab, 8), slab), :], None, rs_buf.at[vp], 0, j, peer)

    def rs_in(j):
        src = lax.rem(vp + n_vp - j, n_vp)
        return v_copy(rs_buf, src, rs_buf.at[src], 0, j, src)

    def vp_copy(buf, stage, j):
        peer = lax.rem(vp + j, n_vp)
        return v_copy(buf, vp, buf.at[vp], stage, j, peer)

    def vp_in(buf, stage, j):
        src = lax.rem(vp + n_vp - j, n_vp)
        return v_copy(buf, src, buf.at[src], stage, j, src)

    def rows_scatter():
        for j in range(1, n_vp):
            rs_copy(j).start()
        rs_buf[vp] = pick[pl.ds(pl.multiple_of(vp * slab, 8), slab), :]

    def rows_stats():
        for j in range(1, n_vp):
            rs_in(j).wait_recv()
        tot = rs_buf[0]
        for j in range(1, n_vp):
            tot = tot + rs_buf[j]
        ag_buf[vp] = tot
        lane = lax.broadcasted_iota(jnp.int32, (slab, 128), 1)
        both = jnp.where(lane == 0, jnp.sum(tot, axis=1, keepdims=True), jnp.sum(tot * tot, axis=1, keepdims=True)).T
        row_st[tp] = jnp.zeros((1, 256), F32)
        row_st[tp, :, 0:slab] = both[0:1]
        row_st[tp, :, 128:128 + slab] = both[1:2]
        tp_start(row_st, 1)

    def rows_norm():
        tp_wait(row_st, 1)
        tot = row_st[0]
        for j in range(1, n_tp):
            tot = tot + row_st[j]
        mu = tot[:, 0:128] / full_width
        rs = lax.rsqrt(tot[:, 128:256] / full_width - mu * mu + NORM_EPS)
        mu = jnp.broadcast_to(mu, (128, 128)).T[0:slab, 0:1]
        rs = jnp.broadcast_to(rs, (128, 128)).T[0:slab, 0:1]
        out = ((ag_buf[vp] - mu) * rs * eg_ref[...] + eb_ref[...]).astype(BF16)
        ag_buf[vp] = out.astype(F32)
        for j in range(1, n_vp):
            vp_copy(ag_buf, 1, j).start()

    def rows_out():
        for j in range(1, n_vp):
            vp_in(ag_buf, 1, j).wait_recv()
        for j in range(n_vp):
            next_ref[j * slab:(j + 1) * slab, :] = ag_buf[j]

    pick[...] = jnp.zeros_like(pick)

    load(OPP, False).wait()
    for q in range(2):
        ex_copy(OPP, q).wait_recv()
        far(q)
    for slot in (LEFT, RIGHT):
        load(slot, False).wait()
        for q in range(2):
            ex_copy(slot, q).wait_recv()
    near(0)
    far(2)
    relay(0)
    load(OWN, False).wait()
    for q in range(2):
        ex_copy(OWN, q).wait_recv()

    def round_body(i, carry):
        near(i)

        @pl.when(i + 2 < n_round)
        def _():
            far(i + 2)

        relay(i)

        @pl.when(i <= 2)
        def _():
            gather(2 * i - 2)
            gather(2 * i - 1)

        @pl.when(i == 3)
        def _():
            rows_scatter()

        @pl.when(i == 4)
        def _():
            rows_stats()

        @pl.when(i == 6)
        def _():
            rows_norm()

        @pl.when(i == 2)
        def _():
            settle(0)

        @pl.when(i >= 3)
        def _():
            settle(i - 2)

        return carry

    lax.fori_loop(1, n_round, round_body, 0)

    def last_body(i, carry):
        settle(i)
        return carry

    lax.fori_loop(n_round - 2, n_round, last_body, 0)

    def merge(buf, n):
        top = buf[0]
        for j in range(1, n):
            top = jnp.maximum(top, buf[j])
        tot = jnp.exp(buf[0] - top)
        for j in range(1, n):
            tot = tot + jnp.exp(buf[j] - top)
        return top + jnp.log(tot)

    m8 = m_acc[...]
    top = jnp.max(m8, axis=0, keepdims=True)
    st_all[vp] = top + jnp.log(jnp.sum(s_acc[...] * jnp.exp(m8 - top), axis=0, keepdims=True))
    for j in range(1, n_vp):
        vp_copy(st_all, 2, j).start()
    rows_out()
    hx_copy.wait_send()
    for slot in range(4):
        for q in range(2):
            ex_copy(slot, q).wait_send()
    for h in range(2):
        f_copy(h, 0).wait_send()
        n_copy(h, 0).wait_send()
        r_copy(h, 0).wait_send()

    def drain(i, carry):
        for h in range(2):
            f_copy(h, i).wait_send()
            n_copy(h, i).wait_send()
            r_copy(h, i).wait_send()
        return carry

    lax.fori_loop(1, n_round, drain, 0)
    tp_drain(st_ln, 0)
    tp_drain(row_st, 1)
    for j in range(1, n_vp):
        rs_copy(j).wait_send()
        vp_copy(ag_buf, 1, j).wait_send()
    for j in range(1, n_vp):
        vp_in(st_all, 2, j).wait_recv()
    st_lse[tp] = merge(st_all, n_vp)
    tp_start(st_lse, 2)
    for j in range(1, n_vp):
        vp_copy(st_all, 2, j).wait_send()
    tp_wait(st_lse, 2)
    lse_ref[...] = merge(st_lse, n_tp)
    tp_drain(st_lse, 2)


def finish_kernel(n_piece, z_ref, lse_ref, next_ref, out_ref, sum_ref, row_ref, buf, sems):
    lse = lse_ref[...]
    n = z_ref.shape[0] // n_piece

    def put(j):
        part = pl.ds(j * n, n)
        return pltpu.make_async_copy(buf.at[part, :], out_ref.at[part, :], sems.at[j])

    for j in range(n_piece):
        buf[j * n:(j + 1) * n, :] = z_ref[j * n:(j + 1) * n, :] - lse
        put(j).start()
    sum_ref[...] = lse
    row_ref[...] = next_ref[...].astype(BF16)
    for j in range(n_piece):
        put(j).wait()


def solution(mesh):
    n_vp, n_tp = mesh.shape["vp"], mesh.shape["tp"]

    def per_device(hidden, lnf_gain, lnf_bias, emb_table, next_tok, eln_gain, eln_bias):
        rows, width = hidden.shape
        n_block = emb_table.shape[0] // n_tp
        slab = rows // n_vp
        n_round = n_block // 2 // CHUNK + 1
        dma = pltpu.SemaphoreType.DMA
        vmem = pl.BlockSpec(memory_space=pltpu.VMEM)
        logits, lse, next_in = pl.pallas_call(
            functools.partial(head_kernel, n_vp, n_tp, n_block, width * n_tp),
            out_shape=(
                pltpu.VMEM((n_block, rows), F32),
                pltpu.VMEM((1, rows), F32),
                pltpu.VMEM((rows, width), F32),
            ),
            in_specs=[pl.BlockSpec(memory_space=pl.ANY)] * 7,
            out_specs=(vmem, vmem, vmem),
            scratch_shapes=[
                pltpu.VMEM((4, n_block, width), BF16),
                pltpu.VMEM((4, n_block, width), BF16),
                pltpu.VMEM((4, n_block, width), F32),
                pltpu.VMEM((4, n_block, width), F32),
                pltpu.VMEM((n_block, rows), F32),
                pltpu.VMEM((n_block, rows), F32),
                pltpu.VMEM((n_block, rows), F32),
                pltpu.VMEM((n_block, rows), F32),
                pltpu.VMEM((n_block, rows), F32),
                pltpu.VMEM((2, width, rows + 256), F32),
                pltpu.VMEM((2, width, rows), BF16),
                pltpu.VMEM((8, rows), F32),
                pltpu.VMEM((8, rows), F32),
                pltpu.VMEM((rows, width), F32),
                pltpu.VMEM((n_tp, 1, 2 * rows), F32),
                pltpu.VMEM((n_tp, 1, rows), F32),
                pltpu.VMEM((n_vp, 1, rows), F32),
                pltpu.VMEM((n_vp, slab, width), F32),
                pltpu.VMEM((n_tp, 1, 256), F32),
                pltpu.VMEM((n_vp, slab, width), F32),
                dma((4,)), dma((4,)), dma((4, 2)), dma((4, 2)), dma((1,)), dma((1,)),
                dma((2, n_round)), dma((2, n_round)), dma((2, n_round)), dma((2, n_round)), dma((2, n_round)), dma((2, n_round)),
                dma((3, n_tp)), dma((3, n_tp)), dma((3, n_vp)), dma((3, n_vp)),
                pltpu.VMEM((rows, width), BF16),
                pltpu.VMEM((1, width), F32),
                pltpu.VMEM((1, width), F32),
                pltpu.VMEM((1, rows), jnp.int32),
                pltpu.VMEM((1, width), F32),
                pltpu.VMEM((1, width), F32),
                dma((6,)),
            ],
            compiler_params=pltpu.CompilerParams(
                collective_id=0, has_side_effects=True, vmem_limit_bytes=53 * 1024 * 1024),
            cost_estimate=pl.CostEstimate(
                flops=4 * rows * n_block * n_tp * width, bytes_accessed=16 * n_block * n_tp * width, transcendentals=rows * n_block),
        )(hidden, lnf_gain[None, :], lnf_bias[None, :], emb_table, next_tok[None, :], eln_gain[None, :], eln_bias[None, :])
        n_piece = 5
        logprobs_t, log_sum, next_bf = pl.pallas_call(
            functools.partial(finish_kernel, n_piece),
            out_shape=(
                jax.ShapeDtypeStruct((n_block, rows), F32),
                jax.ShapeDtypeStruct((1, rows), F32),
                jax.ShapeDtypeStruct((rows, width), BF16),
            ),
            in_specs=[vmem, vmem, vmem],
            out_specs=(pl.BlockSpec(memory_space=pl.ANY), vmem, vmem),
            scratch_shapes=[pltpu.VMEM((n_block, rows), F32), dma((n_piece,))],
            compiler_params=pltpu.CompilerParams(vmem_limit_bytes=16 * 1024 * 1024),
        )(logits, lse, next_in)
        return logprobs_t.T, log_sum[0], next_bf

    return jax.shard_map(
        per_device,
        mesh=mesh,
        in_specs=(P("dp", "tp"), P("tp"), P("tp"), P("vp", "tp"), P("dp"), P("tp"), P("tp")),
        out_specs=(P("dp", ("vp", "tp")), P("dp"), P("dp", "tp")),
        check_vma=False,
    )
```

```python
import functools

import jax
import jax.numpy as jnp
from jax import lax
from jax.experimental import pallas as pl
from jax.experimental.pallas import tpu as pltpu
from jax.sharding import PartitionSpec as P

NORM_EPS = 1e-5
MESH = pl.DeviceIdType.MESH
CHUNK = 128
F32 = jnp.float32
BF16 = jnp.bfloat16

OPP, LEFT, RIGHT, OWN = 0, 1, 2, 3
SIDE = 4
STEP_OF_SLOT = (2, 3, 1, 0)


def head_kernel(n_vp, n_tp, n_block, full_width,
                hid_hbm, g_hbm, b_hbm, emb_ref, tok_hbm, eg_hbm, eb_hbm,
                logits_ref, lse_ref, next_ref,
                e_own, e_oth, e_out, e_in, send_f, recv_f, send_n, recv_l, recv_r,
                hx, xn, m_acc, s_acc, pick, st_ln, st_lse, st_all, rs_buf, row_st, ag_buf,
                raw_src, raw_l, raw_r, slab_src, nb, nb_par, xnb,
                ld_sem, ex_send, ex_recv, hx_send, hx_recv,
                f_send, f_recv, n_send, r_send, l_recv, r_recv,
                t_send, t_recv, v_send, v_recv, raw_send, raw_recv, sx_send, sx_recv, nb_send, nb_recv, hop,
                hid_ref, g_ref, b_ref, tok_ref, eg_ref, eb_ref, in_sem):
    vp = lax.axis_index("vp")
    tp = lax.axis_index("tp")
    core = lax.rem(tp, 2)
    chip = tp // 2
    n_chip = n_tp // 2
    rows, width = hid_hbm.shape
    slab = rows // n_vp
    xslab = width // n_vp
    left_chip = lax.rem(chip + n_chip - 1, n_chip)
    right_chip = lax.rem(chip + 1, n_chip)
    left = {"tp": left_chip * 2 + core}
    right = {"tp": right_chip * 2 + core}
    partner = {"tp": chip * 2 + 1 - core}
    y = lax.rem(vp, SIDE)
    z = vp // SIDE
    n_z = n_vp // SIDE
    y_near = [{"vp": z * SIDE + lax.rem(y + d, SIDE)} for d in (1, SIDE - 1)]
    z_near = [{"vp": lax.rem(z + d, n_z) * SIDE + y} for d in (1, n_z - 1)]
    half = (n_block // 2) // CHUNK
    n_round = half + 1
    small = n_block - 2 * half * CHUNK
    small2 = (small // 16) * 8
    small1 = small - small2
    tail0 = 2 * half * CHUNK

    def piece(h, i):
        if isinstance(i, int) and i == 0:
            return (tail0 + small2, small1) if h == 0 else (tail0, small2)
        off = h * half * CHUNK + (i - 1) * CHUNK
        return (off if isinstance(i, int) else pl.multiple_of(off, CHUNK)), CHUNK

    barrier = pltpu.get_barrier_semaphore()
    for j in range(1, n_tp):
        pl.semaphore_signal(barrier, inc=1, device_id={"tp": lax.rem(tp + j, n_tp)}, device_id_type=MESH)
    for peer in y_near + z_near:
        pl.semaphore_signal(barrier, inc=1, device_id=peer, device_id_type=MESH)

    parts = ((tail0, small), (0, tail0))

    def load(slot, other, q):
        blk = lax.rem(chip + STEP_OF_SLOT[slot], n_chip) * 2 + (1 - core if other else core)
        off, n = parts[q]
        src = emb_ref.at[pl.ds(pl.multiple_of(blk * n_block + off, 8), n), :]
        dst = (e_oth if other else e_own).at[slot, pl.ds(off, n), :]
        return pltpu.make_async_copy(src, dst, ld_sem.at[int(other), slot, q])

    small_in = [pltpu.make_async_copy(src, dst, in_sem.at[k]) for k, (src, dst) in enumerate((
        (hid_hbm, hid_ref), (g_hbm, g_ref), (b_hbm, b_ref), (tok_hbm, tok_ref), (eg_hbm, eg_ref), (eb_hbm, eb_ref)))]
    for copy in small_in[:3]:
        copy.start()
    for slot in (RIGHT, LEFT):
        load(slot, True, 0).start()
        load(slot, False, 0).start()
    for slot, q in ((OPP, 0), (OPP, 1), (LEFT, 1), (RIGHT, 1), (OWN, 0), (OWN, 1)):
        load(slot, True, q).start()
        load(slot, False, q).start()
    for copy in small_in[3:]:
        copy.start()

    def total_recv(ref, sem):
        pltpu.make_async_remote_copy(src_ref=ref, dst_ref=ref, send_sem=sem, recv_sem=sem,
                                     device_id=partner, device_id_type=MESH).wait_recv()

    def total_send(ref, sem):
        pltpu.make_async_remote_copy(src_ref=ref, dst_ref=ref, send_sem=sem, recv_sem=sem,
                                     device_id=partner, device_id_type=MESH).wait_send()

    for copy in small_in[:3]:
        copy.wait()
    h_t = hid_ref[...].astype(F32).T
    hx[0, :, 0:rows] = h_t
    hx[0, :, rows:rows + 128] = jnp.broadcast_to(g_ref[...], (128, width)).T
    hx[0, :, rows + 128:rows + 256] = jnp.broadcast_to(b_ref[...], (128, width)).T
    st_ln[tp, :, 0:rows] = jnp.sum(h_t, axis=0, keepdims=True)
    st_ln[tp, :, rows:2 * rows] = jnp.sum(h_t * h_t, axis=0, keepdims=True)

    def convert(slot, q):
        off, n = parts[q]
        e_out[slot, off:off + n, :] = e_oth[slot, off:off + n, :].astype(F32)

    for slot in (RIGHT, LEFT):
        load(slot, True, 0).wait()
        load(slot, False, 0).wait()
        convert(slot, 0)
        off, n = piece(0 if slot == RIGHT else 1, 0)
        raw_src[off - tail0:off - tail0 + n, :] = e_own[slot, off:off + n, :].astype(F32)

    def raw_copy(slot, other):
        off, n = piece(0 if slot == RIGHT else 1, 0)
        src = e_out.at[slot, pl.ds(off, n), :] if other else raw_src.at[pl.ds(off - tail0, n), :]
        to = (right_chip if slot == RIGHT else left_chip) * 2 + (1 - core if other else core)
        return pltpu.make_async_remote_copy(
            src_ref=src, dst_ref=(raw_l if slot == RIGHT else raw_r).at[int(other)],
            send_sem=raw_send.at[int(slot == LEFT)], recv_sem=raw_recv.at[int(slot == LEFT)],
            device_id={"tp": to}, device_id_type=MESH)

    pl.semaphore_wait(barrier, n_tp + 3)

    def tp_start(buf, stage):
        for j in range(1, n_tp):
            pltpu.make_async_remote_copy(
                src_ref=buf.at[tp], dst_ref=buf.at[tp], send_sem=t_send.at[stage], recv_sem=t_recv.at[stage],
                device_id={"tp": lax.rem(tp + j, n_tp)}, device_id_type=MESH).start()

    def tp_wait(buf, stage):
        total_recv(buf.at[pl.ds(0, n_tp - 1)], t_recv.at[stage])

    def tp_drain(buf, stage):
        total_send(buf.at[pl.ds(0, n_tp - 1)], t_send.at[stage])

    tp_start(st_ln, 0)
    for other in (False, True):
        for slot in (RIGHT, LEFT):
            raw_copy(slot, other).start()

    hx_copy = pltpu.make_async_remote_copy(
        src_ref=hx.at[0], dst_ref=hx.at[1], send_sem=hx_send.at[0], recv_sem=hx_recv.at[0],
        device_id=partner, device_id_type=MESH)
    hx_copy.start()
    for peer in y_near:
        pl.semaphore_signal(hop.at[0], inc=1, device_id=peer, device_id_type=MESH)

    def ex_copy(slot, q):
        off, n = parts[q]
        return pltpu.make_async_remote_copy(
            src_ref=e_out.at[slot, pl.ds(off, n), :], dst_ref=e_in.at[slot, pl.ds(off, n), :],
            send_sem=ex_send.at[0], recv_sem=ex_recv.at[slot, q], device_id=partner, device_id_type=MESH)

    for slot, q in ((OPP, 0), (OPP, 1), (LEFT, 0), (RIGHT, 0), (LEFT, 1), (RIGHT, 1), (OWN, 0), (OWN, 1)):
        if q == 1 or slot in (OPP, OWN):
            load(slot, True, q).wait()
            convert(slot, q)
        ex_copy(slot, q).start()

    tp_wait(st_ln, 0)
    total = st_ln[0]
    for j in range(1, n_tp):
        total = total + st_ln[j]
    mean = total[:, 0:rows] / full_width
    rstd = lax.rsqrt(total[:, rows:2 * rows] / full_width - mean * mean + NORM_EPS)

    def norm(which):
        gain = hx[which, :, rows:rows + 128]
        bias = hx[which, :, rows + 128:rows + 256]
        for c in range(rows // 128):
            cols = slice(c * 128, c * 128 + 128)
            xn[which, :, cols] = ((hx[which, :, cols] - mean[:, cols]) * rstd[:, cols] * gain + bias).astype(BF16)

    def slab_copy(d):
        return pltpu.make_async_remote_copy(
            src_ref=slab_src, dst_ref=nb.at[d, pl.ds(pl.multiple_of(vp * xslab, 8), xslab), :],
            send_sem=sx_send.at[0], recv_sem=sx_recv.at[d], device_id=right if d == 0 else left, device_id_type=MESH)

    norm(0)
    slab_src[...] = xn[0, pl.ds(pl.multiple_of(vp * xslab, 8), xslab), :].astype(F32)
    for d in range(2):
        slab_copy(d).start()
    hx_copy.wait_recv()
    norm(1)

    def part_sum(slot, off, n):
        mine = e_own[slot, pl.ds(off, n), :]
        theirs = e_in[slot, pl.ds(off, n), :].astype(BF16)
        return (jnp.dot(mine, xn[0], preferred_element_type=F32)
                + jnp.dot(theirs, xn[1], preferred_element_type=F32))

    def f_copy(h, i):
        off, n = piece(h, i)
        return pltpu.make_async_remote_copy(
            src_ref=send_f.at[pl.ds(off, n), :], dst_ref=recv_f.at[pl.ds(off, n), :],
            send_sem=f_send.at[0], recv_sem=f_recv.at[h, i],
            device_id=left if h == 0 else right, device_id_type=MESH)

    def r_copy(h, i):
        off, n = piece(h, i)
        dst = (recv_r if h == 0 else recv_l).at[pl.ds(off, n), :]
        return pltpu.make_async_remote_copy(
            src_ref=recv_f.at[pl.ds(off, n), :], dst_ref=dst,
            send_sem=r_send.at[0], recv_sem=(r_recv if h == 0 else l_recv).at[h, i],
            device_id=left if h == 0 else right, device_id_type=MESH)

    def n_copy(h, i):
        off, n = piece(h, i)
        dst = (recv_l if h == 0 else recv_r).at[pl.ds(off, n), :]
        return pltpu.make_async_remote_copy(
            src_ref=send_n.at[pl.ds(off, n), :], dst_ref=dst,
            send_sem=n_send.at[0], recv_sem=(l_recv if h == 0 else r_recv).at[h, i],
            device_id=right if h == 0 else left, device_id_type=MESH)

    def far(i):
        for h in range(2):
            off, n = piece(h, i)
            send_f[pl.ds(off, n), :] = part_sum(OPP, off, n)
            f_copy(h, i).start()

    def near(i):
        for h in range(2):
            off, n = piece(h, i)
            send_n[pl.ds(off, n), :] = part_sum(RIGHT if h == 0 else LEFT, off, n)
            n_copy(h, i).start()

    def relay(i):
        for h in range(2):
            off, n = piece(h, i)
            mine = part_sum(LEFT if h == 0 else RIGHT, off, n)
            f_copy(h, i).wait_recv()
            recv_f[pl.ds(off, n), :] = recv_f[pl.ds(off, n), :] + mine
            r_copy(h, i).start()

    def account(z):
        zr = z.reshape(z.shape[0] // 8, 8, rows)
        old = m_acc[...]
        new = jnp.maximum(old, jnp.max(zr, axis=0))
        m_acc[...] = new
        s_acc[...] = s_acc[...] * jnp.exp(old - new) + jnp.sum(jnp.exp(zr - new[None]), axis=0)

    def settle_raw():
        for h in range(2):
            off, n = piece(h, 0)
            raw = raw_l if h == 0 else raw_r
            mine = part_sum(OWN, off, n)
            total_recv(raw, raw_recv.at[h])
            for other in range(2):
                mine = mine + jnp.dot(raw[other].astype(BF16), xnb[h, other], preferred_element_type=F32)
            r_copy(h, 0).wait_recv()
            z = mine + (recv_r if h == 0 else recv_l)[off:off + n, :]
            account(z)
            logits_ref[off:off + n, :] = z

    def settle(i):
        mine = [part_sum(OWN, *piece(h, i)) for h in range(2)]
        for h in range(2):
            off, n = piece(h, i)
            r_copy(h, i).wait_recv()
            n_copy(h, i).wait_recv()
            z = mine[h] + recv_l[pl.ds(off, n), :] + recv_r[pl.ds(off, n), :]
            account(z)
            logits_ref[pl.ds(off, n), :] = z

    for copy in small_in[3:]:
        copy.wait()
    tok = jnp.broadcast_to(tok_ref[...], (128, rows)).T

    def gather(step):
        for other in range(2):
            blk_chip = lax.rem(chip + jnp.where(step == 0, STEP_OF_SLOT[0], jnp.where(
                step == 1, STEP_OF_SLOT[1], jnp.where(step == 2, STEP_OF_SLOT[2], STEP_OF_SLOT[3]))), n_chip)
            blk = blk_chip * 2 + (1 - core if other else core)
            base = vp * (n_tp * n_block) + blk * n_block
            ref = e_oth if other else e_own
            acc = pick[...]
            for off in range(0, n_block, 512):
                n = min(512, n_block - off)
                for o, k in ((off, n // 128 * 128), (off + n // 128 * 128, n % 128)):
                    if k == 0:
                        continue
                    lane = lax.broadcasted_iota(jnp.int32, (rows, k), 1) + (base + o)
                    if k % 128 == 0:
                        want = jnp.concatenate([tok] * (k // 128), axis=1) if k > 128 else tok
                    else:
                        want = tok[:, :k]
                    hot = jnp.where(want == lane, 1.0, 0.0).astype(BF16)
                    acc = acc + jnp.dot(hot, ref[step, o:o + k, :], preferred_element_type=F32)
            pick[...] = acc

    def v_copy(src, dst, stage, j):
        return pltpu.make_async_remote_copy(
            src_ref=src, dst_ref=dst, send_sem=v_send.at[stage], recv_sem=v_recv.at[stage],
            device_id={"vp": lax.rem(vp + j, n_vp)}, device_id_type=MESH)

    def vp_start(buf, stage):
        for j in range(1, n_vp):
            v_copy(buf.at[vp], buf.at[vp], stage, j).start()

    def vp_wait(buf, stage):
        total_recv(buf.at[pl.ds(0, n_vp - 1)], v_recv.at[stage])

    def vp_drain(buf, stage):
        total_send(buf.at[pl.ds(0, n_vp - 1)], v_send.at[stage])

    def slabs_forward():
        own = pl.ds(pl.multiple_of(vp * xslab, 8), xslab)
        for d in range(2):
            slab_copy(d).wait_recv()
            for j in range(1, n_vp):
                v_copy(nb.at[d, own, :], nb.at[d, own, :], 3, j).start()

    nb_copy = pltpu.make_async_remote_copy(
        src_ref=nb, dst_ref=nb_par, send_sem=nb_send.at[0], recv_sem=nb_recv.at[0], device_id=partner, device_id_type=MESH)
    nb_rest = nb.at[:, pl.ds(0, width - xslab), :]

    def slabs_swap():
        total_recv(nb_rest, v_recv.at[3])
        nb_copy.start()
        for d in range(2):
            xnb[d, 0] = nb[d].astype(BF16)

    def slabs_done():
        nb_copy.wait_recv()
        for d in range(2):
            xnb[d, 1] = nb_par[d].astype(BF16)

    def rows_scatter():
        for j in range(1, n_vp):
            peer = lax.rem(vp + j, n_vp)
            v_copy(pick.at[pl.ds(pl.multiple_of(peer * slab, 8), slab), :], rs_buf.at[vp], 0, j).start()
        rs_buf[vp] = pick[pl.ds(pl.multiple_of(vp * slab, 8), slab), :]

    def rows_stats():
        vp_wait(rs_buf, 0)
        tot = rs_buf[0]
        for j in range(1, n_vp):
            tot = tot + rs_buf[j]
        ag_buf[vp] = tot
        lane = lax.broadcasted_iota(jnp.int32, (slab, 128), 1)
        both = jnp.where(lane == 0, jnp.sum(tot, axis=1, keepdims=True), jnp.sum(tot * tot, axis=1, keepdims=True)).T
        row_st[tp] = jnp.zeros((1, 256), F32)
        row_st[tp, :, 0:slab] = both[0:1]
        row_st[tp, :, 128:128 + slab] = both[1:2]
        tp_start(row_st, 1)

    def rows_norm():
        tp_wait(row_st, 1)
        tot = row_st[0]
        for j in range(1, n_tp):
            tot = tot + row_st[j]
        mu = tot[:, 0:128] / full_width
        rs = lax.rsqrt(tot[:, 128:256] / full_width - mu * mu + NORM_EPS)
        mu = jnp.broadcast_to(mu, (128, 128)).T[0:slab, 0:1]
        rs = jnp.broadcast_to(rs, (128, 128)).T[0:slab, 0:1]
        out = ((ag_buf[vp] - mu) * rs * eg_ref[...] + eb_ref[...]).astype(BF16)
        ag_buf[vp] = out.astype(F32)
        vp_start(ag_buf, 1)

    def rows_out():
        vp_wait(ag_buf, 1)
        for j in range(n_vp):
            next_ref[j * slab:(j + 1) * slab, :] = ag_buf[j].astype(BF16)

    pick[...] = jnp.zeros_like(pick)
    m_acc[...] = jnp.full_like(m_acc, -jnp.inf)
    s_acc[...] = jnp.zeros_like(s_acc)

    for q in range(2):
        load(OPP, False, q).wait()
        ex_copy(OPP, q).wait_recv()
        far(q)
        pl.semaphore_wait(hop.at[q], 2)
        for peer in (z_near, y_near)[q]:
            pl.semaphore_signal(hop.at[q + 1], inc=1, device_id=peer, device_id_type=MESH)
    for slot in (LEFT, RIGHT):
        ex_copy(slot, 0).wait_recv()
    far(2)
    relay(0)
    pl.semaphore_wait(hop.at[2], 2)
    for slot in (LEFT, RIGHT, OWN):
        load(slot, False, 1).wait()
        ex_copy(slot, 1).wait_recv()
    load(OWN, False, 0).wait()
    ex_copy(OWN, 0).wait_recv()

    def at(i, when, *steps):
        @pl.when(i == when)
        def _():
            for step in steps:
                step()

    def round_body(i, carry):
        near(i)

        @pl.when(i + 2 < n_round)
        def _():
            far(i + 2)

        relay(i)
        at(i, 1, slabs_forward)

        @pl.when(i <= 2)
        def _():
            gather(2 * i - 2)
            gather(2 * i - 1)

        at(i, 2, slabs_swap)
        at(i, 3, rows_scatter, slabs_done)
        at(i, 4, rows_stats, settle_raw)
        at(i, 6, rows_norm)

        @pl.when(i >= 3)
        def _():
            settle(i - 2)

        return carry

    lax.fori_loop(1, n_round, round_body, 0)

    def last_body(i, carry):
        settle(i)
        return carry

    lax.fori_loop(n_round - 2, n_round, last_body, 0)

    def merge(buf, n):
        top = buf[0]
        for j in range(1, n):
            top = jnp.maximum(top, buf[j])
        tot = jnp.exp(buf[0] - top)
        for j in range(1, n):
            tot = tot + jnp.exp(buf[j] - top)
        return top + jnp.log(tot)

    m8 = m_acc[...]
    top = jnp.max(m8, axis=0, keepdims=True)
    st_all[vp] = top + jnp.log(jnp.sum(s_acc[...] * jnp.exp(m8 - top), axis=0, keepdims=True))
    vp_start(st_all, 2)
    rows_out()
    hx_copy.wait_send()
    nb_copy.wait_send()
    total_send(e_out, ex_send.at[0])
    total_send(raw_l, raw_send.at[0])
    total_send(raw_r, raw_send.at[1])
    total_send(nb.at[0, pl.ds(0, 2 * xslab), :], sx_send.at[0])
    total_send(send_f, f_send.at[0])
    total_send(recv_f, r_send.at[0])
    total_send(send_n.at[pl.ds(0, tail0), :], n_send.at[0])
    tp_drain(st_ln, 0)
    tp_drain(row_st, 1)
    vp_drain(rs_buf, 0)
    vp_drain(ag_buf, 1)
    total_send(nb_rest, v_send.at[3])
    vp_wait(st_all, 2)
    st_lse[tp] = merge(st_all, n_vp)
    tp_start(st_lse, 2)
    vp_drain(st_all, 2)
    tp_wait(st_lse, 2)
    lse_ref[...] = merge(st_lse, n_tp)
    tp_drain(st_lse, 2)


def finish_kernel(n_piece, z_ref, lse_ref, next_ref, out_ref, sum_ref, row_ref, buf, sems):
    lse = lse_ref[...]
    n = z_ref.shape[0] // n_piece

    def put(j):
        part = pl.ds(j * n, n)
        return pltpu.make_async_copy(buf.at[part, :], out_ref.at[part, :], sems.at[j])

    small = [pltpu.make_async_copy(lse_ref, sum_ref, sems.at[n_piece]),
             pltpu.make_async_copy(next_ref, row_ref, sems.at[n_piece + 1])]
    for copy in small:
        copy.start()
    for j in range(n_piece):
        buf[j * n:(j + 1) * n, :] = z_ref[j * n:(j + 1) * n, :] - lse
        put(j).start()
    for copy in small:
        copy.wait()
    for j in range(n_piece):
        put(j).wait()


def solution(mesh):
    n_vp, n_tp = mesh.shape["vp"], mesh.shape["tp"]

    def per_device(hidden, lnf_gain, lnf_bias, emb_table, next_tok, eln_gain, eln_bias):
        rows, width = hidden.shape
        n_block = emb_table.shape[0] // n_tp
        slab = rows // n_vp
        n_round = n_block // 2 // CHUNK + 1
        small = n_block - 2 * (n_round - 1) * CHUNK
        dma = pltpu.SemaphoreType.DMA
        vmem = pl.BlockSpec(memory_space=pltpu.VMEM)
        logits, lse, next_in = pl.pallas_call(
            functools.partial(head_kernel, n_vp, n_tp, n_block, width * n_tp),
            out_shape=(
                pltpu.VMEM((n_block, rows), F32),
                pltpu.VMEM((1, rows), F32),
                pltpu.VMEM((rows, width), BF16),
            ),
            in_specs=[pl.BlockSpec(memory_space=pl.ANY)] * 7,
            out_specs=(vmem, vmem, vmem),
            scratch_shapes=[
                pltpu.VMEM((4, n_block, width), BF16),
                pltpu.VMEM((4, n_block, width), BF16),
                pltpu.VMEM((4, n_block, width), F32),
                pltpu.VMEM((4, n_block, width), F32),
                pltpu.VMEM((n_block, rows), F32),
                pltpu.VMEM((n_block, rows), F32),
                pltpu.VMEM((n_block, rows), F32),
                pltpu.VMEM((n_block, rows), F32),
                pltpu.VMEM((n_block, rows), F32),
                pltpu.VMEM((2, width, rows + 256), F32),
                pltpu.VMEM((2, width, rows), BF16),
                pltpu.VMEM((8, rows), F32),
                pltpu.VMEM((8, rows), F32),
                pltpu.VMEM((rows, width), F32),
                pltpu.VMEM((n_tp, 1, 2 * rows), F32),
                pltpu.VMEM((n_tp, 1, rows), F32),
                pltpu.VMEM((n_vp, 1, rows), F32),
                pltpu.VMEM((n_vp, slab, width), F32),
                pltpu.VMEM((n_tp, 1, 256), F32),
                pltpu.VMEM((n_vp, slab, width), F32),
                pltpu.VMEM((small, width), F32),
                pltpu.VMEM((2, small - small // 16 * 8, width), F32),
                pltpu.VMEM((2, small // 16 * 8, width), F32),
                pltpu.VMEM((width // n_vp, rows), F32),
                pltpu.VMEM((2, width, rows), F32),
                pltpu.VMEM((2, width, rows), F32),
                pltpu.VMEM((2, 2, width, rows), BF16),
                dma((2, 4, 2)), dma((1,)), dma((4, 2)), dma((1,)), dma((1,)),
                dma((1,)), dma((2, n_round)), dma((1,)), dma((1,)), dma((2, n_round)), dma((2, n_round)),
                dma((3,)), dma((3,)), dma((4,)), dma((4,)), dma((2,)), dma((2,)), dma((1,)), dma((2,)), dma((1,)), dma((1,)),
                pltpu.SemaphoreType.REGULAR((3,)),
                pltpu.VMEM((rows, width), BF16),
                pltpu.VMEM((1, width), F32),
                pltpu.VMEM((1, width), F32),
                pltpu.VMEM((1, rows), jnp.int32),
                pltpu.VMEM((1, width), F32),
                pltpu.VMEM((1, width), F32),
                dma((6,)),
            ],
            compiler_params=pltpu.CompilerParams(
                collective_id=0, has_side_effects=True, vmem_limit_bytes=57 * 1024 * 1024),
            cost_estimate=pl.CostEstimate(
                flops=4 * rows * n_block * n_tp * width, bytes_accessed=16 * n_block * n_tp * width, transcendentals=rows * n_block),
        )(hidden, lnf_gain[None, :], lnf_bias[None, :], emb_table, next_tok[None, :], eln_gain[None, :], eln_bias[None, :])
        n_piece = 5
        logprobs_t, log_sum, next_bf = pl.pallas_call(
            functools.partial(finish_kernel, n_piece),
            out_shape=(
                jax.ShapeDtypeStruct((n_block, rows), F32),
                jax.ShapeDtypeStruct((1, rows), F32),
                jax.ShapeDtypeStruct((rows, width), BF16),
            ),
            in_specs=[vmem, vmem, vmem],
            out_specs=(pl.BlockSpec(memory_space=pl.ANY),) * 3,
            scratch_shapes=[pltpu.VMEM((n_block, rows), F32), dma((n_piece + 2,))],
            compiler_params=pltpu.CompilerParams(vmem_limit_bytes=16 * 1024 * 1024),
        )(logits, lse, next_in)
        return logprobs_t.T, log_sum[0], next_bf

    return jax.shard_map(
        per_device,
        mesh=mesh,
        in_specs=(P("dp", "tp"), P("tp"), P("tp"), P("vp", "tp"), P("dp"), P("tp"), P("tp")),
        out_specs=(P("dp", ("vp", "tp")), P("dp"), P("dp", "tp")),
        check_vma=False,
    )
```

```python
import functools

import jax
import jax.numpy as jnp
from jax import lax
from jax.experimental import pallas as pl
from jax.experimental.pallas import tpu as pltpu
from jax.sharding import PartitionSpec as P

NORM_EPS = 1e-5
MESH = pl.DeviceIdType.MESH
CHUNK = 128
F32 = jnp.float32
BF16 = jnp.bfloat16

OPP, LEFT, RIGHT, OWN = 0, 1, 2, 3
SIDE = 4
STEP_OF_SLOT = (2, 3, 1, 0)


def head_kernel(n_vp, n_tp, n_block, full_width,
                hid_hbm, g_hbm, b_hbm, emb_ref, tok_hbm, eg_hbm, eb_hbm,
                logits_ref, lse_ref, next_ref,
                e_own, e_oth, e_out, e_in, send_f, recv_f, send_n, recv_l, recv_r,
                hx, xn, m_acc, s_acc, pick, st_ln, st_lse, st_all, rs_buf, row_st, ag_buf,
                raw_src, raw_l, raw_r, slab_src, nb, nb_par, xnb,
                ld_sem, ex_send, ex_recv, hx_send, hx_recv,
                f_send, f_recv, n_send, r_send, in_recv,
                t_send, t_recv, v_send, v_recv, raw_send, raw_recv, sx_send, sx_recv, nb_send, nb_recv, hop,
                hid_ref, tok_ref, vec_ref, in_sem):
    vp = lax.axis_index("vp")
    tp = lax.axis_index("tp")
    core = lax.rem(tp, 2)
    chip = tp // 2
    n_chip = n_tp // 2
    rows, width = hid_hbm.shape
    slab = rows // n_vp
    xslab = width // n_vp
    left_chip = lax.rem(chip + n_chip - 1, n_chip)
    right_chip = lax.rem(chip + 1, n_chip)
    left = {"tp": left_chip * 2 + core}
    right = {"tp": right_chip * 2 + core}
    partner = {"tp": chip * 2 + 1 - core}
    y = lax.rem(vp, SIDE)
    z = vp // SIDE
    n_z = n_vp // SIDE
    y_near = [{"vp": z * SIDE + lax.rem(y + d, SIDE)} for d in (1, SIDE - 1)]
    z_near = [{"vp": lax.rem(z + d, n_z) * SIDE + y} for d in (1, n_z - 1)]
    half = (n_block // 2) // CHUNK
    n_round = half + 1
    small = n_block - 2 * half * CHUNK
    small2 = (small // 16) * 8
    small1 = small - small2
    tail0 = 2 * half * CHUNK

    def piece(h, i):
        if isinstance(i, int) and i == 0:
            return (tail0 + small2, small1) if h == 0 else (tail0, small2)
        off = h * half * CHUNK + (i - 1) * CHUNK
        return (off if isinstance(i, int) else pl.multiple_of(off, CHUNK)), CHUNK

    barrier = pltpu.get_barrier_semaphore()
    for j in range(1, n_tp):
        pl.semaphore_signal(barrier, inc=1, device_id={"tp": lax.rem(tp + j, n_tp)}, device_id_type=MESH)
    for peer in y_near + z_near:
        pl.semaphore_signal(barrier, inc=1, device_id=peer, device_id_type=MESH)

    parts = ((tail0, small), (0, tail0), (0, n_block))

    def load(slot, other, q, sem):
        blk = lax.rem(chip + STEP_OF_SLOT[slot], n_chip) * 2 + (1 - core if other else core)
        off, n = parts[q]
        src = emb_ref.at[pl.ds(pl.multiple_of(blk * n_block + off, 8), n), :]
        dst = (e_oth if other else e_own).at[slot, pl.ds(off, n), :]
        return pltpu.make_async_copy(src, dst, ld_sem.at[sem])

    hid_copy = pltpu.make_async_copy(hid_hbm, hid_ref, in_sem.at[0])
    tok_copy = pltpu.make_async_copy(tok_hbm, tok_ref, in_sem.at[1])
    hid_copy.start()
    for k, src in enumerate((g_hbm, b_hbm, eg_hbm, eb_hbm)):
        pltpu.make_async_copy(src, vec_ref.at[k], in_sem.at[2]).start()
    for slot in (RIGHT, LEFT):
        load(slot, True, 0, 0).start()
        load(slot, False, 0, 0).start()

    def total_load(ref, sem):
        pltpu.make_async_copy(ref, ref, sem).wait()

    def total_recv(ref, sem):
        pltpu.make_async_remote_copy(src_ref=ref, dst_ref=ref, send_sem=sem, recv_sem=sem,
                                     device_id=partner, device_id_type=MESH).wait_recv()

    def total_send(ref, sem):
        pltpu.make_async_remote_copy(src_ref=ref, dst_ref=ref, send_sem=sem, recv_sem=sem,
                                     device_id=partner, device_id_type=MESH).wait_send()

    hid_copy.wait()
    h_t = hid_ref[...].astype(F32).T
    hx[0, :, 0:rows] = h_t
    st_ln[tp, :, 0:rows] = jnp.sum(h_t, axis=0, keepdims=True)
    st_ln[tp, :, rows:2 * rows] = jnp.sum(h_t * h_t, axis=0, keepdims=True)

    def convert(slot, q):
        off, n = parts[q]
        e_out[slot, off:off + n, :] = e_oth[slot, off:off + n, :].astype(F32)

    total_load(e_own.at[0, pl.ds(0, 4 * small), :], ld_sem.at[0])
    for slot, q, sem in ((OPP, 2, 1), (LEFT, 1, 3), (RIGHT, 1, 3), (OWN, 2, 4)):
        load(slot, True, q, sem).start()
        if slot == OPP:
            load(slot, False, q, 2).start()
    for slot, q, sem in ((LEFT, 1, 5), (RIGHT, 1, 5), (OWN, 2, 6)):
        load(slot, False, q, sem).start()
    tok_copy.start()
    for slot in (RIGHT, LEFT):
        convert(slot, 0)
        off, n = piece(0 if slot == RIGHT else 1, 0)
        raw_src[off - tail0:off - tail0 + n, :] = e_own[slot, off:off + n, :].astype(F32)

    def raw_copy(slot, other):
        off, n = piece(0 if slot == RIGHT else 1, 0)
        src = e_out.at[slot, pl.ds(off, n), :] if other else raw_src.at[pl.ds(off - tail0, n), :]
        to = (right_chip if slot == RIGHT else left_chip) * 2 + (1 - core if other else core)
        return pltpu.make_async_remote_copy(
            src_ref=src, dst_ref=(raw_l if slot == RIGHT else raw_r).at[int(other)],
            send_sem=raw_send.at[0], recv_sem=raw_recv.at[int(slot == LEFT)],
            device_id={"tp": to}, device_id_type=MESH)

    pl.semaphore_wait(barrier, n_tp + 3)

    def tp_start(buf, stage):
        for j in range(1, n_tp):
            pltpu.make_async_remote_copy(
                src_ref=buf.at[tp], dst_ref=buf.at[tp], send_sem=t_send.at[stage], recv_sem=t_recv.at[stage],
                device_id={"tp": lax.rem(tp + j, n_tp)}, device_id_type=MESH).start()

    def tp_wait(buf, stage):
        total_recv(buf.at[pl.ds(0, n_tp - 1)], t_recv.at[stage])

    def tp_drain(buf, stage):
        total_send(buf.at[pl.ds(0, n_tp - 1)], t_send.at[stage])

    tp_start(st_ln, 0)
    for other in (False, True):
        for slot in (RIGHT, LEFT):
            raw_copy(slot, other).start()

    total_load(vec_ref, in_sem.at[2])
    hx[0, :, rows:rows + 128] = jnp.broadcast_to(vec_ref[0], (128, width)).T
    hx[0, :, rows + 128:rows + 256] = jnp.broadcast_to(vec_ref[1], (128, width)).T
    hx_copy = pltpu.make_async_remote_copy(
        src_ref=hx.at[0], dst_ref=hx.at[1], send_sem=hx_send.at[0], recv_sem=hx_recv.at[0],
        device_id=partner, device_id_type=MESH)
    hx_copy.start()
    for peer in y_near:
        pl.semaphore_signal(hop.at[0], inc=1, device_id=peer, device_id_type=MESH)

    def ex_copy(slot, q, sem):
        off, n = parts[q]
        return pltpu.make_async_remote_copy(
            src_ref=e_out.at[slot, pl.ds(off, n), :], dst_ref=e_in.at[slot, pl.ds(off, n), :],
            send_sem=ex_send.at[0], recv_sem=ex_recv.at[sem], device_id=partner, device_id_type=MESH)

    load(OPP, True, 2, 1).wait()
    for q in range(2):
        convert(OPP, q)
        ex_copy(OPP, q, q).start()
    for slot in (LEFT, RIGHT):
        ex_copy(slot, 0, 2).start()
    sides = e_oth.at[pl.ds(LEFT, 2), pl.ds(0, tail0), :]
    total_load(sides, ld_sem.at[3])
    for slot in (LEFT, RIGHT):
        convert(slot, 1)
        ex_copy(slot, 1, 3).start()
    load(OWN, True, 2, 4).wait()
    convert(OWN, 2)
    ex_copy(OWN, 2, 4).start()

    tp_wait(st_ln, 0)
    total = st_ln[0]
    for j in range(1, n_tp):
        total = total + st_ln[j]
    mean = total[:, 0:rows] / full_width
    rstd = lax.rsqrt(total[:, rows:2 * rows] / full_width - mean * mean + NORM_EPS)

    def norm(which):
        gain = hx[which, :, rows:rows + 128]
        bias = hx[which, :, rows + 128:rows + 256]
        for c in range(rows // 128):
            cols = slice(c * 128, c * 128 + 128)
            xn[which, :, cols] = ((hx[which, :, cols] - mean[:, cols]) * rstd[:, cols] * gain + bias).astype(BF16)

    def slab_copy(d):
        return pltpu.make_async_remote_copy(
            src_ref=slab_src, dst_ref=nb.at[d, pl.ds(pl.multiple_of(vp * xslab, 8), xslab), :],
            send_sem=sx_send.at[0], recv_sem=sx_recv.at[d], device_id=right if d == 0 else left, device_id_type=MESH)

    norm(0)
    slab_src[...] = xn[0, pl.ds(pl.multiple_of(vp * xslab, 8), xslab), :].astype(F32)
    for d in range(2):
        slab_copy(d).start()
    hx_copy.wait_recv()
    norm(1)

    def part_sum(slot, off, n):
        mine = e_own[slot, pl.ds(off, n), :]
        theirs = e_in[slot, pl.ds(off, n), :].astype(BF16)
        return (jnp.dot(mine, xn[0], preferred_element_type=F32)
                + jnp.dot(theirs, xn[1], preferred_element_type=F32))

    def f_copy(h, i):
        off, n = piece(h, i)
        return pltpu.make_async_remote_copy(
            src_ref=send_f.at[pl.ds(off, n), :], dst_ref=recv_f.at[pl.ds(off, n), :],
            send_sem=f_send.at[0], recv_sem=f_recv.at[i],
            device_id=left if h == 0 else right, device_id_type=MESH)

    def r_copy(h, i):
        off, n = piece(h, i)
        dst = (recv_r if h == 0 else recv_l).at[pl.ds(off, n), :]
        return pltpu.make_async_remote_copy(
            src_ref=recv_f.at[pl.ds(off, n), :], dst_ref=dst,
            send_sem=r_send.at[0], recv_sem=in_recv.at[i],
            device_id=left if h == 0 else right, device_id_type=MESH)

    def n_copy(h, i):
        off, n = piece(h, i)
        dst = (recv_l if h == 0 else recv_r).at[pl.ds(off, n), :]
        return pltpu.make_async_remote_copy(
            src_ref=send_n.at[pl.ds(off, n), :], dst_ref=dst,
            send_sem=n_send.at[0], recv_sem=in_recv.at[i],
            device_id=right if h == 0 else left, device_id_type=MESH)

    def far(i):
        for h in range(2):
            off, n = piece(h, i)
            send_f[pl.ds(off, n), :] = part_sum(OPP, off, n)
            f_copy(h, i).start()

    def near(i):
        for h in range(2):
            off, n = piece(h, i)
            send_n[pl.ds(off, n), :] = part_sum(RIGHT if h == 0 else LEFT, off, n)
            n_copy(h, i).start()

    def relay(i):
        mine = [part_sum(LEFT if h == 0 else RIGHT, *piece(h, i)) for h in range(2)]
        total_recv(recv_f.at[pl.ds(0, small if isinstance(i, int) else 2 * CHUNK), :], f_recv.at[i])
        for h in range(2):
            off, n = piece(h, i)
            recv_f[pl.ds(off, n), :] = recv_f[pl.ds(off, n), :] + mine[h]
            r_copy(h, i).start()

    def account(z):
        zr = z.reshape(z.shape[0] // 8, 8, rows)
        old = m_acc[...]
        new = jnp.maximum(old, jnp.max(zr, axis=0))
        m_acc[...] = new
        s_acc[...] = s_acc[...] * jnp.exp(old - new) + jnp.sum(jnp.exp(zr - new[None]), axis=0)

    def settle_raw():
        for h in range(2):
            off, n = piece(h, 0)
            raw = raw_l if h == 0 else raw_r
            if h == 0:
                total_recv(recv_l.at[pl.ds(0, small), :], in_recv.at[0])
            mine = part_sum(OWN, off, n)
            total_recv(raw, raw_recv.at[h])
            for other in range(2):
                mine = mine + jnp.dot(raw[other].astype(BF16), xnb[h, other], preferred_element_type=F32)
            z = mine + (recv_r if h == 0 else recv_l)[off:off + n, :]
            account(z)
            logits_ref[off:off + n, :] = z

    def settle(i):
        mine = [part_sum(OWN, *piece(h, i)) for h in range(2)]
        total_recv(recv_l.at[pl.ds(0, 4 * CHUNK), :], in_recv.at[i])
        for h in range(2):
            off, n = piece(h, i)
            z = mine[h] + recv_l[pl.ds(off, n), :] + recv_r[pl.ds(off, n), :]
            account(z)
            logits_ref[pl.ds(off, n), :] = z

    tok_copy.wait()
    tok = jnp.broadcast_to(tok_ref[...], (128, rows)).T

    def gather(step):
        for other in range(2):
            blk_chip = lax.rem(chip + jnp.where(step == 0, STEP_OF_SLOT[0], jnp.where(
                step == 1, STEP_OF_SLOT[1], jnp.where(step == 2, STEP_OF_SLOT[2], STEP_OF_SLOT[3]))), n_chip)
            blk = blk_chip * 2 + (1 - core if other else core)
            base = vp * (n_tp * n_block) + blk * n_block
            ref = e_oth if other else e_own
            acc = pick[...]
            for off in range(0, n_block, 512):
                n = min(512, n_block - off)
                for o, k in ((off, n // 128 * 128), (off + n // 128 * 128, n % 128)):
                    if k == 0:
                        continue
                    lane = lax.broadcasted_iota(jnp.int32, (rows, k), 1) + (base + o)
                    if k % 128 == 0:
                        want = jnp.concatenate([tok] * (k // 128), axis=1) if k > 128 else tok
                    else:
                        want = tok[:, :k]
                    hot = jnp.where(want == lane, 1.0, 0.0).astype(BF16)
                    acc = acc + jnp.dot(hot, ref[step, o:o + k, :], preferred_element_type=F32)
            pick[...] = acc

    def v_copy(src, dst, stage, j):
        return pltpu.make_async_remote_copy(
            src_ref=src, dst_ref=dst, send_sem=v_send.at[stage], recv_sem=v_recv.at[stage],
            device_id={"vp": lax.rem(vp + j, n_vp)}, device_id_type=MESH)

    def vp_start(buf, stage):
        for j in range(1, n_vp):
            v_copy(buf.at[vp], buf.at[vp], stage, j).start()

    def vp_wait(buf, stage):
        total_recv(buf.at[pl.ds(0, n_vp - 1)], v_recv.at[stage])

    def vp_drain(buf, stage):
        total_send(buf.at[pl.ds(0, n_vp - 1)], v_send.at[stage])

    def slabs_forward():
        own = pl.ds(pl.multiple_of(vp * xslab, 8), xslab)
        for d in range(2):
            slab_copy(d).wait_recv()
            for j in range(1, n_vp):
                v_copy(nb.at[d, own, :], nb.at[d, own, :], 3, j).start()

    nb_copy = pltpu.make_async_remote_copy(
        src_ref=nb, dst_ref=nb_par, send_sem=nb_send.at[0], recv_sem=nb_recv.at[0], device_id=partner, device_id_type=MESH)
    nb_rest = nb.at[:, pl.ds(0, width - xslab), :]

    def slabs_swap():
        total_recv(nb_rest, v_recv.at[3])
        nb_copy.start()
        for d in range(2):
            xnb[d, 0] = nb[d].astype(BF16)

    def slabs_done():
        nb_copy.wait_recv()
        for d in range(2):
            xnb[d, 1] = nb_par[d].astype(BF16)

    def rows_scatter():
        for j in range(1, n_vp):
            peer = lax.rem(vp + j, n_vp)
            v_copy(pick.at[pl.ds(pl.multiple_of(peer * slab, 8), slab), :], rs_buf.at[vp], 0, j).start()
        rs_buf[vp] = pick[pl.ds(pl.multiple_of(vp * slab, 8), slab), :]

    def rows_stats():
        vp_wait(rs_buf, 0)
        tot = rs_buf[0]
        for j in range(1, n_vp):
            tot = tot + rs_buf[j]
        ag_buf[vp] = tot
        lane = lax.broadcasted_iota(jnp.int32, (slab, 128), 1)
        both = jnp.where(lane == 0, jnp.sum(tot, axis=1, keepdims=True), jnp.sum(tot * tot, axis=1, keepdims=True)).T
        row_st[tp] = jnp.zeros((1, 256), F32)
        row_st[tp, :, 0:slab] = both[0:1]
        row_st[tp, :, 128:128 + slab] = both[1:2]
        tp_start(row_st, 1)

    def rows_norm():
        tp_wait(row_st, 1)
        tot = row_st[0]
        for j in range(1, n_tp):
            tot = tot + row_st[j]
        mu = tot[:, 0:128] / full_width
        rs = lax.rsqrt(tot[:, 128:256] / full_width - mu * mu + NORM_EPS)
        mu = jnp.broadcast_to(mu, (128, 128)).T[0:slab, 0:1]
        rs = jnp.broadcast_to(rs, (128, 128)).T[0:slab, 0:1]
        out = ((ag_buf[vp] - mu) * rs * vec_ref[2] + vec_ref[3]).astype(BF16)
        ag_buf[vp] = out.astype(F32)
        vp_start(ag_buf, 1)

    def rows_out():
        vp_wait(ag_buf, 1)
        for j in range(n_vp):
            next_ref[j * slab:(j + 1) * slab, :] = ag_buf[j].astype(BF16)

    pick[...] = jnp.zeros_like(pick)
    m_acc[...] = jnp.full_like(m_acc, -jnp.inf)
    s_acc[...] = jnp.zeros_like(s_acc)

    load(OPP, False, 2, 2).wait()
    for q in range(2):
        ex_copy(OPP, q, q).wait_recv()
        far(q)
        pl.semaphore_wait(hop.at[q], 2)
        for peer in (z_near, y_near)[q]:
            pl.semaphore_signal(hop.at[q + 1], inc=1, device_id=peer, device_id_type=MESH)
    total_recv(e_in.at[pl.ds(LEFT, 2), pl.ds(tail0, small), :], ex_recv.at[2])
    far(2)
    relay(0)
    pl.semaphore_wait(hop.at[2], 2)
    total_load(sides, ld_sem.at[5])
    total_recv(e_in.at[pl.ds(LEFT, 2), pl.ds(0, tail0), :], ex_recv.at[3])
    load(OWN, False, 2, 6).wait()
    ex_copy(OWN, 2, 4).wait_recv()

    def at(i, when, *steps):
        @pl.when(i == when)
        def _():
            for step in steps:
                step()

    def round_body(i, carry):
        near(i)

        @pl.when(i + 2 < n_round)
        def _():
            far(i + 2)

        relay(i)
        at(i, 1, slabs_forward)

        @pl.when(i <= 2)
        def _():
            gather(2 * i - 2)
            gather(2 * i - 1)

        at(i, 2, slabs_swap)
        at(i, 3, rows_scatter, slabs_done)
        at(i, 4, rows_stats, settle_raw)
        at(i, 6, rows_norm)

        @pl.when(i >= 3)
        def _():
            settle(i - 2)

        return carry

    lax.fori_loop(1, n_round, round_body, 0)

    def last_body(i, carry):
        settle(i)
        return carry

    lax.fori_loop(n_round - 2, n_round, last_body, 0)

    def merge(buf, n):
        top = buf[0]
        for j in range(1, n):
            top = jnp.maximum(top, buf[j])
        tot = jnp.exp(buf[0] - top)
        for j in range(1, n):
            tot = tot + jnp.exp(buf[j] - top)
        return top + jnp.log(tot)

    m8 = m_acc[...]
    top = jnp.max(m8, axis=0, keepdims=True)
    st_all[vp] = top + jnp.log(jnp.sum(s_acc[...] * jnp.exp(m8 - top), axis=0, keepdims=True))
    vp_start(st_all, 2)
    rows_out()
    hx_copy.wait_send()
    nb_copy.wait_send()
    total_send(e_out, ex_send.at[0])
    total_send(e_in.at[0, pl.ds(0, 2 * small), :], raw_send.at[0])
    total_send(nb.at[0, pl.ds(0, 2 * xslab), :], sx_send.at[0])
    total_send(send_f, f_send.at[0])
    total_send(recv_f, r_send.at[0])
    total_send(send_n.at[pl.ds(0, tail0), :], n_send.at[0])
    tp_drain(st_ln, 0)
    tp_drain(row_st, 1)
    vp_drain(rs_buf, 0)
    vp_drain(ag_buf, 1)
    total_send(nb_rest, v_send.at[3])
    vp_wait(st_all, 2)
    st_lse[tp] = merge(st_all, n_vp)
    tp_start(st_lse, 2)
    vp_drain(st_all, 2)
    tp_wait(st_lse, 2)
    lse_ref[...] = merge(st_lse, n_tp)
    tp_drain(st_lse, 2)


def finish_kernel(n_piece, z_ref, lse_ref, next_ref, out_ref, sum_ref, row_ref, buf, sems):
    lse = lse_ref[...]
    n = z_ref.shape[0] // n_piece

    def put(j):
        part = pl.ds(j * n, n)
        return pltpu.make_async_copy(buf.at[part, :], out_ref.at[part, :], sems.at[j])

    small = [pltpu.make_async_copy(lse_ref, sum_ref, sems.at[n_piece]),
             pltpu.make_async_copy(next_ref, row_ref, sems.at[n_piece + 1])]
    for copy in small:
        copy.start()
    for j in range(n_piece):
        buf[j * n:(j + 1) * n, :] = z_ref[j * n:(j + 1) * n, :] - lse
        put(j).start()
    for copy in small:
        copy.wait()
    for j in range(n_piece):
        put(j).wait()


def solution(mesh):
    n_vp, n_tp = mesh.shape["vp"], mesh.shape["tp"]

    def per_device(hidden, lnf_gain, lnf_bias, emb_table, next_tok, eln_gain, eln_bias):
        rows, width = hidden.shape
        n_block = emb_table.shape[0] // n_tp
        slab = rows // n_vp
        n_round = n_block // 2 // CHUNK + 1
        small = n_block - 2 * (n_round - 1) * CHUNK
        dma = pltpu.SemaphoreType.DMA
        vmem = pl.BlockSpec(memory_space=pltpu.VMEM)
        logits, lse, next_in = pl.pallas_call(
            functools.partial(head_kernel, n_vp, n_tp, n_block, width * n_tp),
            out_shape=(
                pltpu.VMEM((n_block, rows), F32),
                pltpu.VMEM((1, rows), F32),
                pltpu.VMEM((rows, width), BF16),
            ),
            in_specs=[pl.BlockSpec(memory_space=pl.ANY)] * 7,
            out_specs=(vmem, vmem, vmem),
            scratch_shapes=[
                pltpu.VMEM((4, n_block, width), BF16),
                pltpu.VMEM((4, n_block, width), BF16),
                pltpu.VMEM((4, n_block, width), F32),
                pltpu.VMEM((4, n_block, width), F32),
                pltpu.VMEM((n_block, rows), F32),
                pltpu.VMEM((n_block, rows), F32),
                pltpu.VMEM((n_block, rows), F32),
                pltpu.VMEM((n_block, rows), F32),
                pltpu.VMEM((n_block, rows), F32),
                pltpu.VMEM((2, width, rows + 256), F32),
                pltpu.VMEM((2, width, rows), BF16),
                pltpu.VMEM((8, rows), F32),
                pltpu.VMEM((8, rows), F32),
                pltpu.VMEM((rows, width), F32),
                pltpu.VMEM((n_tp, 1, 2 * rows), F32),
                pltpu.VMEM((n_tp, 1, rows), F32),
                pltpu.VMEM((n_vp, 1, rows), F32),
                pltpu.VMEM((n_vp, slab, width), F32),
                pltpu.VMEM((n_tp, 1, 256), F32),
                pltpu.VMEM((n_vp, slab, width), F32),
                pltpu.VMEM((small, width), F32),
                pltpu.VMEM((2, small - small // 16 * 8, width), F32),
                pltpu.VMEM((2, small // 16 * 8, width), F32),
                pltpu.VMEM((width // n_vp, rows), F32),
                pltpu.VMEM((2, width, rows), F32),
                pltpu.VMEM((2, width, rows), F32),
                pltpu.VMEM((2, 2, width, rows), BF16),
                dma((7,)), dma((1,)), dma((5,)), dma((1,)), dma((1,)),
                dma((1,)), dma((n_round,)), dma((1,)), dma((1,)), dma((n_round,)),
                dma((3,)), dma((3,)), dma((4,)), dma((4,)), dma((1,)), dma((2,)), dma((1,)), dma((2,)), dma((1,)), dma((1,)),
                pltpu.SemaphoreType.REGULAR((3,)),
                pltpu.VMEM((rows, width), BF16),
                pltpu.VMEM((1, rows), jnp.int32),
                pltpu.VMEM((4, 1, width), F32),
                dma((3,)),
            ],
            compiler_params=pltpu.CompilerParams(
                collective_id=0, has_side_effects=True, vmem_limit_bytes=57 * 1024 * 1024),
            cost_estimate=pl.CostEstimate(
                flops=4 * rows * n_block * n_tp * width, bytes_accessed=16 * n_block * n_tp * width, transcendentals=rows * n_block),
        )(hidden, lnf_gain[None, :], lnf_bias[None, :], emb_table, next_tok[None, :], eln_gain[None, :], eln_bias[None, :])
        n_piece = 5
        logprobs_t, log_sum, next_bf = pl.pallas_call(
            functools.partial(finish_kernel, n_piece),
            out_shape=(
                jax.ShapeDtypeStruct((n_block, rows), F32),
                jax.ShapeDtypeStruct((1, rows), F32),
                jax.ShapeDtypeStruct((rows, width), BF16),
            ),
            in_specs=[vmem, vmem, vmem],
            out_specs=(pl.BlockSpec(memory_space=pl.ANY),) * 3,
            scratch_shapes=[pltpu.VMEM((n_block, rows), F32), dma((n_piece + 2,))],
            compiler_params=pltpu.CompilerParams(vmem_limit_bytes=16 * 1024 * 1024),
        )(logits, lse, next_in)
        return logprobs_t.T, log_sum[0], next_bf

    return jax.shard_map(
        per_device,
        mesh=mesh,
        in_specs=(P("dp", "tp"), P("tp"), P("tp"), P("vp", "tp"), P("dp"), P("tp"), P("tp")),
        out_specs=(P("dp", ("vp", "tp")), P("dp"), P("dp", "tp")),
        check_vma=False,
    )
```

```python
import functools

import jax
import jax.numpy as jnp
from jax import lax
from jax.experimental import pallas as pl
from jax.experimental.pallas import tpu as pltpu
from jax.sharding import PartitionSpec as P

NORM_EPS = 1e-5
MESH = pl.DeviceIdType.MESH
CHUNK = 128
F32 = jnp.float32
BF16 = jnp.bfloat16

OPP, LEFT, RIGHT, OWN = 0, 1, 2, 3
SIDE = 4
STEP_OF_SLOT = (2, 3, 1, 0)


def head_kernel(n_vp, n_tp, n_block, full_width,
                hid_hbm, g_hbm, b_hbm, emb_ref, tok_hbm, eg_hbm, eb_hbm,
                logits_ref, lse_ref, next_ref,
                e_own, e_oth, e_out, e_in, send_f, recv_f, send_n, recv_l, recv_r,
                hx, xn, m_acc, s_acc, pick, st_ln, st_lse, st_all, rs_buf, row_st, ag_buf,
                raw_src, raw_l, raw_r, slab_src, nb, nb_par, xnb,
                ld_sem, ex_send, ex_recv, hx_send, hx_recv,
                f_send, f_recv, n_send, r_send, in_recv,
                t_send, t_recv, v_send, v_recv, raw_send, raw_recv, sx_send, sx_recv, nb_send, nb_recv, hop,
                hid_ref, tok_ref, vec_ref, in_sem):
    vp = lax.axis_index("vp")
    tp = lax.axis_index("tp")
    core = lax.rem(tp, 2)
    chip = tp // 2
    n_chip = n_tp // 2
    rows, width = hid_hbm.shape
    slab = rows // n_vp
    xslab = width // n_vp
    left_chip = lax.rem(chip + n_chip - 1, n_chip)
    right_chip = lax.rem(chip + 1, n_chip)
    left = {"tp": left_chip * 2 + core}
    right = {"tp": right_chip * 2 + core}
    partner = {"tp": chip * 2 + 1 - core}
    y = lax.rem(vp, SIDE)
    z = vp // SIDE
    n_z = n_vp // SIDE
    y_near = [{"vp": z * SIDE + lax.rem(y + d, SIDE)} for d in (1, SIDE - 1)]
    z_near = [{"vp": lax.rem(z + d, n_z) * SIDE + y} for d in (1, n_z - 1)]
    half = (n_block // 2) // CHUNK
    n_round = half + 1
    small = n_block - 2 * half * CHUNK
    small1 = (small // 16) * 8
    small2 = small - small1
    tail0 = 2 * half * CHUNK

    def piece(h, i):
        if isinstance(i, int) and i == 0:
            return (tail0, small1) if h == 0 else (tail0 + small1, small2)
        off = h * half * CHUNK + (i - 1) * CHUNK
        return (off if isinstance(i, int) else pl.multiple_of(off, CHUNK)), CHUNK

    barrier = pltpu.get_barrier_semaphore()
    for j in range(1, n_tp):
        pl.semaphore_signal(barrier, inc=1, device_id={"tp": lax.rem(tp + j, n_tp)}, device_id_type=MESH)
    for peer in y_near + z_near:
        pl.semaphore_signal(barrier, inc=1, device_id=peer, device_id_type=MESH)

    parts = ((tail0, small), (0, tail0), (0, n_block))

    def load(slot, other, q, sem):
        blk = lax.rem(chip + STEP_OF_SLOT[slot], n_chip) * 2 + (1 - core if other else core)
        off, n = parts[q]
        src = emb_ref.at[pl.ds(pl.multiple_of(blk * n_block + off, 8), n), :]
        dst = (e_oth if other else e_own).at[slot, pl.ds(off, n), :]
        return pltpu.make_async_copy(src, dst, ld_sem.at[sem])

    hid_copy = pltpu.make_async_copy(hid_hbm, hid_ref, in_sem.at[0])
    tok_copy = pltpu.make_async_copy(tok_hbm, tok_ref, in_sem.at[1])
    hid_copy.start()
    for k, src in enumerate((g_hbm, b_hbm, eg_hbm, eb_hbm)):
        pltpu.make_async_copy(src, vec_ref.at[k], in_sem.at[2]).start()
    for slot in (RIGHT, LEFT):
        load(slot, True, 0, 0).start()
        load(slot, False, 0, 0).start()

    def total_load(ref, sem):
        pltpu.make_async_copy(ref, ref, sem).wait()

    def total_recv(ref, sem):
        pltpu.make_async_remote_copy(src_ref=ref, dst_ref=ref, send_sem=sem, recv_sem=sem,
                                     device_id=partner, device_id_type=MESH).wait_recv()

    def total_send(ref, sem):
        pltpu.make_async_remote_copy(src_ref=ref, dst_ref=ref, send_sem=sem, recv_sem=sem,
                                     device_id=partner, device_id_type=MESH).wait_send()

    hid_copy.wait()
    h_t = hid_ref[...].astype(F32).T
    hx[0, :, 0:rows] = h_t
    st_ln[tp, :, 0:rows] = jnp.sum(h_t, axis=0, keepdims=True)
    st_ln[tp, :, rows:2 * rows] = jnp.sum(h_t * h_t, axis=0, keepdims=True)

    def convert(slot, q):
        off, n = parts[q]
        e_out[slot, off:off + n, :] = e_oth[slot, off:off + n, :].astype(F32)

    total_load(e_own.at[0, pl.ds(0, 4 * small), :], ld_sem.at[0])
    for slot, q, sem in ((OPP, 2, 1), (LEFT, 1, 3), (RIGHT, 1, 3), (OWN, 2, 4)):
        load(slot, True, q, sem).start()
        if slot == OPP:
            load(slot, False, q, 2).start()
    for slot, q, sem in ((LEFT, 1, 5), (RIGHT, 1, 5), (OWN, 2, 6)):
        load(slot, False, q, sem).start()
    tok_copy.start()
    for slot in (RIGHT, LEFT):
        convert(slot, 0)
        off, n = piece(0 if slot == RIGHT else 1, 0)
        raw_src[off - tail0:off - tail0 + n, :] = e_own[slot, off:off + n, :].astype(F32)

    def raw_copy(slot, other):
        off, n = piece(0 if slot == RIGHT else 1, 0)
        src = e_out.at[slot, pl.ds(off, n), :] if other else raw_src.at[pl.ds(off - tail0, n), :]
        to = (right_chip if slot == RIGHT else left_chip) * 2 + (1 - core if other else core)
        return pltpu.make_async_remote_copy(
            src_ref=src, dst_ref=(raw_l if slot == RIGHT else raw_r).at[int(other)],
            send_sem=raw_send.at[0], recv_sem=raw_recv.at[int(slot == LEFT)],
            device_id={"tp": to}, device_id_type=MESH)

    pl.semaphore_wait(barrier, n_tp + 3)

    def tp_start(buf, stage):
        for j in range(1, n_tp):
            pltpu.make_async_remote_copy(
                src_ref=buf.at[tp], dst_ref=buf.at[tp], send_sem=t_send.at[stage], recv_sem=t_recv.at[stage],
                device_id={"tp": lax.rem(tp + j, n_tp)}, device_id_type=MESH).start()

    def tp_wait(buf, stage):
        total_recv(buf.at[pl.ds(0, n_tp - 1)], t_recv.at[stage])

    def tp_drain(buf, stage):
        total_send(buf.at[pl.ds(0, n_tp - 1)], t_send.at[stage])

    tp_start(st_ln, 0)
    for other in (False, True):
        for slot in (RIGHT, LEFT):
            raw_copy(slot, other).start()

    total_load(vec_ref, in_sem.at[2])
    hx[0, :, rows:rows + 128] = jnp.broadcast_to(vec_ref[0], (128, width)).T
    hx[0, :, rows + 128:rows + 256] = jnp.broadcast_to(vec_ref[1], (128, width)).T
    hx_copy = pltpu.make_async_remote_copy(
        src_ref=hx.at[0], dst_ref=hx.at[1], send_sem=hx_send.at[0], recv_sem=hx_recv.at[0],
        device_id=partner, device_id_type=MESH)
    hx_copy.start()
    for peer in y_near:
        pl.semaphore_signal(hop.at[0], inc=1, device_id=peer, device_id_type=MESH)

    def ex_copy(slot, q, sem):
        off, n = parts[q]
        return pltpu.make_async_remote_copy(
            src_ref=e_out.at[slot, pl.ds(off, n), :], dst_ref=e_in.at[slot, pl.ds(off, n), :],
            send_sem=ex_send.at[0], recv_sem=ex_recv.at[sem], device_id=partner, device_id_type=MESH)

    load(OPP, True, 2, 1).wait()
    for q in range(2):
        convert(OPP, q)
        ex_copy(OPP, q, q).start()
    for slot in (LEFT, RIGHT):
        ex_copy(slot, 0, 2).start()
    sides = e_oth.at[pl.ds(LEFT, 2), pl.ds(0, tail0), :]
    total_load(sides, ld_sem.at[3])
    for slot in (LEFT, RIGHT):
        convert(slot, 1)
        ex_copy(slot, 1, 3).start()
    load(OWN, True, 2, 4).wait()
    convert(OWN, 2)
    ex_copy(OWN, 2, 4).start()

    tp_wait(st_ln, 0)
    total = st_ln[0]
    for j in range(1, n_tp):
        total = total + st_ln[j]
    mean = total[:, 0:rows] / full_width
    rstd = lax.rsqrt(total[:, rows:2 * rows] / full_width - mean * mean + NORM_EPS)

    def norm(which):
        gain = hx[which, :, rows:rows + 128]
        bias = hx[which, :, rows + 128:rows + 256]
        for c in range(rows // 128):
            cols = slice(c * 128, c * 128 + 128)
            xn[which, :, cols] = ((hx[which, :, cols] - mean[:, cols]) * rstd[:, cols] * gain + bias).astype(BF16)

    def slab_copy(d):
        return pltpu.make_async_remote_copy(
            src_ref=slab_src, dst_ref=nb.at[d, pl.ds(pl.multiple_of(vp * xslab, 8), xslab), :],
            send_sem=sx_send.at[0], recv_sem=sx_recv.at[d], device_id=right if d == 0 else left, device_id_type=MESH)

    norm(0)
    slab_src[...] = xn[0, pl.ds(pl.multiple_of(vp * xslab, 8), xslab), :].astype(F32)
    for d in range(2):
        slab_copy(d).start()
    hx_copy.wait_recv()
    norm(1)

    def part_sum(slot, off, n):
        mine = e_own[slot, pl.ds(off, n), :]
        theirs = e_in[slot, pl.ds(off, n), :].astype(BF16)
        return (jnp.dot(mine, xn[0], preferred_element_type=F32)
                + jnp.dot(theirs, xn[1], preferred_element_type=F32))

    def f_copy(h, i):
        off, n = piece(h, i)
        return pltpu.make_async_remote_copy(
            src_ref=send_f.at[pl.ds(off, n), :], dst_ref=recv_f.at[pl.ds(off, n), :],
            send_sem=f_send.at[0], recv_sem=f_recv.at[i],
            device_id=left if h == 0 else right, device_id_type=MESH)

    def r_copy(h, i):
        off, n = piece(h, i)
        dst = (recv_r if h == 0 else recv_l).at[pl.ds(off, n), :]
        return pltpu.make_async_remote_copy(
            src_ref=recv_f.at[pl.ds(off, n), :], dst_ref=dst,
            send_sem=r_send.at[0], recv_sem=in_recv.at[i],
            device_id=left if h == 0 else right, device_id_type=MESH)

    def n_copy(h, i):
        off, n = piece(h, i)
        dst = (recv_l if h == 0 else recv_r).at[pl.ds(off, n), :]
        return pltpu.make_async_remote_copy(
            src_ref=send_n.at[pl.ds(off, n), :], dst_ref=dst,
            send_sem=n_send.at[0], recv_sem=in_recv.at[i],
            device_id=right if h == 0 else left, device_id_type=MESH)

    def far(i):
        for h in range(2):
            off, n = piece(h, i)
            send_f[pl.ds(off, n), :] = part_sum(OPP, off, n)
            f_copy(h, i).start()

    def near(i):
        for h in range(2):
            off, n = piece(h, i)
            send_n[pl.ds(off, n), :] = part_sum(RIGHT if h == 0 else LEFT, off, n)
            n_copy(h, i).start()

    def relay(i):
        mine = [part_sum(LEFT if h == 0 else RIGHT, *piece(h, i)) for h in range(2)]
        total_recv(recv_f.at[pl.ds(0, small if isinstance(i, int) else 2 * CHUNK), :], f_recv.at[i])
        for h in range(2):
            off, n = piece(h, i)
            recv_f[pl.ds(off, n), :] = recv_f[pl.ds(off, n), :] + mine[h]
            r_copy(h, i).start()

    def account(z):
        zr = z.reshape(z.shape[0] // 8, 8, rows)
        old = m_acc[...]
        new = jnp.maximum(old, jnp.max(zr, axis=0))
        m_acc[...] = new
        s_acc[...] = s_acc[...] * jnp.exp(old - new) + jnp.sum(jnp.exp(zr - new[None]), axis=0)

    def settle_raw():
        for h in range(2):
            off, n = piece(h, 0)
            raw = raw_l if h == 0 else raw_r
            if h == 0:
                total_recv(recv_l.at[pl.ds(0, small), :], in_recv.at[0])
            mine = part_sum(OWN, off, n)
            total_recv(raw, raw_recv.at[h])
            for other in range(2):
                mine = mine + jnp.dot(raw[other].astype(BF16), xnb[h, other], preferred_element_type=F32)
            z = mine + (recv_r if h == 0 else recv_l)[off:off + n, :]
            account(z)
            logits_ref[off:off + n, :] = z

    def settle(i):
        mine = [part_sum(OWN, *piece(h, i)) for h in range(2)]
        total_recv(recv_l.at[pl.ds(0, 4 * CHUNK), :], in_recv.at[i])
        for h in range(2):
            off, n = piece(h, i)
            z = mine[h] + recv_l[pl.ds(off, n), :] + recv_r[pl.ds(off, n), :]
            account(z)
            logits_ref[pl.ds(off, n), :] = z

    tok_copy.wait()
    tok = jnp.broadcast_to(tok_ref[...], (128, rows)).T

    def gather(step):
        for other in range(2):
            blk_chip = lax.rem(chip + jnp.where(step == 0, STEP_OF_SLOT[0], jnp.where(
                step == 1, STEP_OF_SLOT[1], jnp.where(step == 2, STEP_OF_SLOT[2], STEP_OF_SLOT[3]))), n_chip)
            blk = blk_chip * 2 + (1 - core if other else core)
            base = vp * (n_tp * n_block) + blk * n_block
            ref = e_oth if other else e_own
            acc = pick[...]
            for off in range(0, n_block, 512):
                n = min(512, n_block - off)
                for o, k in ((off, n // 128 * 128), (off + n // 128 * 128, n % 128)):
                    if k == 0:
                        continue
                    lane = lax.broadcasted_iota(jnp.int32, (rows, k), 1) + (base + o)
                    if k % 128 == 0:
                        want = jnp.concatenate([tok] * (k // 128), axis=1) if k > 128 else tok
                    else:
                        want = tok[:, :k]
                    hot = jnp.where(want == lane, 1.0, 0.0).astype(BF16)
                    acc = acc + jnp.dot(hot, ref[step, o:o + k, :], preferred_element_type=F32)
            pick[...] = acc

    def v_copy(src, dst, stage, j):
        return pltpu.make_async_remote_copy(
            src_ref=src, dst_ref=dst, send_sem=v_send.at[stage], recv_sem=v_recv.at[stage],
            device_id={"vp": lax.rem(vp + j, n_vp)}, device_id_type=MESH)

    def vp_start(buf, stage):
        for j in range(1, n_vp):
            v_copy(buf.at[vp], buf.at[vp], stage, j).start()

    def vp_wait(buf, stage):
        total_recv(buf.at[pl.ds(0, n_vp - 1)], v_recv.at[stage])

    def vp_drain(buf, stage):
        total_send(buf.at[pl.ds(0, n_vp - 1)], v_send.at[stage])

    def slabs_forward():
        own = pl.ds(pl.multiple_of(vp * xslab, 8), xslab)
        for d in range(2):
            slab_copy(d).wait_recv()
            for j in range(1, n_vp):
                v_copy(nb.at[d, own, :], nb.at[d, own, :], 3, j).start()

    nb_copy = pltpu.make_async_remote_copy(
        src_ref=nb, dst_ref=nb_par, send_sem=nb_send.at[0], recv_sem=nb_recv.at[0], device_id=partner, device_id_type=MESH)
    nb_rest = nb.at[:, pl.ds(0, width - xslab), :]

    def slabs_swap():
        total_recv(nb_rest, v_recv.at[3])
        nb_copy.start()
        for d in range(2):
            xnb[d, 0] = nb[d].astype(BF16)

    def slabs_done():
        nb_copy.wait_recv()
        for d in range(2):
            xnb[d, 1] = nb_par[d].astype(BF16)

    def rows_scatter():
        for j in range(1, n_vp):
            peer = lax.rem(vp + j, n_vp)
            v_copy(pick.at[pl.ds(pl.multiple_of(peer * slab, 8), slab), :], rs_buf.at[vp], 0, j).start()
        rs_buf[vp] = pick[pl.ds(pl.multiple_of(vp * slab, 8), slab), :]

    def rows_stats():
        vp_wait(rs_buf, 0)
        tot = rs_buf[0]
        for j in range(1, n_vp):
            tot = tot + rs_buf[j]
        ag_buf[vp] = tot
        lane = lax.broadcasted_iota(jnp.int32, (slab, 128), 1)
        both = jnp.where(lane == 0, jnp.sum(tot, axis=1, keepdims=True), jnp.sum(tot * tot, axis=1, keepdims=True)).T
        row_st[tp] = jnp.zeros((1, 256), F32)
        row_st[tp, :, 0:slab] = both[0:1]
        row_st[tp, :, 128:128 + slab] = both[1:2]
        tp_start(row_st, 1)

    def rows_norm():
        tp_wait(row_st, 1)
        tot = row_st[0]
        for j in range(1, n_tp):
            tot = tot + row_st[j]
        mu = tot[:, 0:128] / full_width
        rs = lax.rsqrt(tot[:, 128:256] / full_width - mu * mu + NORM_EPS)
        mu = jnp.broadcast_to(mu, (128, 128)).T[0:slab, 0:1]
        rs = jnp.broadcast_to(rs, (128, 128)).T[0:slab, 0:1]
        out = ((ag_buf[vp] - mu) * rs * vec_ref[2] + vec_ref[3]).astype(BF16)
        ag_buf[vp] = out.astype(F32)
        vp_start(ag_buf, 1)

    def rows_out():
        vp_wait(ag_buf, 1)
        for j in range(n_vp):
            next_ref[j * slab:(j + 1) * slab, :] = ag_buf[j].astype(BF16)

    pick[...] = jnp.zeros_like(pick)
    m_acc[...] = jnp.full_like(m_acc, -jnp.inf)
    s_acc[...] = jnp.zeros_like(s_acc)

    load(OPP, False, 2, 2).wait()
    for q in range(2):
        ex_copy(OPP, q, q).wait_recv()
        far(q)
        pl.semaphore_wait(hop.at[q], 2)
        for peer in (z_near, y_near)[q]:
            pl.semaphore_signal(hop.at[q + 1], inc=1, device_id=peer, device_id_type=MESH)
    total_recv(e_in.at[pl.ds(LEFT, 2), pl.ds(tail0, small), :], ex_recv.at[2])
    far(2)
    relay(0)
    pl.semaphore_wait(hop.at[2], 2)
    total_load(sides, ld_sem.at[5])
    total_recv(e_in.at[pl.ds(LEFT, 2), pl.ds(0, tail0), :], ex_recv.at[3])
    load(OWN, False, 2, 6).wait()
    ex_copy(OWN, 2, 4).wait_recv()

    def at(i, when, *steps):
        @pl.when(i == when)
        def _():
            for step in steps:
                step()

    def round_body(i, carry):
        near(i)

        @pl.when(i + 2 < n_round)
        def _():
            far(i + 2)

        relay(i)
        at(i, 1, slabs_forward)

        @pl.when(i <= 2)
        def _():
            gather(2 * i - 2)
            gather(2 * i - 1)

        at(i, 2, slabs_swap)
        at(i, 3, rows_scatter, slabs_done)
        at(i, 4, rows_stats, settle_raw)
        at(i, 6, rows_norm)

        @pl.when(i >= 3)
        def _():
            settle(i - 2)

        return carry

    lax.fori_loop(1, n_round, round_body, 0)

    def last_body(i, carry):
        settle(i)
        return carry

    lax.fori_loop(n_round - 2, n_round, last_body, 0)

    def merge(buf, n):
        top = buf[0]
        for j in range(1, n):
            top = jnp.maximum(top, buf[j])
        tot = jnp.exp(buf[0] - top)
        for j in range(1, n):
            tot = tot + jnp.exp(buf[j] - top)
        return top + jnp.log(tot)

    m8 = m_acc[...]
    top = jnp.max(m8, axis=0, keepdims=True)
    mine = vp * 2 + core
    st_all[mine] = top + jnp.log(jnp.sum(s_acc[...] * jnp.exp(m8 - top), axis=0, keepdims=True))

    def collect(peer):
        return pltpu.make_async_remote_copy(
            src_ref=st_all.at[mine], dst_ref=st_all.at[mine], send_sem=v_send.at[2], recv_sem=v_recv.at[2],
            device_id={"vp": peer, "tp": chip * 2 + 1}, device_id_type=MESH)

    for j in range(1, n_vp):
        collect(lax.rem(vp + j, n_vp)).start()

    @pl.when(core == 0)
    def _():
        collect(vp).start()

    rows_out()
    hx_copy.wait_send()
    nb_copy.wait_send()
    total_send(e_out, ex_send.at[0])
    total_send(e_in.at[0, pl.ds(0, 2 * small), :], raw_send.at[0])
    total_send(nb.at[0, pl.ds(0, 2 * xslab), :], sx_send.at[0])
    total_send(send_f, f_send.at[0])
    total_send(recv_f, r_send.at[0])
    total_send(send_n.at[pl.ds(0, tail0), :], n_send.at[0])
    tp_drain(st_ln, 0)
    tp_drain(row_st, 1)
    vp_drain(rs_buf, 0)
    vp_drain(ag_buf, 1)
    total_send(nb_rest, v_send.at[3])

    @pl.when(core == 1)
    def _():
        total_recv(st_all.at[pl.ds(0, 2 * n_vp - 1)], v_recv.at[2])
        st_lse[chip] = merge(st_all, 2 * n_vp)
        for peer in [lax.rem(tp + j, n_tp) for j in range(1, n_tp)]:
            pltpu.make_async_remote_copy(
                src_ref=st_lse.at[chip], dst_ref=st_lse.at[chip], send_sem=t_send.at[2], recv_sem=t_recv.at[2],
                device_id={"tp": peer}, device_id_type=MESH).start()
        total_send(st_all.at[pl.ds(0, n_vp - 1)], v_send.at[2])
        total_recv(st_lse.at[pl.ds(0, n_chip - 1)], t_recv.at[2])
        total_send(st_all.at[pl.ds(0, n_tp - 1)], t_send.at[2])

    @pl.when(core == 0)
    def _():
        total_send(st_all.at[pl.ds(0, n_vp)], v_send.at[2])
        total_recv(st_lse, t_recv.at[2])

    lse_ref[...] = merge(st_lse, n_chip)


def finish_kernel(n_piece, z_ref, lse_ref, next_ref, out_ref, sum_ref, row_ref, buf, sems):
    lse = lse_ref[...]
    n = z_ref.shape[0] // n_piece

    def put(j):
        part = pl.ds(j * n, n)
        return pltpu.make_async_copy(buf.at[part, :], out_ref.at[part, :], sems.at[j])

    small = [pltpu.make_async_copy(lse_ref, sum_ref, sems.at[n_piece]),
             pltpu.make_async_copy(next_ref, row_ref, sems.at[n_piece + 1])]
    for copy in small:
        copy.start()
    for j in range(n_piece):
        buf[j * n:(j + 1) * n, :] = z_ref[j * n:(j + 1) * n, :] - lse
        put(j).start()
    for copy in small:
        copy.wait()
    for j in range(n_piece):
        put(j).wait()


def solution(mesh):
    n_vp, n_tp = mesh.shape["vp"], mesh.shape["tp"]

    def per_device(hidden, lnf_gain, lnf_bias, emb_table, next_tok, eln_gain, eln_bias):
        rows, width = hidden.shape
        n_block = emb_table.shape[0] // n_tp
        slab = rows // n_vp
        n_round = n_block // 2 // CHUNK + 1
        small = n_block - 2 * (n_round - 1) * CHUNK
        dma = pltpu.SemaphoreType.DMA
        vmem = pl.BlockSpec(memory_space=pltpu.VMEM)
        logits, lse, next_in = pl.pallas_call(
            functools.partial(head_kernel, n_vp, n_tp, n_block, width * n_tp),
            out_shape=(
                pltpu.VMEM((n_block, rows), F32),
                pltpu.VMEM((1, rows), F32),
                pltpu.VMEM((rows, width), BF16),
            ),
            in_specs=[pl.BlockSpec(memory_space=pl.ANY)] * 7,
            out_specs=(vmem, vmem, vmem),
            scratch_shapes=[
                pltpu.VMEM((4, n_block, width), BF16),
                pltpu.VMEM((4, n_block, width), BF16),
                pltpu.VMEM((4, n_block, width), F32),
                pltpu.VMEM((4, n_block, width), F32),
                pltpu.VMEM((n_block, rows), F32),
                pltpu.VMEM((n_block, rows), F32),
                pltpu.VMEM((n_block, rows), F32),
                pltpu.VMEM((n_block, rows), F32),
                pltpu.VMEM((n_block, rows), F32),
                pltpu.VMEM((2, width, rows + 256), F32),
                pltpu.VMEM((2, width, rows), BF16),
                pltpu.VMEM((8, rows), F32),
                pltpu.VMEM((8, rows), F32),
                pltpu.VMEM((rows, width), F32),
                pltpu.VMEM((n_tp, 1, 2 * rows), F32),
                pltpu.VMEM((n_tp // 2, 1, rows), F32),
                pltpu.VMEM((2 * n_vp, 1, rows), F32),
                pltpu.VMEM((n_vp, slab, width), F32),
                pltpu.VMEM((n_tp, 1, 256), F32),
                pltpu.VMEM((n_vp, slab, width), F32),
                pltpu.VMEM((small, width), F32),
                pltpu.VMEM((2, small // 16 * 8, width), F32),
                pltpu.VMEM((2, small - small // 16 * 8, width), F32),
                pltpu.VMEM((width // n_vp, rows), F32),
                pltpu.VMEM((2, width, rows), F32),
                pltpu.VMEM((2, width, rows), F32),
                pltpu.VMEM((2, 2, width, rows), BF16),
                dma((7,)), dma((1,)), dma((5,)), dma((1,)), dma((1,)),
                dma((1,)), dma((n_round,)), dma((1,)), dma((1,)), dma((n_round,)),
                dma((3,)), dma((3,)), dma((4,)), dma((4,)), dma((1,)), dma((2,)), dma((1,)), dma((2,)), dma((1,)), dma((1,)),
                pltpu.SemaphoreType.REGULAR((3,)),
                pltpu.VMEM((rows, width), BF16),
                pltpu.VMEM((1, rows), jnp.int32),
                pltpu.VMEM((4, 1, width), F32),
                dma((3,)),
            ],
            compiler_params=pltpu.CompilerParams(
                collective_id=0, has_side_effects=True, vmem_limit_bytes=57 * 1024 * 1024),
            cost_estimate=pl.CostEstimate(
                flops=4 * rows * n_block * n_tp * width, bytes_accessed=16 * n_block * n_tp * width, transcendentals=rows * n_block),
        )(hidden, lnf_gain[None, :], lnf_bias[None, :], emb_table, next_tok[None, :], eln_gain[None, :], eln_bias[None, :])
        n_piece = 5
        logprobs_t, log_sum, next_bf = pl.pallas_call(
            functools.partial(finish_kernel, n_piece),
            out_shape=(
                jax.ShapeDtypeStruct((n_block, rows), F32),
                jax.ShapeDtypeStruct((1, rows), F32),
                jax.ShapeDtypeStruct((rows, width), BF16),
            ),
            in_specs=[vmem, vmem, vmem],
            out_specs=(pl.BlockSpec(memory_space=pl.ANY),) * 3,
            scratch_shapes=[pltpu.VMEM((n_block, rows), F32), dma((n_piece + 2,))],
            compiler_params=pltpu.CompilerParams(vmem_limit_bytes=16 * 1024 * 1024),
        )(logits, lse, next_in)
        return logprobs_t.T, log_sum[0], next_bf

    return jax.shard_map(
        per_device,
        mesh=mesh,
        in_specs=(P("dp", "tp"), P("tp"), P("tp"), P("vp", "tp"), P("dp"), P("tp"), P("tp")),
        out_specs=(P("dp", ("vp", "tp")), P("dp"), P("dp", "tp")),
        check_vma=False,
    )
```

```python
import functools

import jax
import jax.numpy as jnp
from jax import lax
from jax.experimental import pallas as pl
from jax.experimental.pallas import tpu as pltpu
from jax.sharding import PartitionSpec as P

NORM_EPS = 1e-5
MESH = pl.DeviceIdType.MESH
CHUNK = 128
F32 = jnp.float32
BF16 = jnp.bfloat16

OPP, LEFT, RIGHT, OWN = 0, 1, 2, 3
SIDE = 4
N_HOP = 5
STEP_OF_SLOT = (2, 3, 1, 0)


def head_kernel(n_vp, n_tp, n_block, full_width,
                hid_hbm, g_hbm, b_hbm, emb_ref, tok_hbm, eg_hbm, eb_hbm,
                logits_ref, lse_ref, next_ref,
                e_own, e_oth, e_out, e_in, send_f, recv_f, send_n, recv_l, recv_r,
                hx, xn, m_acc, s_acc, pick, st_ln, st_lse, st_all, rs_buf, row_st, ag_buf,
                raw_src, raw_l, raw_r, slab_src, nb, nb_par, xnb,
                ld_sem, ex_send, ex_recv, hx_send, hx_recv,
                f_send, f_recv, n_send, r_send, in_recv,
                t_send, t_recv, v_send, v_recv, raw_send, raw_recv, sx_send, sx_recv, nb_send, nb_recv, hop,
                hid_ref, tok_ref, vec_ref, in_sem):
    vp = lax.axis_index("vp")
    tp = lax.axis_index("tp")
    core = lax.rem(tp, 2)
    chip = tp // 2
    n_chip = n_tp // 2
    rows, width = hid_hbm.shape
    slab = rows // n_vp
    xslab = width // (n_vp // 2)
    left_chip = lax.rem(chip + n_chip - 1, n_chip)
    right_chip = lax.rem(chip + 1, n_chip)
    left = {"tp": left_chip * 2 + core}
    right = {"tp": right_chip * 2 + core}
    partner = {"tp": chip * 2 + 1 - core}
    y = lax.rem(vp, SIDE)
    z = vp // SIDE
    n_z = n_vp // SIDE
    near_by = ((y > 0, {"vp": lax.rem(vp + n_vp - 1, n_vp)}), (y < SIDE - 1, {"vp": lax.rem(vp + 1, n_vp)}),
               (z > 0, {"vp": lax.rem(vp + n_vp - SIDE, n_vp)}), (z < n_z - 1, {"vp": lax.rem(vp + SIDE, n_vp)}))
    n_near = sum(jnp.where(there, 1, 0) for there, _ in near_by)

    def tell_near(sem):
        for there, peer in near_by:
            @pl.when(there)
            def _(peer=peer):
                pl.semaphore_signal(sem, inc=1, device_id=peer, device_id_type=MESH)

    def hear_near(step):
        pl.semaphore_wait(hop.at[step], n_near)
        if step + 1 < N_HOP:
            tell_near(hop.at[step + 1])

    n_carry = n_vp // 2
    carries = vp < n_carry
    half = (n_block // 2) // CHUNK
    n_round = half + 1
    small = n_block - 2 * half * CHUNK
    small1 = (small // 16) * 8
    small2 = small - small1
    tail0 = 2 * half * CHUNK

    def piece(h, i):
        if isinstance(i, int) and i == 0:
            return (tail0, small1) if h == 0 else (tail0 + small1, small2)
        off = h * half * CHUNK + (i - 1) * CHUNK
        return (off if isinstance(i, int) else pl.multiple_of(off, CHUNK)), CHUNK

    barrier = pltpu.get_barrier_semaphore()
    for j in range(1, n_tp):
        pl.semaphore_signal(barrier, inc=1, device_id={"tp": lax.rem(tp + j, n_tp)}, device_id_type=MESH)
    tell_near(barrier)

    parts = ((tail0, small), (0, tail0), (0, n_block))

    def load(slot, other, q, sem):
        blk = lax.rem(chip + STEP_OF_SLOT[slot], n_chip) * 2 + (1 - core if other else core)
        off, n = parts[q]
        src = emb_ref.at[pl.ds(pl.multiple_of(blk * n_block + off, 8), n), :]
        dst = (e_oth if other else e_own).at[slot, pl.ds(off, n), :]
        return pltpu.make_async_copy(src, dst, ld_sem.at[sem])

    hid_copy = pltpu.make_async_copy(hid_hbm, hid_ref, in_sem.at[0])
    tok_copy = pltpu.make_async_copy(tok_hbm, tok_ref, in_sem.at[1])
    hid_copy.start()
    for k, src in enumerate((g_hbm, b_hbm, eg_hbm, eb_hbm)):
        pltpu.make_async_copy(src, vec_ref.at[k], in_sem.at[2]).start()
    for slot in (RIGHT, LEFT):
        load(slot, True, 0, 0).start()
        load(slot, False, 0, 0).start()

    def total_load(ref, sem):
        pltpu.make_async_copy(ref, ref, sem).wait()

    def total_recv(ref, sem):
        pltpu.make_async_remote_copy(src_ref=ref, dst_ref=ref, send_sem=sem, recv_sem=sem,
                                     device_id=partner, device_id_type=MESH).wait_recv()

    def total_send(ref, sem):
        pltpu.make_async_remote_copy(src_ref=ref, dst_ref=ref, send_sem=sem, recv_sem=sem,
                                     device_id=partner, device_id_type=MESH).wait_send()

    hid_copy.wait()
    h_t = hid_ref[...].astype(F32).T
    hx[0, :, 0:rows] = h_t
    st_ln[tp, :, 0:rows] = jnp.sum(h_t, axis=0, keepdims=True)
    st_ln[tp, :, rows:2 * rows] = jnp.sum(h_t * h_t, axis=0, keepdims=True)

    def convert(slot, q):
        off, n = parts[q]
        e_out[slot, off:off + n, :] = e_oth[slot, off:off + n, :].astype(F32)

    total_load(e_own.at[0, pl.ds(0, 4 * small), :], ld_sem.at[0])
    for slot, q, sem in ((OPP, 2, 1), (LEFT, 1, 3), (RIGHT, 1, 3), (OWN, 2, 4)):
        load(slot, True, q, sem).start()
        if slot == OPP:
            load(slot, False, q, 2).start()
    for slot, q, sem in ((LEFT, 1, 5), (RIGHT, 1, 5), (OWN, 2, 6)):
        load(slot, False, q, sem).start()
    tok_copy.start()
    for slot in (RIGHT, LEFT):
        convert(slot, 0)
        off, n = piece(0 if slot == RIGHT else 1, 0)
        raw_src[off - tail0:off - tail0 + n, :] = e_own[slot, off:off + n, :].astype(F32)

    def raw_copy(slot, other):
        off, n = piece(0 if slot == RIGHT else 1, 0)
        src = e_out.at[slot, pl.ds(off, n), :] if other else raw_src.at[pl.ds(off - tail0, n), :]
        to = (right_chip if slot == RIGHT else left_chip) * 2 + (1 - core if other else core)
        return pltpu.make_async_remote_copy(
            src_ref=src, dst_ref=(raw_l if slot == RIGHT else raw_r).at[int(other)],
            send_sem=raw_send.at[0], recv_sem=raw_recv.at[int(slot == LEFT)],
            device_id={"tp": to}, device_id_type=MESH)

    pl.semaphore_wait(barrier, n_tp - 1 + n_near)

    def tp_start(buf, stage):
        for j in range(1, n_tp):
            pltpu.make_async_remote_copy(
                src_ref=buf.at[tp], dst_ref=buf.at[tp], send_sem=t_send.at[stage], recv_sem=t_recv.at[stage],
                device_id={"tp": lax.rem(tp + j, n_tp)}, device_id_type=MESH).start()

    def tp_wait(buf, stage):
        total_recv(buf.at[pl.ds(0, n_tp - 1)], t_recv.at[stage])

    def tp_drain(buf, stage):
        total_send(buf.at[pl.ds(0, n_tp - 1)], t_send.at[stage])

    tp_start(st_ln, 0)
    for other in (False, True):
        for slot in (RIGHT, LEFT):
            raw_copy(slot, other).start()

    total_load(vec_ref, in_sem.at[2])
    hx[0, :, rows:rows + 128] = jnp.broadcast_to(vec_ref[0], (128, width)).T
    hx[0, :, rows + 128:rows + 256] = jnp.broadcast_to(vec_ref[1], (128, width)).T
    hx_copy = pltpu.make_async_remote_copy(
        src_ref=hx.at[0], dst_ref=hx.at[1], send_sem=hx_send.at[0], recv_sem=hx_recv.at[0],
        device_id=partner, device_id_type=MESH)
    hx_copy.start()
    tell_near(hop.at[0])

    def ex_copy(slot, q, sem):
        off, n = parts[q]
        return pltpu.make_async_remote_copy(
            src_ref=e_out.at[slot, pl.ds(off, n), :], dst_ref=e_in.at[slot, pl.ds(off, n), :],
            send_sem=ex_send.at[0], recv_sem=ex_recv.at[sem], device_id=partner, device_id_type=MESH)

    load(OPP, True, 2, 1).wait()
    for q in range(2):
        convert(OPP, q)
        ex_copy(OPP, q, q).start()
    for slot in (LEFT, RIGHT):
        ex_copy(slot, 0, 2).start()
    sides = e_oth.at[pl.ds(LEFT, 2), pl.ds(0, tail0), :]
    total_load(sides, ld_sem.at[3])
    for slot in (LEFT, RIGHT):
        convert(slot, 1)
        ex_copy(slot, 1, 3).start()
    load(OWN, True, 2, 4).wait()
    convert(OWN, 2)
    ex_copy(OWN, 2, 4).start()

    tp_wait(st_ln, 0)
    total = st_ln[0]
    for j in range(1, n_tp):
        total = total + st_ln[j]
    mean = total[:, 0:rows] / full_width
    rstd = lax.rsqrt(total[:, rows:2 * rows] / full_width - mean * mean + NORM_EPS)

    def norm(which):
        gain = hx[which, :, rows:rows + 128]
        bias = hx[which, :, rows + 128:rows + 256]
        for c in range(rows // 128):
            cols = slice(c * 128, c * 128 + 128)
            xn[which, :, cols] = ((hx[which, :, cols] - mean[:, cols]) * rstd[:, cols] * gain + bias).astype(BF16)

    def slab_copy(d):
        return pltpu.make_async_remote_copy(
            src_ref=slab_src, dst_ref=nb.at[d, pl.ds(pl.multiple_of(vp * xslab, 8), xslab), :],
            send_sem=sx_send.at[0], recv_sem=sx_recv.at[d], device_id=right if d == 0 else left, device_id_type=MESH)

    norm(0)

    @pl.when(carries)
    def _():
        slab_src[...] = xn[0, pl.ds(pl.multiple_of(vp * xslab, 32), xslab), :].astype(F32)
        for d in range(2):
            slab_copy(d).start()

    hx_copy.wait_recv()
    norm(1)

    def part_sum(slot, off, n):
        mine = e_own[slot, pl.ds(off, n), :]
        theirs = e_in[slot, pl.ds(off, n), :].astype(BF16)
        return (jnp.dot(mine, xn[0], preferred_element_type=F32)
                + jnp.dot(theirs, xn[1], preferred_element_type=F32))

    def f_copy(h, i):
        off, n = piece(h, i)
        return pltpu.make_async_remote_copy(
            src_ref=send_f.at[pl.ds(off, n), :], dst_ref=recv_f.at[pl.ds(off, n), :],
            send_sem=f_send.at[0], recv_sem=f_recv.at[i],
            device_id=left if h == 0 else right, device_id_type=MESH)

    def r_copy(h, i):
        off, n = piece(h, i)
        dst = (recv_r if h == 0 else recv_l).at[pl.ds(off, n), :]
        return pltpu.make_async_remote_copy(
            src_ref=recv_f.at[pl.ds(off, n), :], dst_ref=dst,
            send_sem=r_send.at[0], recv_sem=in_recv.at[i],
            device_id=left if h == 0 else right, device_id_type=MESH)

    def n_copy(h, i):
        off, n = piece(h, i)
        dst = (recv_l if h == 0 else recv_r).at[pl.ds(off, n), :]
        return pltpu.make_async_remote_copy(
            src_ref=send_n.at[pl.ds(off, n), :], dst_ref=dst,
            send_sem=n_send.at[0], recv_sem=in_recv.at[i],
            device_id=right if h == 0 else left, device_id_type=MESH)

    def far(i):
        for h in range(2):
            off, n = piece(h, i)
            send_f[pl.ds(off, n), :] = part_sum(OPP, off, n)
            f_copy(h, i).start()

    def near(i):
        for h in range(2):
            off, n = piece(h, i)
            send_n[pl.ds(off, n), :] = part_sum(RIGHT if h == 0 else LEFT, off, n)
            n_copy(h, i).start()

    def relay(i):
        mine = [part_sum(LEFT if h == 0 else RIGHT, *piece(h, i)) for h in range(2)]
        total_recv(recv_f.at[pl.ds(0, small if isinstance(i, int) else 2 * CHUNK), :], f_recv.at[i])
        for h in range(2):
            off, n = piece(h, i)
            recv_f[pl.ds(off, n), :] = recv_f[pl.ds(off, n), :] + mine[h]
            r_copy(h, i).start()

    def account(z):
        zr = z.reshape(z.shape[0] // 8, 8, rows)
        old = m_acc[...]
        new = jnp.maximum(old, jnp.max(zr, axis=0))
        m_acc[...] = new
        s_acc[...] = s_acc[...] * jnp.exp(old - new) + jnp.sum(jnp.exp(zr - new[None]), axis=0)

    def settle_raw():
        for h in range(2):
            off, n = piece(h, 0)
            raw = raw_l if h == 0 else raw_r
            if h == 0:
                total_recv(recv_l.at[pl.ds(0, small), :], in_recv.at[0])
            mine = part_sum(OWN, off, n)
            total_recv(raw, raw_recv.at[h])
            for other in range(2):
                mine = mine + jnp.dot(raw[other].astype(BF16), xnb[h, other], preferred_element_type=F32)
            z = mine + (recv_r if h == 0 else recv_l)[off:off + n, :]
            account(z)
            logits_ref[off:off + n, :] = z

    def settle(i):
        mine = [part_sum(OWN, *piece(h, i)) for h in range(2)]
        total_recv(recv_l.at[pl.ds(0, 4 * CHUNK), :], in_recv.at[i])
        for h in range(2):
            off, n = piece(h, i)
            z = mine[h] + recv_l[pl.ds(off, n), :] + recv_r[pl.ds(off, n), :]
            account(z)
            logits_ref[pl.ds(off, n), :] = z

    tok_copy.wait()
    tok = jnp.broadcast_to(tok_ref[...], (128, rows)).T

    def gather(step):
        for other in range(2):
            blk_chip = lax.rem(chip + jnp.where(step == 0, STEP_OF_SLOT[0], jnp.where(
                step == 1, STEP_OF_SLOT[1], jnp.where(step == 2, STEP_OF_SLOT[2], STEP_OF_SLOT[3]))), n_chip)
            blk = blk_chip * 2 + (1 - core if other else core)
            base = vp * (n_tp * n_block) + blk * n_block
            ref = e_oth if other else e_own
            acc = pick[...]
            for off in range(0, n_block, 512):
                n = min(512, n_block - off)
                for o, k in ((off, n // 128 * 128), (off + n // 128 * 128, n % 128)):
                    if k == 0:
                        continue
                    lane = lax.broadcasted_iota(jnp.int32, (rows, k), 1) + (base + o)
                    if k % 128 == 0:
                        want = jnp.concatenate([tok] * (k // 128), axis=1) if k > 128 else tok
                    else:
                        want = tok[:, :k]
                    hot = jnp.where(want == lane, 1.0, 0.0).astype(BF16)
                    acc = acc + jnp.dot(hot, ref[step, o:o + k, :], preferred_element_type=F32)
            pick[...] = acc

    def v_copy(src, dst, stage, j):
        return pltpu.make_async_remote_copy(
            src_ref=src, dst_ref=dst, send_sem=v_send.at[stage], recv_sem=v_recv.at[stage],
            device_id={"vp": lax.rem(vp + j, n_vp)}, device_id_type=MESH)

    def vp_start(buf, stage):
        for j in range(1, n_vp):
            v_copy(buf.at[vp], buf.at[vp], stage, j).start()

    def vp_wait(buf, stage):
        total_recv(buf.at[pl.ds(0, n_vp - 1)], v_recv.at[stage])

    def vp_drain(buf, stage):
        total_send(buf.at[pl.ds(0, n_vp - 1)], v_send.at[stage])

    def slabs_forward():
        hear_near(N_HOP - 1)

        @pl.when(carries)
        def _():
            own = pl.ds(pl.multiple_of(vp * xslab, 8), xslab)
            for d in range(2):
                slab_copy(d).wait_recv()
                for j in range(1, n_vp):
                    v_copy(nb.at[d, own, :], nb.at[d, own, :], 3, j).start()

    nb_copy = pltpu.make_async_remote_copy(
        src_ref=nb, dst_ref=nb_par, send_sem=nb_send.at[0], recv_sem=nb_recv.at[0], device_id=partner, device_id_type=MESH)

    def slabs_swap():
        @pl.when(carries)
        def _():
            total_recv(nb.at[:, pl.ds(0, width - xslab), :], v_recv.at[3])

        @pl.when(jnp.logical_not(carries))
        def _():
            total_recv(nb, v_recv.at[3])

        nb_copy.start()
        for d in range(2):
            xnb[d, 0] = nb[d].astype(BF16)

    def slabs_done():
        nb_copy.wait_recv()
        for d in range(2):
            xnb[d, 1] = nb_par[d].astype(BF16)

    def rows_scatter():
        for j in range(1, n_vp):
            peer = lax.rem(vp + j, n_vp)
            v_copy(pick.at[pl.ds(pl.multiple_of(peer * slab, 8), slab), :], rs_buf.at[vp], 0, j).start()
        rs_buf[vp] = pick[pl.ds(pl.multiple_of(vp * slab, 8), slab), :]

    def rows_stats():
        vp_wait(rs_buf, 0)
        tot = rs_buf[0]
        for j in range(1, n_vp):
            tot = tot + rs_buf[j]
        ag_buf[vp] = tot
        lane = lax.broadcasted_iota(jnp.int32, (slab, 128), 1)
        both = jnp.where(lane == 0, jnp.sum(tot, axis=1, keepdims=True), jnp.sum(tot * tot, axis=1, keepdims=True)).T
        row_st[tp] = jnp.zeros((1, 256), F32)
        row_st[tp, :, 0:slab] = both[0:1]
        row_st[tp, :, 128:128 + slab] = both[1:2]
        tp_start(row_st, 1)

    def rows_norm():
        tp_wait(row_st, 1)
        tot = row_st[0]
        for j in range(1, n_tp):
            tot = tot + row_st[j]
        mu = tot[:, 0:128] / full_width
        rs = lax.rsqrt(tot[:, 128:256] / full_width - mu * mu + NORM_EPS)
        mu = jnp.broadcast_to(mu, (128, 128)).T[0:slab, 0:1]
        rs = jnp.broadcast_to(rs, (128, 128)).T[0:slab, 0:1]
        out = ((ag_buf[vp] - mu) * rs * vec_ref[2] + vec_ref[3]).astype(BF16)
        ag_buf[vp] = out.astype(F32)
        vp_start(ag_buf, 1)

    def rows_out():
        vp_wait(ag_buf, 1)
        for j in range(n_vp):
            next_ref[j * slab:(j + 1) * slab, :] = ag_buf[j].astype(BF16)

    pick[...] = jnp.zeros_like(pick)
    m_acc[...] = jnp.full_like(m_acc, -jnp.inf)
    s_acc[...] = jnp.zeros_like(s_acc)

    load(OPP, False, 2, 2).wait()
    for q in range(2):
        ex_copy(OPP, q, q).wait_recv()
        far(q)
        hear_near(q)
    total_recv(e_in.at[pl.ds(LEFT, 2), pl.ds(tail0, small), :], ex_recv.at[2])
    far(2)
    hear_near(2)
    relay(0)
    hear_near(3)
    total_load(sides, ld_sem.at[5])
    total_recv(e_in.at[pl.ds(LEFT, 2), pl.ds(0, tail0), :], ex_recv.at[3])
    load(OWN, False, 2, 6).wait()
    ex_copy(OWN, 2, 4).wait_recv()

    def at(i, when, *steps):
        @pl.when(i == when)
        def _():
            for step in steps:
                step()

    def round_body(i, carry):
        near(i)

        @pl.when(i + 2 < n_round)
        def _():
            far(i + 2)

        relay(i)
        at(i, 1, slabs_forward)

        @pl.when(i <= 2)
        def _():
            gather(2 * i - 2)
            gather(2 * i - 1)

        at(i, 2, slabs_swap)
        at(i, 3, rows_scatter, slabs_done)
        at(i, 4, rows_stats, settle_raw)
        at(i, 6, rows_norm)

        @pl.when(i >= 3)
        def _():
            settle(i - 2)

        return carry

    lax.fori_loop(1, n_round, round_body, 0)

    def last_body(i, carry):
        settle(i)
        return carry

    lax.fori_loop(n_round - 2, n_round, last_body, 0)

    def merge(buf, n):
        top = buf[0]
        for j in range(1, n):
            top = jnp.maximum(top, buf[j])
        tot = jnp.exp(buf[0] - top)
        for j in range(1, n):
            tot = tot + jnp.exp(buf[j] - top)
        return top + jnp.log(tot)

    m8 = m_acc[...]
    top = jnp.max(m8, axis=0, keepdims=True)
    mine = vp * 2 + core
    st_all[mine] = top + jnp.log(jnp.sum(s_acc[...] * jnp.exp(m8 - top), axis=0, keepdims=True))

    def collect(peer):
        return pltpu.make_async_remote_copy(
            src_ref=st_all.at[mine], dst_ref=st_all.at[mine], send_sem=v_send.at[2], recv_sem=v_recv.at[2],
            device_id={"vp": peer, "tp": chip * 2 + 1}, device_id_type=MESH)

    shifts = sorted(((dz, dy) for dz in range(n_z) for dy in range(SIDE) if dz or dy),
                    key=lambda d: -min(d[0], n_z - d[0]) - min(d[1], SIDE - d[1]))
    for dz, dy in shifts:
        collect(lax.rem(z + dz, n_z) * SIDE + lax.rem(y + dy, SIDE)).start()

    @pl.when(core == 0)
    def _():
        collect(vp).start()

    rows_out()
    hx_copy.wait_send()
    nb_copy.wait_send()
    total_send(e_out, ex_send.at[0])
    total_send(e_in.at[0, pl.ds(0, 2 * small), :], raw_send.at[0])

    @pl.when(carries)
    def _():
        total_send(nb.at[0, pl.ds(0, 2 * xslab), :], sx_send.at[0])
        total_send(send_f.at[pl.ds(0, 2 * (n_vp - 1) * xslab), :], v_send.at[3])

    total_send(send_f, f_send.at[0])
    total_send(recv_f, r_send.at[0])
    total_send(send_n.at[pl.ds(0, tail0), :], n_send.at[0])
    tp_drain(st_ln, 0)
    tp_drain(row_st, 1)
    vp_drain(rs_buf, 0)
    vp_drain(ag_buf, 1)

    @pl.when(core == 1)
    def _():
        total_recv(st_all.at[pl.ds(0, 2 * n_vp - 1)], v_recv.at[2])
        st_lse[chip] = merge(st_all, 2 * n_vp)
        for peer in [lax.rem(tp + j, n_tp) for j in (3, 4, 1, 2, 5, 6, 7)]:
            pltpu.make_async_remote_copy(
                src_ref=st_lse.at[chip], dst_ref=st_lse.at[chip], send_sem=t_send.at[2], recv_sem=t_recv.at[2],
                device_id={"tp": peer}, device_id_type=MESH).start()
        total_send(st_all.at[pl.ds(0, n_vp - 1)], v_send.at[2])
        total_recv(st_lse.at[pl.ds(0, n_chip - 1)], t_recv.at[2])
        total_send(st_all.at[pl.ds(0, n_tp - 1)], t_send.at[2])

    @pl.when(core == 0)
    def _():
        total_send(st_all.at[pl.ds(0, n_vp)], v_send.at[2])
        total_recv(st_lse, t_recv.at[2])

    lse_ref[...] = merge(st_lse, n_chip)


def finish_kernel(n_piece, z_ref, lse_ref, next_ref, out_ref, sum_ref, row_ref, buf, sems):
    lse = lse_ref[...]
    n = z_ref.shape[0] // n_piece

    def put(j):
        part = pl.ds(j * n, n)
        return pltpu.make_async_copy(buf.at[part, :], out_ref.at[part, :], sems.at[j])

    small = [pltpu.make_async_copy(lse_ref, sum_ref, sems.at[n_piece]),
             pltpu.make_async_copy(next_ref, row_ref, sems.at[n_piece + 1])]
    for copy in small:
        copy.start()
    for j in range(n_piece):
        buf[j * n:(j + 1) * n, :] = z_ref[j * n:(j + 1) * n, :] - lse
        put(j).start()
    for copy in small:
        copy.wait()
    for j in range(n_piece):
        put(j).wait()


def solution(mesh):
    n_vp, n_tp = mesh.shape["vp"], mesh.shape["tp"]

    def per_device(hidden, lnf_gain, lnf_bias, emb_table, next_tok, eln_gain, eln_bias):
        rows, width = hidden.shape
        n_block = emb_table.shape[0] // n_tp
        slab = rows // n_vp
        n_round = n_block // 2 // CHUNK + 1
        small = n_block - 2 * (n_round - 1) * CHUNK
        dma = pltpu.SemaphoreType.DMA
        vmem = pl.BlockSpec(memory_space=pltpu.VMEM)
        logits, lse, next_in = pl.pallas_call(
            functools.partial(head_kernel, n_vp, n_tp, n_block, width * n_tp),
            out_shape=(
                pltpu.VMEM((n_block, rows), F32),
                pltpu.VMEM((1, rows), F32),
                pltpu.VMEM((rows, width), BF16),
            ),
            in_specs=[pl.BlockSpec(memory_space=pl.ANY)] * 7,
            out_specs=(vmem, vmem, vmem),
            scratch_shapes=[
                pltpu.VMEM((4, n_block, width), BF16),
                pltpu.VMEM((4, n_block, width), BF16),
                pltpu.VMEM((4, n_block, width), F32),
                pltpu.VMEM((4, n_block, width), F32),
                pltpu.VMEM((n_block, rows), F32),
                pltpu.VMEM((n_block, rows), F32),
                pltpu.VMEM((n_block, rows), F32),
                pltpu.VMEM((n_block, rows), F32),
                pltpu.VMEM((n_block, rows), F32),
                pltpu.VMEM((2, width, rows + 256), F32),
                pltpu.VMEM((2, width, rows), BF16),
                pltpu.VMEM((8, rows), F32),
                pltpu.VMEM((8, rows), F32),
                pltpu.VMEM((rows, width), F32),
                pltpu.VMEM((n_tp, 1, 2 * rows), F32),
                pltpu.VMEM((n_tp // 2, 1, rows), F32),
                pltpu.VMEM((2 * n_vp, 1, rows), F32),
                pltpu.VMEM((n_vp, slab, width), F32),
                pltpu.VMEM((n_tp, 1, 256), F32),
                pltpu.VMEM((n_vp, slab, width), F32),
                pltpu.VMEM((small, width), F32),
                pltpu.VMEM((2, small // 16 * 8, width), F32),
                pltpu.VMEM((2, small - small // 16 * 8, width), F32),
                pltpu.VMEM((width // (n_vp // 2), rows), F32),
                pltpu.VMEM((2, width, rows), F32),
                pltpu.VMEM((2, width, rows), F32),
                pltpu.VMEM((2, 2, width, rows), BF16),
                dma((7,)), dma((1,)), dma((5,)), dma((1,)), dma((1,)),
                dma((1,)), dma((n_round,)), dma((1,)), dma((1,)), dma((n_round,)),
                dma((3,)), dma((3,)), dma((4,)), dma((4,)), dma((1,)), dma((2,)), dma((1,)), dma((2,)), dma((1,)), dma((1,)),
                pltpu.SemaphoreType.REGULAR((N_HOP,)),
                pltpu.VMEM((rows, width), BF16),
                pltpu.VMEM((1, rows), jnp.int32),
                pltpu.VMEM((4, 1, width), F32),
                dma((3,)),
            ],
            compiler_params=pltpu.CompilerParams(
                collective_id=0, has_side_effects=True, vmem_limit_bytes=57 * 1024 * 1024),
            cost_estimate=pl.CostEstimate(
                flops=4 * rows * n_block * n_tp * width, bytes_accessed=16 * n_block * n_tp * width, transcendentals=rows * n_block),
        )(hidden, lnf_gain[None, :], lnf_bias[None, :], emb_table, next_tok[None, :], eln_gain[None, :], eln_bias[None, :])
        n_piece = 5
        logprobs_t, log_sum, next_bf = pl.pallas_call(
            functools.partial(finish_kernel, n_piece),
            out_shape=(
                jax.ShapeDtypeStruct((n_block, rows), F32),
                jax.ShapeDtypeStruct((1, rows), F32),
                jax.ShapeDtypeStruct((rows, width), BF16),
            ),
            in_specs=[vmem, vmem, vmem],
            out_specs=(pl.BlockSpec(memory_space=pl.ANY),) * 3,
            scratch_shapes=[pltpu.VMEM((n_block, rows), F32), dma((n_piece + 2,))],
            compiler_params=pltpu.CompilerParams(vmem_limit_bytes=16 * 1024 * 1024),
        )(logits, lse, next_in)
        return logprobs_t.T, log_sum[0], next_bf

    return jax.shard_map(
        per_device,
        mesh=mesh,
        in_specs=(P("dp", "tp"), P("tp"), P("tp"), P("vp", "tp"), P("dp"), P("tp"), P("tp")),
        out_specs=(P("dp", ("vp", "tp")), P("dp"), P("dp", "tp")),
        check_vma=False,
    )
```

```python
import functools

import jax
import jax.numpy as jnp
from jax import lax
from jax.experimental import pallas as pl
from jax.experimental.pallas import tpu as pltpu
from jax.sharding import PartitionSpec as P

NORM_EPS = 1e-5
MESH = pl.DeviceIdType.MESH
CHUNK = 144
F32 = jnp.float32
BF16 = jnp.bfloat16

OPP, LEFT, RIGHT, OWN = 0, 1, 2, 3
SIDE = 4
N_HOP = 5
STEP_OF_SLOT = (2, 3, 1, 0)


def head_kernel(n_vp, n_tp, n_block, full_width,
                hid_hbm, g_hbm, b_hbm, emb_ref, tok_hbm, eg_hbm, eb_hbm,
                logits_ref, lse_ref, next_ref,
                e_own, e_oth, e_out, e_in, send_f, recv_f, send_n, recv_l, recv_r,
                hx, xn, m_acc, s_acc, pick, st_ln, st_lse, st_all, rs_buf, row_st, ag_buf,
                raw_src, raw_l, raw_r, slab_src, nb, nb_par, xnb,
                ld_sem, ex_send, ex_recv, hx_send, hx_recv,
                f_send, f_recv, n_send, r_send, in_recv,
                t_send, t_recv, v_send, v_recv, raw_send, raw_recv, sx_send, sx_recv, nb_send, nb_recv, hop,
                hid_ref, tok_ref, vec_ref, in_sem):
    vp = lax.axis_index("vp")
    tp = lax.axis_index("tp")
    core = lax.rem(tp, 2)
    chip = tp // 2
    n_chip = n_tp // 2
    rows, width = hid_hbm.shape
    slab = rows // n_vp
    xslab = width // (n_vp // 2)
    left_chip = lax.rem(chip + n_chip - 1, n_chip)
    right_chip = lax.rem(chip + 1, n_chip)
    left = {"tp": left_chip * 2 + core}
    right = {"tp": right_chip * 2 + core}
    partner = {"tp": chip * 2 + 1 - core}
    y = lax.rem(vp, SIDE)
    z = vp // SIDE
    n_z = n_vp // SIDE
    near_by = ((y > 0, {"vp": lax.rem(vp + n_vp - 1, n_vp)}), (y < SIDE - 1, {"vp": lax.rem(vp + 1, n_vp)}),
               (z > 0, {"vp": lax.rem(vp + n_vp - SIDE, n_vp)}), (z < n_z - 1, {"vp": lax.rem(vp + SIDE, n_vp)}))
    n_near = sum(jnp.where(there, 1, 0) for there, _ in near_by)

    def tell_near(sem):
        for there, peer in near_by:
            @pl.when(there)
            def _(peer=peer):
                pl.semaphore_signal(sem, inc=1, device_id=peer, device_id_type=MESH)

    def hear_near(step):
        pl.semaphore_wait(hop.at[step], n_near)
        if step + 1 < N_HOP:
            tell_near(hop.at[step + 1])

    n_carry = n_vp // 2
    carries = vp < n_carry
    half = (n_block // 2) // CHUNK
    n_round = half + 1
    small = n_block - 2 * half * CHUNK
    small1 = (small // 16) * 8
    small2 = small - small1
    tail0 = 2 * half * CHUNK

    def piece(h, i):
        if isinstance(i, int) and i == 0:
            return (tail0, small1) if h == 0 else (tail0 + small1, small2)
        off = h * half * CHUNK + (i - 1) * CHUNK
        return (off if isinstance(i, int) else pl.multiple_of(off, 16)), CHUNK

    barrier = pltpu.get_barrier_semaphore()
    for j in range(1, n_tp):
        pl.semaphore_signal(barrier, inc=1, device_id={"tp": lax.rem(tp + j, n_tp)}, device_id_type=MESH)
    tell_near(barrier)

    parts = ((tail0, small), (0, tail0), (0, n_block))

    def load(slot, other, q, sem):
        blk = lax.rem(chip + STEP_OF_SLOT[slot], n_chip) * 2 + (1 - core if other else core)
        off, n = parts[q]
        src = emb_ref.at[pl.ds(pl.multiple_of(blk * n_block + off, 8), n), :]
        dst = (e_oth if other else e_own).at[slot, pl.ds(off, n), :]
        return pltpu.make_async_copy(src, dst, ld_sem.at[sem])

    hid_copy = pltpu.make_async_copy(hid_hbm, hid_ref, in_sem.at[0])
    tok_copy = pltpu.make_async_copy(tok_hbm, tok_ref, in_sem.at[1])
    hid_copy.start()
    for k, src in enumerate((g_hbm, b_hbm, eg_hbm, eb_hbm)):
        pltpu.make_async_copy(src, vec_ref.at[k], in_sem.at[2]).start()
    for slot in (RIGHT, LEFT):
        load(slot, True, 0, 0).start()
        load(slot, False, 0, 0).start()

    def total_load(ref, sem):
        pltpu.make_async_copy(ref, ref, sem).wait()

    def total_recv(ref, sem):
        pltpu.make_async_remote_copy(src_ref=ref, dst_ref=ref, send_sem=sem, recv_sem=sem,
                                     device_id=partner, device_id_type=MESH).wait_recv()

    def total_send(ref, sem):
        pltpu.make_async_remote_copy(src_ref=ref, dst_ref=ref, send_sem=sem, recv_sem=sem,
                                     device_id=partner, device_id_type=MESH).wait_send()

    hid_copy.wait()
    h_t = hid_ref[...].astype(F32).T
    hx[0, :, 0:rows] = h_t
    st_ln[tp, :, 0:rows] = jnp.sum(h_t, axis=0, keepdims=True)
    st_ln[tp, :, rows:2 * rows] = jnp.sum(h_t * h_t, axis=0, keepdims=True)

    def convert(slot, q):
        off, n = parts[q]
        e_out[slot, off:off + n, :] = e_oth[slot, off:off + n, :].astype(F32)

    total_load(e_own.at[0, pl.ds(0, 4 * small), :], ld_sem.at[0])
    for slot, q, sem in ((OPP, 2, 1), (LEFT, 1, 3), (RIGHT, 1, 3), (OWN, 2, 4)):
        load(slot, True, q, sem).start()
        if slot == OPP:
            load(slot, False, q, 2).start()
    for slot, q, sem in ((LEFT, 1, 5), (RIGHT, 1, 5), (OWN, 2, 6)):
        load(slot, False, q, sem).start()
    tok_copy.start()
    for slot in (RIGHT, LEFT):
        convert(slot, 0)
        off, n = piece(0 if slot == RIGHT else 1, 0)
        raw_src[off - tail0:off - tail0 + n, :] = e_own[slot, off:off + n, :].astype(F32)

    def raw_copy(slot, other):
        off, n = piece(0 if slot == RIGHT else 1, 0)
        src = e_out.at[slot, pl.ds(off, n), :] if other else raw_src.at[pl.ds(off - tail0, n), :]
        to = (right_chip if slot == RIGHT else left_chip) * 2 + (1 - core if other else core)
        return pltpu.make_async_remote_copy(
            src_ref=src, dst_ref=(raw_l if slot == RIGHT else raw_r).at[int(other)],
            send_sem=raw_send.at[0], recv_sem=raw_recv.at[int(slot == LEFT)],
            device_id={"tp": to}, device_id_type=MESH)

    pl.semaphore_wait(barrier, n_tp - 1 + n_near)

    def tp_start(buf, stage):
        for j in range(1, n_tp):
            pltpu.make_async_remote_copy(
                src_ref=buf.at[tp], dst_ref=buf.at[tp], send_sem=t_send.at[stage], recv_sem=t_recv.at[stage],
                device_id={"tp": lax.rem(tp + j, n_tp)}, device_id_type=MESH).start()

    def tp_wait(buf, stage):
        total_recv(buf.at[pl.ds(0, n_tp - 1)], t_recv.at[stage])

    def tp_drain(buf, stage):
        total_send(buf.at[pl.ds(0, n_tp - 1)], t_send.at[stage])

    tp_start(st_ln, 0)
    for other in (False, True):
        for slot in (RIGHT, LEFT):
            raw_copy(slot, other).start()

    total_load(vec_ref, in_sem.at[2])
    hx[0, :, rows:rows + 128] = jnp.broadcast_to(vec_ref[0], (128, width)).T
    hx[0, :, rows + 128:rows + 256] = jnp.broadcast_to(vec_ref[1], (128, width)).T
    hx_copy = pltpu.make_async_remote_copy(
        src_ref=hx.at[0], dst_ref=hx.at[1], send_sem=hx_send.at[0], recv_sem=hx_recv.at[0],
        device_id=partner, device_id_type=MESH)
    hx_copy.start()
    tell_near(hop.at[0])

    def ex_copy(slot, q, sem):
        off, n = parts[q]
        return pltpu.make_async_remote_copy(
            src_ref=e_out.at[slot, pl.ds(off, n), :], dst_ref=e_in.at[slot, pl.ds(off, n), :],
            send_sem=ex_send.at[0], recv_sem=ex_recv.at[sem], device_id=partner, device_id_type=MESH)

    load(OPP, True, 2, 1).wait()
    for q in range(2):
        convert(OPP, q)
        ex_copy(OPP, q, q).start()
    for slot in (LEFT, RIGHT):
        ex_copy(slot, 0, 2).start()
    sides = e_oth.at[pl.ds(LEFT, 2), pl.ds(0, tail0), :]
    total_load(sides, ld_sem.at[3])
    for slot in (LEFT, RIGHT):
        convert(slot, 1)
        ex_copy(slot, 1, 3).start()
    load(OWN, True, 2, 4).wait()
    convert(OWN, 2)
    ex_copy(OWN, 2, 4).start()

    tp_wait(st_ln, 0)
    total = st_ln[0]
    for j in range(1, n_tp):
        total = total + st_ln[j]
    mean = total[:, 0:rows] / full_width
    rstd = lax.rsqrt(total[:, rows:2 * rows] / full_width - mean * mean + NORM_EPS)

    def norm(which):
        gain = hx[which, :, rows:rows + 128]
        bias = hx[which, :, rows + 128:rows + 256]
        for c in range(rows // 128):
            cols = slice(c * 128, c * 128 + 128)
            xn[which, :, cols] = ((hx[which, :, cols] - mean[:, cols]) * rstd[:, cols] * gain + bias).astype(BF16)

    def slab_copy(d):
        return pltpu.make_async_remote_copy(
            src_ref=slab_src, dst_ref=nb.at[d, pl.ds(pl.multiple_of(vp * xslab, 8), xslab), :],
            send_sem=sx_send.at[0], recv_sem=sx_recv.at[d], device_id=right if d == 0 else left, device_id_type=MESH)

    norm(0)

    @pl.when(carries)
    def _():
        slab_src[...] = xn[0, pl.ds(pl.multiple_of(vp * xslab, 32), xslab), :].astype(F32)
        for d in range(2):
            slab_copy(d).start()

    hx_copy.wait_recv()
    norm(1)

    def part_sum(slot, off, n):
        mine = e_own[slot, pl.ds(off, n), :]
        theirs = e_in[slot, pl.ds(off, n), :].astype(BF16)
        return (jnp.dot(mine, xn[0], preferred_element_type=F32)
                + jnp.dot(theirs, xn[1], preferred_element_type=F32))

    def f_copy(h, i):
        off, n = piece(h, i)
        return pltpu.make_async_remote_copy(
            src_ref=send_f.at[pl.ds(off, n), :], dst_ref=recv_f.at[pl.ds(off, n), :],
            send_sem=f_send.at[0], recv_sem=f_recv.at[i],
            device_id=left if h == 0 else right, device_id_type=MESH)

    def r_copy(h, i):
        off, n = piece(h, i)
        dst = (recv_r if h == 0 else recv_l).at[pl.ds(off, n), :]
        return pltpu.make_async_remote_copy(
            src_ref=recv_f.at[pl.ds(off, n), :], dst_ref=dst,
            send_sem=r_send.at[0], recv_sem=in_recv.at[i],
            device_id=left if h == 0 else right, device_id_type=MESH)

    def n_copy(h, i):
        off, n = piece(h, i)
        dst = (recv_l if h == 0 else recv_r).at[pl.ds(off, n), :]
        return pltpu.make_async_remote_copy(
            src_ref=send_n.at[pl.ds(off, n), :], dst_ref=dst,
            send_sem=n_send.at[0], recv_sem=in_recv.at[i],
            device_id=right if h == 0 else left, device_id_type=MESH)

    def far(i):
        for h in range(2):
            off, n = piece(h, i)
            send_f[pl.ds(off, n), :] = part_sum(OPP, off, n)
            f_copy(h, i).start()

    def near(i):
        for h in range(2):
            off, n = piece(h, i)
            send_n[pl.ds(off, n), :] = part_sum(RIGHT if h == 0 else LEFT, off, n)
            n_copy(h, i).start()

    def relay(i):
        mine = [part_sum(LEFT if h == 0 else RIGHT, *piece(h, i)) for h in range(2)]
        total_recv(recv_f.at[pl.ds(0, small if isinstance(i, int) else 2 * CHUNK), :], f_recv.at[i])
        for h in range(2):
            off, n = piece(h, i)
            recv_f[pl.ds(off, n), :] = recv_f[pl.ds(off, n), :] + mine[h]
            r_copy(h, i).start()

    def account(z):
        zr = z.reshape(z.shape[0] // 8, 8, rows)
        old = m_acc[...]
        new = jnp.maximum(old, jnp.max(zr, axis=0))
        m_acc[...] = new
        s_acc[...] = s_acc[...] * jnp.exp(old - new) + jnp.sum(jnp.exp(zr - new[None]), axis=0)

    def settle_raw():
        for h in range(2):
            off, n = piece(h, 0)
            raw = raw_l if h == 0 else raw_r
            if h == 0:
                total_recv(recv_l.at[pl.ds(0, small), :], in_recv.at[0])
            mine = part_sum(OWN, off, n)
            total_recv(raw, raw_recv.at[h])
            for other in range(2):
                mine = mine + jnp.dot(raw[other].astype(BF16), xnb[h, other], preferred_element_type=F32)
            z = mine + (recv_r if h == 0 else recv_l)[off:off + n, :]
            account(z)
            logits_ref[off:off + n, :] = z

    def settle(i):
        mine = [part_sum(OWN, *piece(h, i)) for h in range(2)]
        total_recv(recv_l.at[pl.ds(0, 4 * CHUNK), :], in_recv.at[i])
        for h in range(2):
            off, n = piece(h, i)
            z = mine[h] + recv_l[pl.ds(off, n), :] + recv_r[pl.ds(off, n), :]
            account(z)
            logits_ref[pl.ds(off, n), :] = z

    tok_copy.wait()
    tok = jnp.broadcast_to(tok_ref[...], (128, rows)).T

    def gather(step):
        for other in range(2):
            blk_chip = lax.rem(chip + jnp.where(step == 0, STEP_OF_SLOT[0], jnp.where(
                step == 1, STEP_OF_SLOT[1], jnp.where(step == 2, STEP_OF_SLOT[2], STEP_OF_SLOT[3]))), n_chip)
            blk = blk_chip * 2 + (1 - core if other else core)
            base = vp * (n_tp * n_block) + blk * n_block
            ref = e_oth if other else e_own
            acc = pick[...]
            for off in range(0, n_block, 512):
                n = min(512, n_block - off)
                for o, k in ((off, n // 128 * 128), (off + n // 128 * 128, n % 128)):
                    if k == 0:
                        continue
                    lane = lax.broadcasted_iota(jnp.int32, (rows, k), 1) + (base + o)
                    if k % 128 == 0:
                        want = jnp.concatenate([tok] * (k // 128), axis=1) if k > 128 else tok
                    else:
                        want = tok[:, :k]
                    hot = jnp.where(want == lane, 1.0, 0.0).astype(BF16)
                    acc = acc + jnp.dot(hot, ref[step, o:o + k, :], preferred_element_type=F32)
            pick[...] = acc

    def v_copy(src, dst, stage, j):
        return pltpu.make_async_remote_copy(
            src_ref=src, dst_ref=dst, send_sem=v_send.at[stage], recv_sem=v_recv.at[stage],
            device_id={"vp": lax.rem(vp + j, n_vp)}, device_id_type=MESH)

    def vp_start(buf, stage):
        for j in range(1, n_vp):
            v_copy(buf.at[vp], buf.at[vp], stage, j).start()

    def vp_wait(buf, stage):
        total_recv(buf.at[pl.ds(0, n_vp - 1)], v_recv.at[stage])

    def vp_drain(buf, stage):
        total_send(buf.at[pl.ds(0, n_vp - 1)], v_send.at[stage])

    def slabs_forward():
        hear_near(N_HOP - 1)

        @pl.when(carries)
        def _():
            own = pl.ds(pl.multiple_of(vp * xslab, 8), xslab)
            for d in range(2):
                slab_copy(d).wait_recv()
                for j in range(1, n_vp):
                    v_copy(nb.at[d, own, :], nb.at[d, own, :], 3, j).start()

    nb_copy = pltpu.make_async_remote_copy(
        src_ref=nb, dst_ref=nb_par, send_sem=nb_send.at[0], recv_sem=nb_recv.at[0], device_id=partner, device_id_type=MESH)

    def slabs_swap():
        @pl.when(carries)
        def _():
            total_recv(nb.at[:, pl.ds(0, width - xslab), :], v_recv.at[3])

        @pl.when(jnp.logical_not(carries))
        def _():
            total_recv(nb, v_recv.at[3])

        nb_copy.start()
        for d in range(2):
            xnb[d, 0] = nb[d].astype(BF16)

    def slabs_done():
        nb_copy.wait_recv()
        for d in range(2):
            xnb[d, 1] = nb_par[d].astype(BF16)

    def rows_scatter():
        for j in range(1, n_vp):
            peer = lax.rem(vp + j, n_vp)
            v_copy(pick.at[pl.ds(pl.multiple_of(peer * slab, 8), slab), :], rs_buf.at[vp], 0, j).start()
        rs_buf[vp] = pick[pl.ds(pl.multiple_of(vp * slab, 8), slab), :]

    def rows_stats():
        vp_wait(rs_buf, 0)
        tot = rs_buf[0]
        for j in range(1, n_vp):
            tot = tot + rs_buf[j]
        ag_buf[vp] = tot
        lane = lax.broadcasted_iota(jnp.int32, (slab, 128), 1)
        both = jnp.where(lane == 0, jnp.sum(tot, axis=1, keepdims=True), jnp.sum(tot * tot, axis=1, keepdims=True)).T
        row_st[tp] = jnp.zeros((1, 256), F32)
        row_st[tp, :, 0:slab] = both[0:1]
        row_st[tp, :, 128:128 + slab] = both[1:2]
        tp_start(row_st, 1)

    def rows_norm():
        tp_wait(row_st, 1)
        tot = row_st[0]
        for j in range(1, n_tp):
            tot = tot + row_st[j]
        mu = tot[:, 0:128] / full_width
        rs = lax.rsqrt(tot[:, 128:256] / full_width - mu * mu + NORM_EPS)
        mu = jnp.broadcast_to(mu, (128, 128)).T[0:slab, 0:1]
        rs = jnp.broadcast_to(rs, (128, 128)).T[0:slab, 0:1]
        out = ((ag_buf[vp] - mu) * rs * vec_ref[2] + vec_ref[3]).astype(BF16)
        ag_buf[vp] = out.astype(F32)
        vp_start(ag_buf, 1)

    def rows_out():
        vp_wait(ag_buf, 1)
        for j in range(n_vp):
            next_ref[j * slab:(j + 1) * slab, :] = ag_buf[j].astype(BF16)

    pick[...] = jnp.zeros_like(pick)
    m_acc[...] = jnp.full_like(m_acc, -jnp.inf)
    s_acc[...] = jnp.zeros_like(s_acc)

    load(OPP, False, 2, 2).wait()
    for q in range(2):
        ex_copy(OPP, q, q).wait_recv()
        far(q)
        hear_near(q)
    total_recv(e_in.at[pl.ds(LEFT, 2), pl.ds(tail0, small), :], ex_recv.at[2])
    far(2)
    hear_near(2)
    relay(0)
    hear_near(3)
    total_load(sides, ld_sem.at[5])
    total_recv(e_in.at[pl.ds(LEFT, 2), pl.ds(0, tail0), :], ex_recv.at[3])
    load(OWN, False, 2, 6).wait()
    ex_copy(OWN, 2, 4).wait_recv()

    def at(i, when, *steps):
        @pl.when(i == when)
        def _():
            for step in steps:
                step()

    def round_body(i, carry):
        near(i)

        @pl.when(i + 2 < n_round)
        def _():
            far(i + 2)

        relay(i)
        at(i, 1, slabs_forward)

        @pl.when(i <= 2)
        def _():
            gather(2 * i - 2)
            gather(2 * i - 1)

        at(i, 3, rows_scatter)
        at(i, 4, slabs_swap, rows_stats)
        at(i, 5, slabs_done, settle_raw)
        at(i, 6, rows_norm)

        @pl.when(i >= 3)
        def _():
            settle(i - 2)

        return carry

    lax.fori_loop(1, n_round, round_body, 0)

    def last_body(i, carry):
        settle(i)
        return carry

    lax.fori_loop(n_round - 2, n_round, last_body, 0)

    def merge(buf, n):
        top = buf[0]
        for j in range(1, n):
            top = jnp.maximum(top, buf[j])
        tot = jnp.exp(buf[0] - top)
        for j in range(1, n):
            tot = tot + jnp.exp(buf[j] - top)
        return top + jnp.log(tot)

    m8 = m_acc[...]
    top = jnp.max(m8, axis=0, keepdims=True)
    st_lse[tp] = top + jnp.log(jnp.sum(s_acc[...] * jnp.exp(m8 - top), axis=0, keepdims=True))

    def collect(to_chip):
        return pltpu.make_async_remote_copy(
            src_ref=st_lse.at[tp], dst_ref=st_lse.at[tp], send_sem=t_send.at[2], recv_sem=t_recv.at[2],
            device_id={"tp": to_chip * 2 + 1}, device_id_type=MESH)

    for j in (2, 3, 1):
        collect(lax.rem(chip + j, n_chip)).start()

    @pl.when(core == 0)
    def _():
        collect(chip).start()

    rows_out()
    hx_copy.wait_send()
    nb_copy.wait_send()
    total_send(e_out, ex_send.at[0])
    total_send(e_in.at[0, pl.ds(0, 2 * small), :], raw_send.at[0])

    @pl.when(carries)
    def _():
        total_send(nb.at[0, pl.ds(0, 2 * xslab), :], sx_send.at[0])
        total_send(send_f.at[pl.ds(0, 2 * (n_vp - 1) * xslab), :], v_send.at[3])

    total_send(send_f, f_send.at[0])
    total_send(recv_f, r_send.at[0])
    total_send(send_n.at[pl.ds(0, tail0), :], n_send.at[0])
    tp_drain(st_ln, 0)
    tp_drain(row_st, 1)
    vp_drain(rs_buf, 0)
    vp_drain(ag_buf, 1)

    def spread(to_vp, to_tp):
        return pltpu.make_async_remote_copy(
            src_ref=st_all.at[vp], dst_ref=st_all.at[vp], send_sem=v_send.at[2], recv_sem=v_recv.at[2],
            device_id={"vp": to_vp, "tp": to_tp}, device_id_type=MESH)

    shifts = sorted(((dz, dy) for dz in range(n_z) for dy in range(SIDE) if dz or dy),
                    key=lambda d: -min(d[0], n_z - d[0]) - min(d[1], SIDE - d[1]))

    @pl.when(core == 1)
    def _():
        total_recv(st_lse.at[pl.ds(0, n_tp - 1)], t_recv.at[2])
        st_all[vp] = merge(st_lse, n_tp)
        for dz, dy in shifts:
            for to_tp in (tp - 1, tp):
                spread(lax.rem(z + dz, n_z) * SIDE + lax.rem(y + dy, SIDE), to_tp).start()
        spread(vp, tp - 1).start()
        total_send(st_lse.at[pl.ds(0, n_chip - 1)], t_send.at[2])
        total_recv(st_all.at[pl.ds(0, n_vp - 1)], v_recv.at[2])

    @pl.when(core == 0)
    def _():
        total_send(st_lse.at[pl.ds(0, n_chip)], t_send.at[2])
        total_recv(st_all.at[pl.ds(0, n_vp)], v_recv.at[2])

    lse_ref[...] = merge(st_all, n_vp)

    @pl.when(core == 1)
    def _():
        total_send(st_all.at[pl.ds(0, 2 * n_vp - 1)], v_send.at[2])


def finish_kernel(n_piece, z_ref, lse_ref, next_ref, out_ref, sum_ref, row_ref, buf, sems):
    lse = lse_ref[...]
    n = z_ref.shape[0] // n_piece

    def put(j):
        part = pl.ds(j * n, n)
        return pltpu.make_async_copy(buf.at[part, :], out_ref.at[part, :], sems.at[j])

    small = [pltpu.make_async_copy(lse_ref, sum_ref, sems.at[n_piece]),
             pltpu.make_async_copy(next_ref, row_ref, sems.at[n_piece + 1])]
    for copy in small:
        copy.start()
    for j in range(n_piece):
        buf[j * n:(j + 1) * n, :] = z_ref[j * n:(j + 1) * n, :] - lse
        put(j).start()
    for copy in small:
        copy.wait()
    for j in range(n_piece):
        put(j).wait()


def solution(mesh):
    n_vp, n_tp = mesh.shape["vp"], mesh.shape["tp"]

    def per_device(hidden, lnf_gain, lnf_bias, emb_table, next_tok, eln_gain, eln_bias):
        rows, width = hidden.shape
        n_block = emb_table.shape[0] // n_tp
        slab = rows // n_vp
        n_round = n_block // 2 // CHUNK + 1
        small = n_block - 2 * (n_round - 1) * CHUNK
        dma = pltpu.SemaphoreType.DMA
        vmem = pl.BlockSpec(memory_space=pltpu.VMEM)
        logits, lse, next_in = pl.pallas_call(
            functools.partial(head_kernel, n_vp, n_tp, n_block, width * n_tp),
            out_shape=(
                pltpu.VMEM((n_block, rows), F32),
                pltpu.VMEM((1, rows), F32),
                pltpu.VMEM((rows, width), BF16),
            ),
            in_specs=[pl.BlockSpec(memory_space=pl.ANY)] * 7,
            out_specs=(vmem, vmem, vmem),
            scratch_shapes=[
                pltpu.VMEM((4, n_block, width), BF16),
                pltpu.VMEM((4, n_block, width), BF16),
                pltpu.VMEM((4, n_block, width), F32),
                pltpu.VMEM((4, n_block, width), F32),
                pltpu.VMEM((n_block, rows), F32),
                pltpu.VMEM((n_block, rows), F32),
                pltpu.VMEM((n_block, rows), F32),
                pltpu.VMEM((n_block, rows), F32),
                pltpu.VMEM((n_block, rows), F32),
                pltpu.VMEM((2, width, rows + 256), F32),
                pltpu.VMEM((2, width, rows), BF16),
                pltpu.VMEM((8, rows), F32),
                pltpu.VMEM((8, rows), F32),
                pltpu.VMEM((rows, width), F32),
                pltpu.VMEM((n_tp, 1, 2 * rows), F32),
                pltpu.VMEM((n_tp, 1, rows), F32),
                pltpu.VMEM((2 * n_vp, 1, rows), F32),
                pltpu.VMEM((n_vp, slab, width), F32),
                pltpu.VMEM((n_tp, 1, 256), F32),
                pltpu.VMEM((n_vp, slab, width), F32),
                pltpu.VMEM((small, width), F32),
                pltpu.VMEM((2, small // 16 * 8, width), F32),
                pltpu.VMEM((2, small - small // 16 * 8, width), F32),
                pltpu.VMEM((width // (n_vp // 2), rows), F32),
                pltpu.VMEM((2, width, rows), F32),
                pltpu.VMEM((2, width, rows), F32),
                pltpu.VMEM((2, 2, width, rows), BF16),
                dma((7,)), dma((1,)), dma((5,)), dma((1,)), dma((1,)),
                dma((1,)), dma((n_round,)), dma((1,)), dma((1,)), dma((n_round,)),
                dma((3,)), dma((3,)), dma((4,)), dma((4,)), dma((1,)), dma((2,)), dma((1,)), dma((2,)), dma((1,)), dma((1,)),
                pltpu.SemaphoreType.REGULAR((N_HOP,)),
                pltpu.VMEM((rows, width), BF16),
                pltpu.VMEM((1, rows), jnp.int32),
                pltpu.VMEM((4, 1, width), F32),
                dma((3,)),
            ],
            compiler_params=pltpu.CompilerParams(
                collective_id=0, has_side_effects=True, vmem_limit_bytes=57 * 1024 * 1024),
            cost_estimate=pl.CostEstimate(
                flops=4 * rows * n_block * n_tp * width, bytes_accessed=16 * n_block * n_tp * width, transcendentals=rows * n_block),
        )(hidden, lnf_gain[None, :], lnf_bias[None, :], emb_table, next_tok[None, :], eln_gain[None, :], eln_bias[None, :])
        n_piece = 5
        logprobs_t, log_sum, next_bf = pl.pallas_call(
            functools.partial(finish_kernel, n_piece),
            out_shape=(
                jax.ShapeDtypeStruct((n_block, rows), F32),
                jax.ShapeDtypeStruct((1, rows), F32),
                jax.ShapeDtypeStruct((rows, width), BF16),
            ),
            in_specs=[vmem, vmem, vmem],
            out_specs=(pl.BlockSpec(memory_space=pl.ANY),) * 3,
            scratch_shapes=[pltpu.VMEM((n_block, rows), F32), dma((n_piece + 2,))],
            compiler_params=pltpu.CompilerParams(vmem_limit_bytes=16 * 1024 * 1024),
        )(logits, lse, next_in)
        return logprobs_t.T, log_sum[0], next_bf

    return jax.shard_map(
        per_device,
        mesh=mesh,
        in_specs=(P("dp", "tp"), P("tp"), P("tp"), P("vp", "tp"), P("dp"), P("tp"), P("tp")),
        out_specs=(P("dp", ("vp", "tp")), P("dp"), P("dp", "tp")),
        check_vma=False,
    )
```

```python
import functools

import jax
import jax.numpy as jnp
from jax import lax
from jax.experimental import pallas as pl
from jax.experimental.pallas import tpu as pltpu
from jax.sharding import PartitionSpec as P

NORM_EPS = 1e-5
MESH = pl.DeviceIdType.MESH
CHUNK = 144
F32 = jnp.float32
BF16 = jnp.bfloat16

OPP, LEFT, RIGHT, OWN = 0, 1, 2, 3
SIDE = 4
N_HOP = 5
FIRST = 1
STEP_OF_SLOT = (2, 3, 1, 0)


def head_kernel(n_vp, n_tp, n_block, full_width,
                hid_hbm, g_hbm, b_hbm, emb_ref, tok_hbm, eg_hbm, eb_hbm,
                logits_ref, lse_ref, next_ref,
                e_own, e_oth, e_out, e_in, send_f, recv_f, send_n, recv_l, recv_r,
                hx, xn, m_acc, s_acc, pick, st_ln, st_lse, st_all, rs_buf, row_st, ag_buf, st_dir,
                raw_src, raw_l, raw_r, slab_src, nb, nb_par, xnb,
                ld_sem, ex_send, ex_recv, hx_send, hx_recv,
                f_send, f_recv, n_send, r_send, in_recv,
                t_send, t_recv, v_send, v_recv, raw_send, raw_recv, sx_recv, nb_recv, d_recv, hop,
                hid_ref, tok_ref, vec_ref, in_sem):
    vp = lax.axis_index("vp")
    tp = lax.axis_index("tp")
    core = lax.rem(tp, 2)
    chip = tp // 2
    n_chip = n_tp // 2
    rows, width = hid_hbm.shape
    slab = rows // n_vp
    xslab = width // (n_vp // 2)
    left_chip = lax.rem(chip + n_chip - 1, n_chip)
    right_chip = lax.rem(chip + 1, n_chip)
    left = {"tp": left_chip * 2 + core}
    right = {"tp": right_chip * 2 + core}
    partner = {"tp": chip * 2 + 1 - core}
    y = lax.rem(vp, SIDE)
    z = vp // SIDE
    n_z = n_vp // SIDE
    near_by = ((y > 0, {"vp": lax.rem(vp + n_vp - 1, n_vp)}), (y < SIDE - 1, {"vp": lax.rem(vp + 1, n_vp)}),
               (z > 0, {"vp": lax.rem(vp + n_vp - SIDE, n_vp)}), (z < n_z - 1, {"vp": lax.rem(vp + SIDE, n_vp)}))
    n_near = sum(jnp.where(there, 1, 0) for there, _ in near_by)

    def tell_near(sem):
        for there, peer in near_by:
            @pl.when(there)
            def _(peer=peer):
                pl.semaphore_signal(sem, inc=1, device_id=peer, device_id_type=MESH)

    def hear_near(step):
        pl.semaphore_wait(hop.at[step], n_near)
        if step + 1 < N_HOP:
            tell_near(hop.at[step + 1])

    n_carry = n_vp // 2
    carries = vp < n_carry
    half = (n_block // 2) // CHUNK
    n_round = half + 1
    small = n_block - 2 * half * CHUNK
    small1 = (small // 16) * 8
    small2 = small - small1
    tail0 = 2 * half * CHUNK

    def piece(h, i):
        if isinstance(i, int) and i == 0:
            return (tail0, small1) if h == 0 else (tail0 + small1, small2)
        off = h * half * CHUNK + (i - 1) * CHUNK
        return (off if isinstance(i, int) else pl.multiple_of(off, 16)), CHUNK

    barrier = pltpu.get_barrier_semaphore()
    for j in range(1, n_tp):
        pl.semaphore_signal(barrier, inc=1, device_id={"tp": lax.rem(tp + j, n_tp)}, device_id_type=MESH)
    tell_near(barrier)

    parts = ((tail0, small), (0, tail0), (0, n_block))

    def load(slot, other, q, sem):
        blk = lax.rem(chip + STEP_OF_SLOT[slot], n_chip) * 2 + (1 - core if other else core)
        off, n = parts[q]
        src = emb_ref.at[pl.ds(pl.multiple_of(blk * n_block + off, 8), n), :]
        dst = (e_oth if other else e_own).at[slot, pl.ds(off, n), :]
        return pltpu.make_async_copy(src, dst, ld_sem.at[sem])

    hid_copy = pltpu.make_async_copy(hid_hbm, hid_ref, in_sem.at[0])
    tok_copy = pltpu.make_async_copy(tok_hbm, tok_ref, in_sem.at[1])
    hid_copy.start()
    for k, src in enumerate((g_hbm, b_hbm, eg_hbm, eb_hbm)):
        pltpu.make_async_copy(src, vec_ref.at[k], in_sem.at[2]).start()
    for slot in (RIGHT, LEFT):
        load(slot, True, 0, 0).start()
        load(slot, False, 0, 0).start()

    def total_load(ref, sem):
        pltpu.make_async_copy(ref, ref, sem).wait()

    def total_recv(ref, sem):
        pltpu.make_async_remote_copy(src_ref=ref, dst_ref=ref, send_sem=sem, recv_sem=sem,
                                     device_id=partner, device_id_type=MESH).wait_recv()

    def total_send(ref, sem):
        pltpu.make_async_remote_copy(src_ref=ref, dst_ref=ref, send_sem=sem, recv_sem=sem,
                                     device_id=partner, device_id_type=MESH).wait_send()

    hid_copy.wait()
    h_t = hid_ref[...].astype(F32).T
    hx[0, :, 0:rows] = h_t
    st_ln[tp, :, 0:rows] = jnp.sum(h_t, axis=0, keepdims=True)
    st_ln[tp, :, rows:2 * rows] = jnp.sum(h_t * h_t, axis=0, keepdims=True)

    def convert(slot, q):
        off, n = parts[q]
        e_out[slot, off:off + n, :] = e_oth[slot, off:off + n, :].astype(F32)

    total_load(e_own.at[0, pl.ds(0, 4 * small), :], ld_sem.at[0])
    for slot, q, sem in ((OPP, 2, 1), (LEFT, 1, 3), (RIGHT, 1, 3), (OWN, 2, 4)):
        load(slot, True, q, sem).start()
        if slot == OPP:
            load(slot, False, q, 2).start()
    for slot, q, sem in ((LEFT, 1, 5), (RIGHT, 1, 5), (OWN, 2, 6)):
        load(slot, False, q, sem).start()
    tok_copy.start()
    for slot in (RIGHT, LEFT):
        convert(slot, 0)
        off, n = piece(0 if slot == RIGHT else 1, 0)
        raw_src[off - tail0:off - tail0 + n, :] = e_own[slot, off:off + n, :].astype(F32)

    def raw_copy(slot, other):
        off, n = piece(0 if slot == RIGHT else 1, 0)
        src = e_out.at[slot, pl.ds(off, n), :] if other else raw_src.at[pl.ds(off - tail0, n), :]
        to = (right_chip if slot == RIGHT else left_chip) * 2 + (1 - core if other else core)
        return pltpu.make_async_remote_copy(
            src_ref=src, dst_ref=(raw_l if slot == RIGHT else raw_r).at[int(other)],
            send_sem=raw_send.at[0], recv_sem=raw_recv.at[int(slot == LEFT)],
            device_id={"tp": to}, device_id_type=MESH)

    pl.semaphore_wait(barrier, n_tp - 1 + n_near)

    def tp_start(buf, stage):
        for j in range(1, n_tp):
            pltpu.make_async_remote_copy(
                src_ref=buf.at[tp], dst_ref=buf.at[tp], send_sem=t_send.at[0], recv_sem=t_recv.at[stage],
                device_id={"tp": lax.rem(tp + j, n_tp)}, device_id_type=MESH).start()

    def tp_wait(buf, stage):
        total_recv(buf.at[pl.ds(0, n_tp - 1)], t_recv.at[stage])

    def tp_drain(buf):
        total_send(buf.at[pl.ds(0, n_tp - 1)], t_send.at[0])

    tp_start(st_ln, 0)
    for other in (False, True):
        for slot in (RIGHT, LEFT):
            raw_copy(slot, other).start()

    total_load(vec_ref, in_sem.at[2])
    hx[0, :, rows:rows + 128] = jnp.broadcast_to(vec_ref[0], (128, width)).T
    hx[0, :, rows + 128:rows + 256] = jnp.broadcast_to(vec_ref[1], (128, width)).T
    hx_copy = pltpu.make_async_remote_copy(
        src_ref=hx.at[0], dst_ref=hx.at[1], send_sem=hx_send.at[0], recv_sem=hx_recv.at[0],
        device_id=partner, device_id_type=MESH)
    hx_copy.start()
    tell_near(hop.at[0])

    def ex_copy(slot, q, sem):
        off, n = parts[q]
        return pltpu.make_async_remote_copy(
            src_ref=e_out.at[slot, pl.ds(off, n), :], dst_ref=e_in.at[slot, pl.ds(off, n), :],
            send_sem=ex_send.at[0], recv_sem=ex_recv.at[sem], device_id=partner, device_id_type=MESH)

    load(OPP, True, 2, 1).wait()
    for q in range(2):
        convert(OPP, q)
        ex_copy(OPP, q, q).start()
    for slot in (LEFT, RIGHT):
        ex_copy(slot, 0, 2).start()
    sides = e_oth.at[pl.ds(LEFT, 2), pl.ds(0, tail0), :]
    total_load(sides, ld_sem.at[3])
    for slot in (LEFT, RIGHT):
        convert(slot, 1)
        ex_copy(slot, 1, 3).start()
    load(OWN, True, 2, 4).wait()
    convert(OWN, 2)
    ex_copy(OWN, 2, 4).start()

    tp_wait(st_ln, 0)
    total = st_ln[0]
    for j in range(1, n_tp):
        total = total + st_ln[j]
    mean = total[:, 0:rows] / full_width
    rstd = lax.rsqrt(total[:, rows:2 * rows] / full_width - mean * mean + NORM_EPS)

    def norm(which):
        gain = hx[which, :, rows:rows + 128]
        bias = hx[which, :, rows + 128:rows + 256]
        for c in range(rows // 128):
            cols = slice(c * 128, c * 128 + 128)
            xn[which, :, cols] = ((hx[which, :, cols] - mean[:, cols]) * rstd[:, cols] * gain + bias).astype(BF16)

    def slab_copy(d):
        return pltpu.make_async_remote_copy(
            src_ref=slab_src, dst_ref=nb.at[d, pl.ds(pl.multiple_of(vp * xslab, 8), xslab), :],
            send_sem=hx_send.at[0], recv_sem=sx_recv.at[d], device_id=right if d == 0 else left, device_id_type=MESH)

    norm(0)
    hx_copy.wait_send()

    @pl.when(carries)
    def _():
        slab_src[...] = xn[0, pl.ds(pl.multiple_of(vp * xslab, 32), xslab), :].astype(F32)
        for d in range(2):
            slab_copy(d).start()

    hx_copy.wait_recv()
    norm(1)

    def part_sum(slot, off, n):
        mine = e_own[slot, pl.ds(off, n), :]
        theirs = e_in[slot, pl.ds(off, n), :].astype(BF16)
        return (jnp.dot(mine, xn[0], preferred_element_type=F32)
                + jnp.dot(theirs, xn[1], preferred_element_type=F32))

    def f_copy(h, i):
        off, n = piece(h, i)
        return pltpu.make_async_remote_copy(
            src_ref=send_f.at[pl.ds(off, n), :], dst_ref=recv_f.at[pl.ds(off, n), :],
            send_sem=f_send.at[0], recv_sem=f_recv.at[i],
            device_id=left if h == 0 else right, device_id_type=MESH)

    def r_copy(h, i):
        off, n = piece(h, i)
        dst = (recv_r if h == 0 else recv_l).at[pl.ds(off, n), :]
        return pltpu.make_async_remote_copy(
            src_ref=recv_f.at[pl.ds(off, n), :], dst_ref=dst,
            send_sem=r_send.at[0], recv_sem=in_recv.at[i],
            device_id=left if h == 0 else right, device_id_type=MESH)

    def n_copy(h, i):
        off, n = piece(h, i)
        dst = (recv_l if h == 0 else recv_r).at[pl.ds(off, n), :]
        return pltpu.make_async_remote_copy(
            src_ref=send_n.at[pl.ds(off, n), :], dst_ref=dst,
            send_sem=n_send.at[0], recv_sem=in_recv.at[i],
            device_id=right if h == 0 else left, device_id_type=MESH)

    def far(i):
        for h in range(2):
            off, n = piece(h, i)
            send_f[pl.ds(off, n), :] = part_sum(OPP, off, n)
            f_copy(h, i).start()

    def near(i):
        for h in range(2):
            off, n = piece(h, i)
            send_n[pl.ds(off, n), :] = part_sum(RIGHT if h == 0 else LEFT, off, n)
            n_copy(h, i).start()

    def relay(i):
        mine = [part_sum(LEFT if h == 0 else RIGHT, *piece(h, i)) for h in range(2)]
        total_recv(recv_f.at[pl.ds(0, small if isinstance(i, int) else 2 * CHUNK), :], f_recv.at[i])
        for h in range(2):
            off, n = piece(h, i)
            recv_f[pl.ds(off, n), :] = recv_f[pl.ds(off, n), :] + mine[h]
            r_copy(h, i).start()

    def account(z):
        zr = z.reshape(z.shape[0] // 8, 8, rows)
        old = m_acc[...]
        new = jnp.maximum(old, jnp.max(zr, axis=0))
        m_acc[...] = new
        s_acc[...] = s_acc[...] * jnp.exp(old - new) + jnp.sum(jnp.exp(zr - new[None]), axis=0)

    def settle_raw():
        for h in range(2):
            off, n = piece(h, 0)
            raw = raw_l if h == 0 else raw_r
            if h == 0:
                total_recv(recv_l.at[pl.ds(0, small), :], in_recv.at[0])
            mine = part_sum(OWN, off, n)
            total_recv(raw, raw_recv.at[h])
            for other in range(2):
                mine = mine + jnp.dot(raw[other].astype(BF16), xnb[h, other], preferred_element_type=F32)
            z = mine + (recv_r if h == 0 else recv_l)[off:off + n, :]
            account(z)
            logits_ref[off:off + n, :] = z

    def settle(i):
        mine = [part_sum(OWN, *piece(h, i)) for h in range(2)]
        total_recv(recv_l.at[pl.ds(0, 4 * CHUNK), :], in_recv.at[i])
        for h in range(2):
            off, n = piece(h, i)
            z = mine[h] + recv_l[pl.ds(off, n), :] + recv_r[pl.ds(off, n), :]
            account(z)
            logits_ref[pl.ds(off, n), :] = z

    tok_copy.wait()
    tok = jnp.broadcast_to(tok_ref[...], (128, rows)).T

    def gather(step):
        for other in range(2):
            blk_chip = lax.rem(chip + jnp.where(step == 0, STEP_OF_SLOT[0], jnp.where(
                step == 1, STEP_OF_SLOT[1], jnp.where(step == 2, STEP_OF_SLOT[2], STEP_OF_SLOT[3]))), n_chip)
            blk = blk_chip * 2 + (1 - core if other else core)
            base = vp * (n_tp * n_block) + blk * n_block
            ref = e_oth if other else e_own
            acc = pick[...]
            for off in range(0, n_block, 512):
                n = min(512, n_block - off)
                for o, k in ((off, n // 128 * 128), (off + n // 128 * 128, n % 128)):
                    if k == 0:
                        continue
                    lane = lax.broadcasted_iota(jnp.int32, (rows, k), 1) + (base + o)
                    if k % 128 == 0:
                        want = jnp.concatenate([tok] * (k // 128), axis=1) if k > 128 else tok
                    else:
                        want = tok[:, :k]
                    hot = jnp.where(want == lane, 1.0, 0.0).astype(BF16)
                    acc = acc + jnp.dot(hot, ref[step, o:o + k, :], preferred_element_type=F32)
            pick[...] = acc

    def v_copy(src, dst, stage, j):
        return pltpu.make_async_remote_copy(
            src_ref=src, dst_ref=dst, send_sem=v_send.at[0], recv_sem=v_recv.at[stage],
            device_id={"vp": lax.rem(vp + j, n_vp)}, device_id_type=MESH)

    def vp_start(buf, stage):
        for j in range(1, n_vp):
            v_copy(buf.at[vp], buf.at[vp], stage, j).start()

    def vp_wait(buf, stage):
        total_recv(buf.at[pl.ds(0, n_vp - 1)], v_recv.at[stage])

    def vp_drain(buf):
        total_send(buf.at[pl.ds(0, n_vp - 1)], v_send.at[0])

    def slabs_forward():
        hear_near(N_HOP - 1)

        @pl.when(carries)
        def _():
            own = pl.ds(pl.multiple_of(vp * xslab, 8), xslab)
            for d in range(2):
                slab_copy(d).wait_recv()
                for j in range(1, n_vp):
                    v_copy(nb.at[d, own, :], nb.at[d, own, :], 3, j).start()

    nb_copy = pltpu.make_async_remote_copy(
        src_ref=nb, dst_ref=nb_par, send_sem=hx_send.at[0], recv_sem=nb_recv.at[0], device_id=partner, device_id_type=MESH)

    def slabs_swap():
        @pl.when(carries)
        def _():
            total_send(nb.at[0, pl.ds(0, 2 * xslab), :], hx_send.at[0])
            total_recv(nb.at[:, pl.ds(0, width - xslab), :], v_recv.at[3])

        @pl.when(jnp.logical_not(carries))
        def _():
            total_recv(nb, v_recv.at[3])

        nb_copy.start()
        for d in range(2):
            xnb[d, 0] = nb[d].astype(BF16)

    def slabs_done():
        nb_copy.wait_recv()
        for d in range(2):
            xnb[d, 1] = nb_par[d].astype(BF16)

    def rows_scatter():
        @pl.when(carries)
        def _():
            total_send(send_f.at[pl.ds(0, 2 * (n_vp - 1) * xslab), :], v_send.at[0])

        for j in range(1, n_vp):
            peer = lax.rem(vp + j, n_vp)
            v_copy(pick.at[pl.ds(pl.multiple_of(peer * slab, 8), slab), :], rs_buf.at[vp], 0, j).start()
        rs_buf[vp] = pick[pl.ds(pl.multiple_of(vp * slab, 8), slab), :]

    def rows_stats():
        vp_wait(rs_buf, 0)
        tot = rs_buf[0]
        for j in range(1, n_vp):
            tot = tot + rs_buf[j]
        ag_buf[vp] = tot
        lane = lax.broadcasted_iota(jnp.int32, (slab, 128), 1)
        both = jnp.where(lane == 0, jnp.sum(tot, axis=1, keepdims=True), jnp.sum(tot * tot, axis=1, keepdims=True)).T
        tp_drain(st_ln)
        row_st[tp] = jnp.zeros((1, 256), F32)
        row_st[tp, :, 0:slab] = both[0:1]
        row_st[tp, :, 128:128 + slab] = both[1:2]
        tp_start(row_st, 1)

    def rows_norm():
        tp_wait(row_st, 1)
        tp_drain(row_st)
        tot = row_st[0]
        for j in range(1, n_tp):
            tot = tot + row_st[j]
        mu = tot[:, 0:128] / full_width
        rs = lax.rsqrt(tot[:, 128:256] / full_width - mu * mu + NORM_EPS)
        mu = jnp.broadcast_to(mu, (128, 128)).T[0:slab, 0:1]
        rs = jnp.broadcast_to(rs, (128, 128)).T[0:slab, 0:1]
        out = ((ag_buf[vp] - mu) * rs * vec_ref[2] + vec_ref[3]).astype(BF16)
        ag_buf[vp] = out.astype(F32)
        vp_drain(rs_buf)
        vp_start(ag_buf, 1)

    def rows_out():
        vp_wait(ag_buf, 1)
        for j in range(n_vp):
            next_ref[j * slab:(j + 1) * slab, :] = ag_buf[j].astype(BF16)

    pick[...] = jnp.zeros_like(pick)
    m_acc[...] = jnp.full_like(m_acc, -jnp.inf)
    s_acc[...] = jnp.zeros_like(s_acc)

    load(OPP, False, 2, 2).wait()
    for q in range(2):
        ex_copy(OPP, q, q).wait_recv()
        far(q)
        hear_near(q)
    total_recv(e_in.at[pl.ds(LEFT, 2), pl.ds(tail0, small), :], ex_recv.at[2])
    far(2)
    hear_near(2)
    relay(0)
    hear_near(3)
    total_load(sides, ld_sem.at[5])
    total_recv(e_in.at[pl.ds(LEFT, 2), pl.ds(0, tail0), :], ex_recv.at[3])
    load(OWN, False, 2, 6).wait()
    ex_copy(OWN, 2, 4).wait_recv()

    def raw_drain():
        total_send(e_in.at[0, pl.ds(0, 2 * small), :], raw_send.at[0])

    def at(i, when, *steps):
        @pl.when(i == when)
        def _():
            for step in steps:
                step()

    def round_body(i, carry):
        near(i)

        @pl.when(i + 2 < n_round)
        def _():
            far(i + 2)

        relay(i)
        at(i, 1, slabs_forward, raw_drain)

        @pl.when(i <= 2)
        def _():
            gather(2 * i - 2)
            gather(2 * i - 1)

        at(i, 3, rows_scatter)
        at(i, 4, slabs_swap, rows_stats)
        at(i, 5, slabs_done, settle_raw)
        at(i, 6, rows_norm)

        @pl.when(i >= 3)
        def _():
            settle(i - 2)

        return carry

    lax.fori_loop(1, n_round, round_body, 0)

    def last_body(i, carry):
        settle(i)
        return carry

    lax.fori_loop(n_round - 2, n_round, last_body, 0)

    def merge(buf, n):
        sums = buf[0:n]
        top = jnp.max(sums, axis=0)
        return top + jnp.log(jnp.sum(jnp.exp(sums - top[None]), axis=0))

    def put(dst, at, value):
        for k in range(rows // 128):
            dst[at, k:k + 1, :] = value[:, k * 128:k * 128 + 128]

    m8 = m_acc[...]
    top = jnp.max(m8, axis=0, keepdims=True)
    put(st_lse, tp, top + jnp.log(jnp.sum(s_acc[...] * jnp.exp(m8 - top), axis=0, keepdims=True)))

    me = vp * n_tp + tp
    is_first = me == FIRST

    @pl.when(jnp.logical_not(is_first))
    def _():
        pltpu.make_async_remote_copy(
            src_ref=st_lse.at[tp], dst_ref=st_dir.at[me], send_sem=raw_send.at[0], recv_sem=d_recv.at[0],
            device_id={"vp": FIRST // n_tp, "tp": FIRST % n_tp}, device_id_type=MESH).start()

    def collect(to_chip):
        return pltpu.make_async_remote_copy(
            src_ref=st_lse.at[tp], dst_ref=st_lse.at[tp], send_sem=t_send.at[0], recv_sem=t_recv.at[2],
            device_id={"tp": to_chip * 2 + 1}, device_id_type=MESH)

    for to in range(n_chip):
        @pl.when(jnp.logical_or(chip != to, core == 0))
        def _(to=to):
            collect(to).start()

    rows_out()
    nb_copy.wait_send()
    total_send(e_out, ex_send.at[0])
    total_send(send_f, f_send.at[0])
    total_send(recv_f, r_send.at[0])
    total_send(send_n.at[pl.ds(0, tail0), :], n_send.at[0])
    vp_drain(ag_buf)

    def spread(to, to_core):
        return pltpu.make_async_remote_copy(
            src_ref=st_all.at[vp], dst_ref=st_all.at[vp], send_sem=v_send.at[0], recv_sem=v_recv.at[2],
            device_id={"vp": to, "tp": chip * 2 + to_core}, device_id_type=MESH)

    def is_first_at(to, to_core):
        return jnp.logical_and(to == FIRST // n_tp, chip * 2 + to_core == FIRST % n_tp)

    @pl.when(core == 1)
    def _():
        total_recv(st_lse.at[pl.ds(0, n_tp - 1)], t_recv.at[2])
        st_all[vp] = merge(st_lse, n_tp)
        for to in range(n_vp):
            @pl.when(jnp.logical_and(vp != to, jnp.logical_not(is_first_at(to, 1))))
            def _(to=to):
                spread(to, 1).start()
        for to in range(n_vp):
            spread(to, 0).start()
        total_send(st_lse.at[pl.ds(0, n_chip - 1)], t_send.at[0])

        @pl.when(jnp.logical_not(is_first))
        def _():
            total_recv(st_all.at[pl.ds(0, n_vp - 1)], v_recv.at[2])

    @pl.when(core == 0)
    def _():
        total_send(st_lse.at[pl.ds(0, n_chip)], t_send.at[0])
        total_recv(st_all.at[pl.ds(0, n_vp)], v_recv.at[2])

    def result(value):
        for k in range(rows // 128):
            lse_ref[:, k * 128:k * 128 + 128] = value[k:k + 1, :]

    @pl.when(is_first)
    def _():
        put_row = st_lse[tp]
        st_dir[me] = put_row
        total_recv(st_dir.at[pl.ds(0, n_vp * n_tp - 1)], d_recv.at[0])
        result(merge(st_dir, n_vp * n_tp))

    @pl.when(jnp.logical_not(is_first))
    def _():
        result(merge(st_all, n_vp))
        total_send(st_lse.at[pl.ds(0, 1)], raw_send.at[0])

    sends = 2 * n_vp - 1
    short = jnp.logical_and(chip == FIRST % n_tp // 2, vp != FIRST // n_tp)

    @pl.when(jnp.logical_and(core == 1, short))
    def _():
        total_send(st_all.at[pl.ds(0, sends - 1)], v_send.at[0])

    @pl.when(jnp.logical_and(core == 1, jnp.logical_not(short)))
    def _():
        total_send(st_all.at[pl.ds(0, sends)], v_send.at[0])


def finish_kernel(n_piece, z_ref, lse_ref, next_ref, out_ref, sum_ref, row_ref, buf, sems):
    lse = lse_ref[...]
    n = z_ref.shape[0] // n_piece

    def put(j):
        part = pl.ds(j * n, n)
        return pltpu.make_async_copy(buf.at[part, :], out_ref.at[part, :], sems.at[j])

    small = [pltpu.make_async_copy(lse_ref, sum_ref, sems.at[n_piece]),
             pltpu.make_async_copy(next_ref, row_ref, sems.at[n_piece + 1])]
    for copy in small:
        copy.start()
    for j in range(n_piece):
        buf[j * n:(j + 1) * n, :] = z_ref[j * n:(j + 1) * n, :] - lse
        put(j).start()
    for copy in small:
        copy.wait()
    for j in range(n_piece):
        put(j).wait()


def solution(mesh):
    n_vp, n_tp = mesh.shape["vp"], mesh.shape["tp"]

    def per_device(hidden, lnf_gain, lnf_bias, emb_table, next_tok, eln_gain, eln_bias):
        rows, width = hidden.shape
        n_block = emb_table.shape[0] // n_tp
        slab = rows // n_vp
        n_round = n_block // 2 // CHUNK + 1
        small = n_block - 2 * (n_round - 1) * CHUNK
        dma = pltpu.SemaphoreType.DMA
        vmem = pl.BlockSpec(memory_space=pltpu.VMEM)
        logits, lse, next_in = pl.pallas_call(
            functools.partial(head_kernel, n_vp, n_tp, n_block, width * n_tp),
            out_shape=(
                pltpu.VMEM((n_block, rows), F32),
                pltpu.VMEM((1, rows), F32),
                pltpu.VMEM((rows, width), BF16),
            ),
            in_specs=[pl.BlockSpec(memory_space=pl.ANY)] * 7,
            out_specs=(vmem, vmem, vmem),
            scratch_shapes=[
                pltpu.VMEM((4, n_block, width), BF16),
                pltpu.VMEM((4, n_block, width), BF16),
                pltpu.VMEM((4, n_block, width), F32),
                pltpu.VMEM((4, n_block, width), F32),
                pltpu.VMEM((n_block, rows), F32),
                pltpu.VMEM((n_block, rows), F32),
                pltpu.VMEM((n_block, rows), F32),
                pltpu.VMEM((n_block, rows), F32),
                pltpu.VMEM((n_block, rows), F32),
                pltpu.VMEM((2, width, rows + 256), F32),
                pltpu.VMEM((2, width, rows), BF16),
                pltpu.VMEM((8, rows), F32),
                pltpu.VMEM((8, rows), F32),
                pltpu.VMEM((rows, width), F32),
                pltpu.VMEM((n_tp, 1, 2 * rows), F32),
                pltpu.VMEM((n_tp, rows // 128, 128), F32),
                pltpu.VMEM((2 * n_vp, rows // 128, 128), F32),
                pltpu.VMEM((n_vp, slab, width), F32),
                pltpu.VMEM((n_tp, 1, 256), F32),
                pltpu.VMEM((n_vp, slab, width), F32),
                pltpu.VMEM((n_vp * n_tp, rows // 128, 128), F32),
                pltpu.VMEM((small, width), F32),
                pltpu.VMEM((2, small // 16 * 8, width), F32),
                pltpu.VMEM((2, small - small // 16 * 8, width), F32),
                pltpu.VMEM((width // (n_vp // 2), rows), F32),
                pltpu.VMEM((2, width, rows), F32),
                pltpu.VMEM((2, width, rows), F32),
                pltpu.VMEM((2, 2, width, rows), BF16),
                dma((7,)), dma((1,)), dma((5,)), dma((1,)), dma((1,)),
                dma((1,)), dma((n_round,)), dma((1,)), dma((1,)), dma((n_round,)),
                dma((1,)), dma((3,)), dma((1,)), dma((4,)), dma((1,)), dma((2,)), dma((2,)), dma((1,)), dma((1,)),
                pltpu.SemaphoreType.REGULAR((N_HOP,)),
                pltpu.VMEM((rows, width), BF16),
                pltpu.VMEM((1, rows), jnp.int32),
                pltpu.VMEM((4, 1, width), F32),
                dma((3,)),
            ],
            compiler_params=pltpu.CompilerParams(
                collective_id=0, has_side_effects=True, vmem_limit_bytes=57 * 1024 * 1024),
            cost_estimate=pl.CostEstimate(
                flops=4 * rows * n_block * n_tp * width, bytes_accessed=16 * n_block * n_tp * width, transcendentals=rows * n_block),
        )(hidden, lnf_gain[None, :], lnf_bias[None, :], emb_table, next_tok[None, :], eln_gain[None, :], eln_bias[None, :])
        n_piece = 5
        logprobs_t, log_sum, next_bf = pl.pallas_call(
            functools.partial(finish_kernel, n_piece),
            out_shape=(
                jax.ShapeDtypeStruct((n_block, rows), F32),
                jax.ShapeDtypeStruct((1, rows), F32),
                jax.ShapeDtypeStruct((rows, width), BF16),
            ),
            in_specs=[vmem, vmem, vmem],
            out_specs=(pl.BlockSpec(memory_space=pl.ANY),) * 3,
            scratch_shapes=[pltpu.VMEM((n_block, rows), F32), dma((n_piece + 2,))],
            compiler_params=pltpu.CompilerParams(vmem_limit_bytes=16 * 1024 * 1024),
        )(logits, lse, next_in)
        return logprobs_t.T, log_sum[0], next_bf

    return jax.shard_map(
        per_device,
        mesh=mesh,
        in_specs=(P("dp", "tp"), P("tp"), P("tp"), P("vp", "tp"), P("dp"), P("tp"), P("tp")),
        out_specs=(P("dp", ("vp", "tp")), P("dp"), P("dp", "tp")),
        check_vma=False,
    )
```

```python
import functools

import jax
import jax.numpy as jnp
from jax import lax
from jax.experimental import pallas as pl
from jax.experimental.pallas import tpu as pltpu
from jax.sharding import PartitionSpec as P

NORM_EPS = 1e-5
MESH = pl.DeviceIdType.MESH
CHUNK = 144
LANE = 128
F32 = jnp.float32
BF16 = jnp.bfloat16

OPP, LEFT, RIGHT, OWN = 0, 1, 2, 3
SIDE = 4
N_HOP = 5
FIRST = 1
STEP_OF_SLOT = (2, 3, 1, 0)


def head_kernel(n_vp, n_tp, n_block, full_width,
                hid_hbm, g_hbm, b_hbm, emb_ref, tok_hbm, eg_hbm, eb_hbm,
                logits_ref, lse_ref, next_ref,
                e_own, e_oth, e_out, e_in, send_f, recv_f, send_n, recv_l, recv_r,
                hx, xn, m_acc, s_acc, pick, st_ln, st_lse, st_all, rs_buf, row_st, ag_buf, st_dir,
                raw_src, raw_l, raw_r, slab_src, nb, nb_par, xnb,
                ld_sem, ex_send, ex_recv, hx_send, hx_recv,
                f_send, f_recv, n_send, r_send, in_recv,
                t_send, t_recv, v_send, v_recv, raw_send, raw_recv, sx_recv, nb_recv, d_recv, hop,
                hid_ref, tok_ref, vec_ref, in_sem):
    vp = lax.axis_index("vp")
    tp = lax.axis_index("tp")
    core = lax.rem(tp, 2)
    chip = tp // 2
    n_chip = n_tp // 2
    rows, width = hid_hbm.shape
    slab = rows // n_vp
    xslab = width // (n_vp // 2)
    left_chip = lax.rem(chip + n_chip - 1, n_chip)
    right_chip = lax.rem(chip + 1, n_chip)
    left = {"tp": left_chip * 2 + core}
    right = {"tp": right_chip * 2 + core}
    partner = {"tp": chip * 2 + 1 - core}
    y = lax.rem(vp, SIDE)
    z = vp // SIDE
    n_z = n_vp // SIDE
    near_by = ((y > 0, {"vp": lax.rem(vp + n_vp - 1, n_vp)}), (y < SIDE - 1, {"vp": lax.rem(vp + 1, n_vp)}),
               (z > 0, {"vp": lax.rem(vp + n_vp - SIDE, n_vp)}), (z < n_z - 1, {"vp": lax.rem(vp + SIDE, n_vp)}))
    n_near = sum(jnp.where(there, 1, 0) for there, _ in near_by)

    def tell_near(sem):
        for there, peer in near_by:
            @pl.when(there)
            def _(peer=peer):
                pl.semaphore_signal(sem, inc=1, device_id=peer, device_id_type=MESH)

    def hear_near(step):
        pl.semaphore_wait(hop.at[step], n_near)
        if step + 1 < N_HOP:
            tell_near(hop.at[step + 1])

    n_carry = n_vp // 2
    carries = vp < n_carry
    half = (n_block // 2) // CHUNK
    n_round = half + 1
    small = n_block - 2 * half * CHUNK
    small1 = (small // 16) * 8
    small2 = small - small1
    tail0 = 2 * half * CHUNK

    def piece(h, i):
        if isinstance(i, int) and i == 0:
            return (tail0, small1) if h == 0 else (tail0 + small1, small2)
        off = h * half * CHUNK + (i - 1) * CHUNK
        return (off if isinstance(i, int) else pl.multiple_of(off, 16)), CHUNK

    barrier = pltpu.get_barrier_semaphore()
    for j in range(1, n_tp):
        pl.semaphore_signal(barrier, inc=1, device_id={"tp": lax.rem(tp + j, n_tp)}, device_id_type=MESH)
    tell_near(barrier)

    parts = ((tail0, small), (0, tail0), (0, n_block))

    def load(slot, other, q, sem):
        blk = lax.rem(chip + STEP_OF_SLOT[slot], n_chip) * 2 + (1 - core if other else core)
        off, n = parts[q]
        src = emb_ref.at[pl.ds(pl.multiple_of(blk * n_block + off, 8), n), :]
        dst = (e_oth if other else e_own).at[slot, pl.ds(off, n), :]
        return pltpu.make_async_copy(src, dst, ld_sem.at[sem])

    hid_copy = pltpu.make_async_copy(hid_hbm, hid_ref, in_sem.at[0])
    tok_copy = pltpu.make_async_copy(tok_hbm, tok_ref, in_sem.at[1])
    hid_copy.start()
    for k, src in enumerate((g_hbm, b_hbm, eg_hbm, eb_hbm)):
        pltpu.make_async_copy(src, vec_ref.at[k], in_sem.at[2]).start()
    for slot in (RIGHT, LEFT):
        load(slot, True, 0, 0).start()
        load(slot, False, 0, 0).start()

    def total_load(ref, sem):
        pltpu.make_async_copy(ref, ref, sem).wait()

    def total_recv(ref, sem):
        pltpu.make_async_remote_copy(src_ref=ref, dst_ref=ref, send_sem=sem, recv_sem=sem,
                                     device_id=partner, device_id_type=MESH).wait_recv()

    def total_send(ref, sem):
        pltpu.make_async_remote_copy(src_ref=ref, dst_ref=ref, send_sem=sem, recv_sem=sem,
                                     device_id=partner, device_id_type=MESH).wait_send()

    hid_copy.wait()
    h_t = hid_ref[...].astype(F32).T
    hx[0, :, 0:rows] = h_t
    st_ln[tp, :, 0:rows] = jnp.sum(h_t, axis=0, keepdims=True)
    st_ln[tp, :, rows:2 * rows] = jnp.sum(h_t * h_t, axis=0, keepdims=True)

    def convert(slot, q):
        off, n = parts[q]
        e_out[slot, off:off + n, :] = e_oth[slot, off:off + n, :].astype(F32)

    total_load(e_own.at[0, pl.ds(0, 4 * small), :], ld_sem.at[0])
    for slot, q, sem in ((OPP, 2, 1), (LEFT, 1, 3), (RIGHT, 1, 3), (OWN, 2, 4)):
        load(slot, True, q, sem).start()
        if slot == OPP:
            load(slot, False, q, 2).start()
    for slot, q, sem in ((LEFT, 1, 5), (RIGHT, 1, 5), (OWN, 2, 6)):
        load(slot, False, q, sem).start()
    tok_copy.start()
    for slot in (RIGHT, LEFT):
        convert(slot, 0)
        off, n = piece(0 if slot == RIGHT else 1, 0)
        raw_src[off - tail0:off - tail0 + n, :] = e_own[slot, off:off + n, :].astype(F32)

    def raw_copy(slot, other):
        off, n = piece(0 if slot == RIGHT else 1, 0)
        src = e_out.at[slot, pl.ds(off, n), :] if other else raw_src.at[pl.ds(off - tail0, n), :]
        to = (right_chip if slot == RIGHT else left_chip) * 2 + (1 - core if other else core)
        return pltpu.make_async_remote_copy(
            src_ref=src, dst_ref=(raw_l if slot == RIGHT else raw_r).at[int(other)],
            send_sem=raw_send, recv_sem=raw_recv.at[int(slot == LEFT)],
            device_id={"tp": to}, device_id_type=MESH)

    pl.semaphore_wait(barrier, n_tp - 1 + n_near)

    def tp_start(buf, stage):
        for j in range(1, n_tp):
            pltpu.make_async_remote_copy(
                src_ref=buf.at[tp], dst_ref=buf.at[tp], send_sem=t_send, recv_sem=t_recv.at[stage],
                device_id={"tp": lax.rem(tp + j, n_tp)}, device_id_type=MESH).start()

    def tp_wait(buf, stage):
        total_recv(buf.at[pl.ds(0, n_tp - 1)], t_recv.at[stage])

    def tp_drain(buf):
        total_send(buf.at[pl.ds(0, n_tp - 1)], t_send)

    tp_start(st_ln, 0)
    for other in (False, True):
        for slot in (RIGHT, LEFT):
            raw_copy(slot, other).start()

    total_load(vec_ref, in_sem.at[2])
    hx[0, :, rows:rows + LANE] = jnp.broadcast_to(vec_ref[0], (LANE, width)).T
    hx[0, :, rows + LANE:rows + 256] = jnp.broadcast_to(vec_ref[1], (LANE, width)).T
    hx_copy = pltpu.make_async_remote_copy(
        src_ref=hx.at[0], dst_ref=hx.at[1], send_sem=hx_send, recv_sem=hx_recv,
        device_id=partner, device_id_type=MESH)
    hx_copy.start()
    tell_near(hop.at[0])

    def ex_copy(slot, q, sem):
        off, n = parts[q]
        return pltpu.make_async_remote_copy(
            src_ref=e_out.at[slot, pl.ds(off, n), :], dst_ref=e_in.at[slot, pl.ds(off, n), :],
            send_sem=ex_send, recv_sem=ex_recv.at[sem], device_id=partner, device_id_type=MESH)

    load(OPP, True, 2, 1).wait()
    for q in range(2):
        convert(OPP, q)
        ex_copy(OPP, q, q).start()
    for slot in (LEFT, RIGHT):
        ex_copy(slot, 0, 2).start()
    sides = e_oth.at[pl.ds(LEFT, 2), pl.ds(0, tail0), :]
    total_load(sides, ld_sem.at[3])
    for slot in (LEFT, RIGHT):
        convert(slot, 1)
        ex_copy(slot, 1, 3).start()
    load(OWN, True, 2, 4).wait()
    convert(OWN, 2)
    ex_copy(OWN, 2, 4).start()

    tp_wait(st_ln, 0)
    total = st_ln[0]
    for j in range(1, n_tp):
        total = total + st_ln[j]
    mean = total[:, 0:rows] / full_width
    rstd = lax.rsqrt(total[:, rows:2 * rows] / full_width - mean * mean + NORM_EPS)

    def norm(which):
        gain = hx[which, :, rows:rows + LANE]
        bias = hx[which, :, rows + LANE:rows + 256]
        for c in range(rows // LANE):
            cols = slice(c * LANE, c * LANE + LANE)
            xn[which, :, cols] = ((hx[which, :, cols] - mean[:, cols]) * rstd[:, cols] * gain + bias).astype(BF16)

    def slab_copy(d):
        return pltpu.make_async_remote_copy(
            src_ref=slab_src, dst_ref=nb.at[d, pl.ds(pl.multiple_of(vp * xslab, 8), xslab), :],
            send_sem=hx_send, recv_sem=sx_recv.at[d], device_id=right if d == 0 else left, device_id_type=MESH)

    norm(0)
    hx_copy.wait_send()

    @pl.when(carries)
    def _():
        slab_src[...] = xn[0, pl.ds(pl.multiple_of(vp * xslab, 32), xslab), :].astype(F32)
        for d in range(2):
            slab_copy(d).start()

    hx_copy.wait_recv()
    norm(1)

    def part_sum(slot, off, n):
        mine = e_own[slot, pl.ds(off, n), :]
        theirs = e_in[slot, pl.ds(off, n), :].astype(BF16)
        return (jnp.dot(mine, xn[0], preferred_element_type=F32)
                + jnp.dot(theirs, xn[1], preferred_element_type=F32))

    def f_copy(h, i):
        off, n = piece(h, i)
        return pltpu.make_async_remote_copy(
            src_ref=send_f.at[pl.ds(off, n), :], dst_ref=recv_f.at[pl.ds(off, n), :],
            send_sem=f_send, recv_sem=f_recv.at[i],
            device_id=left if h == 0 else right, device_id_type=MESH)

    def r_copy(h, i):
        off, n = piece(h, i)
        dst = (recv_r if h == 0 else recv_l).at[pl.ds(off, n), :]
        return pltpu.make_async_remote_copy(
            src_ref=recv_f.at[pl.ds(off, n), :], dst_ref=dst,
            send_sem=r_send, recv_sem=in_recv.at[i],
            device_id=left if h == 0 else right, device_id_type=MESH)

    def n_copy(h, i):
        off, n = piece(h, i)
        dst = (recv_l if h == 0 else recv_r).at[pl.ds(off, n), :]
        return pltpu.make_async_remote_copy(
            src_ref=send_n.at[pl.ds(off, n), :], dst_ref=dst,
            send_sem=n_send, recv_sem=in_recv.at[i],
            device_id=right if h == 0 else left, device_id_type=MESH)

    def far(i):
        for h in range(2):
            off, n = piece(h, i)
            send_f[pl.ds(off, n), :] = part_sum(OPP, off, n)
            f_copy(h, i).start()

    def near(i):
        for h in range(2):
            off, n = piece(h, i)
            send_n[pl.ds(off, n), :] = part_sum(RIGHT if h == 0 else LEFT, off, n)
            n_copy(h, i).start()

    def relay(i):
        mine = [part_sum(LEFT if h == 0 else RIGHT, *piece(h, i)) for h in range(2)]
        total_recv(recv_f.at[pl.ds(0, small if isinstance(i, int) else 2 * CHUNK), :], f_recv.at[i])
        for h in range(2):
            off, n = piece(h, i)
            recv_f[pl.ds(off, n), :] = recv_f[pl.ds(off, n), :] + mine[h]
            r_copy(h, i).start()

    def account(z):
        zr = z.reshape(z.shape[0] // 8, 8, rows)
        old = m_acc[...]
        new = jnp.maximum(old, jnp.max(zr, axis=0))
        m_acc[...] = new
        s_acc[...] = s_acc[...] * jnp.exp(old - new) + jnp.sum(jnp.exp(zr - new[None]), axis=0)

    def settle_raw():
        for h in range(2):
            off, n = piece(h, 0)
            raw = raw_l if h == 0 else raw_r
            if h == 0:
                total_recv(recv_l.at[pl.ds(0, small), :], in_recv.at[0])
            mine = part_sum(OWN, off, n)
            total_recv(raw, raw_recv.at[h])
            for other in range(2):
                mine = mine + jnp.dot(raw[other].astype(BF16), xnb[h, other], preferred_element_type=F32)
            z = mine + (recv_r if h == 0 else recv_l)[off:off + n, :]
            account(z)
            logits_ref[off:off + n, :] = z

    def settle(i):
        mine = [part_sum(OWN, *piece(h, i)) for h in range(2)]
        total_recv(recv_l.at[pl.ds(0, 4 * CHUNK), :], in_recv.at[i])
        for h in range(2):
            off, n = piece(h, i)
            z = mine[h] + recv_l[pl.ds(off, n), :] + recv_r[pl.ds(off, n), :]
            account(z)
            logits_ref[pl.ds(off, n), :] = z

    tok_copy.wait()
    tok = jnp.broadcast_to(tok_ref[...], (LANE, rows)).T

    def gather(step):
        for other in range(2):
            blk_chip = lax.rem(chip + jnp.where(step == 0, STEP_OF_SLOT[0], jnp.where(
                step == 1, STEP_OF_SLOT[1], jnp.where(step == 2, STEP_OF_SLOT[2], STEP_OF_SLOT[3]))), n_chip)
            blk = blk_chip * 2 + (1 - core if other else core)
            base = vp * (n_tp * n_block) + blk * n_block
            ref = e_oth if other else e_own
            acc = pick[...]
            for off in range(0, n_block, 512):
                n = min(512, n_block - off)
                for o, k in ((off, n // LANE * LANE), (off + n // LANE * LANE, n % LANE)):
                    if k == 0:
                        continue
                    lane = lax.broadcasted_iota(jnp.int32, (rows, k), 1) + (base + o)
                    if k % LANE == 0:
                        want = jnp.concatenate([tok] * (k // LANE), axis=1) if k > LANE else tok
                    else:
                        want = tok[:, :k]
                    hot = jnp.where(want == lane, 1.0, 0.0).astype(BF16)
                    acc = acc + jnp.dot(hot, ref[step, o:o + k, :], preferred_element_type=F32)
            pick[...] = acc

    def v_copy(src, dst, stage, j):
        return pltpu.make_async_remote_copy(
            src_ref=src, dst_ref=dst, send_sem=v_send, recv_sem=v_recv.at[stage],
            device_id={"vp": lax.rem(vp + j, n_vp)}, device_id_type=MESH)

    def vp_start(buf, stage):
        for j in range(1, n_vp):
            v_copy(buf.at[vp], buf.at[vp], stage, j).start()

    def vp_wait(buf, stage):
        total_recv(buf.at[pl.ds(0, n_vp - 1)], v_recv.at[stage])

    def vp_drain(buf):
        total_send(buf.at[pl.ds(0, n_vp - 1)], v_send)

    def slabs_forward():
        hear_near(N_HOP - 1)

        @pl.when(carries)
        def _():
            own = pl.ds(pl.multiple_of(vp * xslab, 8), xslab)
            for d in range(2):
                slab_copy(d).wait_recv()
                for j in range(1, n_vp):
                    v_copy(nb.at[d, own, :], nb.at[d, own, :], 3, j).start()

    nb_copy = pltpu.make_async_remote_copy(
        src_ref=nb, dst_ref=nb_par, send_sem=hx_send, recv_sem=nb_recv, device_id=partner, device_id_type=MESH)

    def slabs_swap():
        @pl.when(carries)
        def _():
            total_send(nb.at[0, pl.ds(0, 2 * xslab), :], hx_send)
            total_recv(nb.at[:, pl.ds(0, width - xslab), :], v_recv.at[3])

        @pl.when(jnp.logical_not(carries))
        def _():
            total_recv(nb, v_recv.at[3])

        nb_copy.start()
        for d in range(2):
            xnb[d, 0] = nb[d].astype(BF16)

    def slabs_done():
        nb_copy.wait_recv()
        for d in range(2):
            xnb[d, 1] = nb_par[d].astype(BF16)

    def rows_scatter():
        @pl.when(carries)
        def _():
            total_send(send_f.at[pl.ds(0, 2 * (n_vp - 1) * xslab), :], v_send)

        for j in range(1, n_vp):
            peer = lax.rem(vp + j, n_vp)
            v_copy(pick.at[pl.ds(pl.multiple_of(peer * slab, 8), slab), :], rs_buf.at[vp], 0, j).start()
        rs_buf[vp] = pick[pl.ds(pl.multiple_of(vp * slab, 8), slab), :]

    def rows_stats():
        vp_wait(rs_buf, 0)
        tot = rs_buf[0]
        for j in range(1, n_vp):
            tot = tot + rs_buf[j]
        ag_buf[vp] = tot
        lane = lax.broadcasted_iota(jnp.int32, (slab, LANE), 1)
        both = jnp.where(lane == 0, jnp.sum(tot, axis=1, keepdims=True), jnp.sum(tot * tot, axis=1, keepdims=True)).T
        tp_drain(st_ln)
        row_st[tp] = jnp.zeros((1, 256), F32)
        row_st[tp, :, 0:slab] = both[0:1]
        row_st[tp, :, LANE:LANE + slab] = both[1:2]
        tp_start(row_st, 1)

    def rows_norm():
        tp_wait(row_st, 1)
        tp_drain(row_st)
        tot = row_st[0]
        for j in range(1, n_tp):
            tot = tot + row_st[j]
        mu = tot[:, 0:LANE] / full_width
        rs = lax.rsqrt(tot[:, LANE:256] / full_width - mu * mu + NORM_EPS)
        mu = jnp.broadcast_to(mu, (LANE, LANE)).T[0:slab, 0:1]
        rs = jnp.broadcast_to(rs, (LANE, LANE)).T[0:slab, 0:1]
        out = ((ag_buf[vp] - mu) * rs * vec_ref[2] + vec_ref[3]).astype(BF16)
        ag_buf[vp] = out.astype(F32)
        vp_drain(rs_buf)
        vp_start(ag_buf, 1)

    def rows_out():
        vp_wait(ag_buf, 1)
        for j in range(n_vp):
            next_ref[j * slab:(j + 1) * slab, :] = ag_buf[j].astype(BF16)

    pick[...] = jnp.zeros_like(pick)
    m_acc[...] = jnp.full_like(m_acc, -jnp.inf)
    s_acc[...] = jnp.zeros_like(s_acc)

    load(OPP, False, 2, 2).wait()
    for q in range(2):
        ex_copy(OPP, q, q).wait_recv()
        far(q)
        hear_near(q)
    total_recv(e_in.at[pl.ds(LEFT, 2), pl.ds(tail0, small), :], ex_recv.at[2])
    far(2)
    hear_near(2)
    relay(0)
    hear_near(3)
    total_load(sides, ld_sem.at[5])
    total_recv(e_in.at[pl.ds(LEFT, 2), pl.ds(0, tail0), :], ex_recv.at[3])
    load(OWN, False, 2, 6).wait()
    ex_copy(OWN, 2, 4).wait_recv()

    def raw_drain():
        total_send(e_in.at[0, pl.ds(0, 2 * small), :], raw_send)

    def at(i, when, *steps):
        @pl.when(i == when)
        def _():
            for step in steps:
                step()

    def round_body(i, carry):
        near(i)

        @pl.when(i + 2 < n_round)
        def _():
            far(i + 2)

        relay(i)
        at(i, 1, slabs_forward, raw_drain)

        @pl.when(i <= 2)
        def _():
            gather(2 * i - 2)
            gather(2 * i - 1)

        at(i, 3, rows_scatter)
        at(i, 4, slabs_swap, rows_stats)
        at(i, 5, slabs_done, settle_raw)
        at(i, 6, rows_norm)

        @pl.when(i >= 3)
        def _():
            settle(i - 2)

        return carry

    lax.fori_loop(1, n_round, round_body, 0)

    def last_body(i, carry):
        settle(i)
        return carry

    lax.fori_loop(n_round - 2, n_round, last_body, 0)

    def merge(buf, n):
        sums = buf[0:n]
        top = jnp.max(sums, axis=0)
        return top + jnp.log(jnp.sum(jnp.exp(sums - top[None]), axis=0))

    def put(dst, at, value):
        for k in range(rows // LANE):
            dst[at, k:k + 1, :] = value[:, k * LANE:k * LANE + LANE]

    m8 = m_acc[...]
    top = jnp.max(m8, axis=0, keepdims=True)
    put(st_lse, tp, top + jnp.log(jnp.sum(s_acc[...] * jnp.exp(m8 - top), axis=0, keepdims=True)))

    me = vp * n_tp + tp
    is_first = me == FIRST

    @pl.when(jnp.logical_not(is_first))
    def _():
        pltpu.make_async_remote_copy(
            src_ref=st_lse.at[tp], dst_ref=st_dir.at[me], send_sem=raw_send, recv_sem=d_recv,
            device_id={"vp": FIRST // n_tp, "tp": FIRST % n_tp}, device_id_type=MESH).start()

    def collect(to_chip):
        return pltpu.make_async_remote_copy(
            src_ref=st_lse.at[tp], dst_ref=st_lse.at[tp], send_sem=t_send, recv_sem=t_recv.at[2],
            device_id={"tp": to_chip * 2 + 1}, device_id_type=MESH)

    for to in range(n_chip):
        @pl.when(jnp.logical_or(chip != to, core == 0))
        def _(to=to):
            collect(to).start()

    rows_out()
    nb_copy.wait_send()
    total_send(e_out, ex_send)
    total_send(send_f, f_send)
    total_send(recv_f, r_send)
    total_send(send_n.at[pl.ds(0, tail0), :], n_send)
    vp_drain(ag_buf)

    def spread(to, to_core):
        return pltpu.make_async_remote_copy(
            src_ref=st_all.at[vp], dst_ref=st_all.at[vp], send_sem=v_send, recv_sem=v_recv.at[2],
            device_id={"vp": to, "tp": chip * 2 + to_core}, device_id_type=MESH)

    def is_first_at(to, to_core):
        return jnp.logical_and(to == FIRST // n_tp, chip * 2 + to_core == FIRST % n_tp)

    @pl.when(core == 1)
    def _():
        total_recv(st_lse.at[pl.ds(0, n_tp - 1)], t_recv.at[2])
        st_all[vp] = merge(st_lse, n_tp)
        for to in range(n_vp):
            @pl.when(jnp.logical_and(vp != to, jnp.logical_not(is_first_at(to, 1))))
            def _(to=to):
                spread(to, 1).start()
        for to in range(n_vp):
            spread(to, 0).start()
        total_send(st_lse.at[pl.ds(0, n_chip - 1)], t_send)

        @pl.when(jnp.logical_not(is_first))
        def _():
            total_recv(st_all.at[pl.ds(0, n_vp - 1)], v_recv.at[2])

    @pl.when(core == 0)
    def _():
        total_send(st_lse.at[pl.ds(0, n_chip)], t_send)
        total_recv(st_all.at[pl.ds(0, n_vp)], v_recv.at[2])

    def result(value):
        for k in range(rows // LANE):
            lse_ref[:, k * LANE:k * LANE + LANE] = value[k:k + 1, :]

    @pl.when(is_first)
    def _():
        put_row = st_lse[tp]
        st_dir[me] = put_row
        total_recv(st_dir.at[pl.ds(0, n_vp * n_tp - 1)], d_recv)
        result(merge(st_dir, n_vp * n_tp))

    @pl.when(jnp.logical_not(is_first))
    def _():
        result(merge(st_all, n_vp))
        total_send(st_lse.at[pl.ds(0, 1)], raw_send)

    sends = 2 * n_vp - 1
    short = jnp.logical_and(chip == FIRST % n_tp // 2, vp != FIRST // n_tp)

    @pl.when(jnp.logical_and(core == 1, short))
    def _():
        total_send(st_all.at[pl.ds(0, sends - 1)], v_send)

    @pl.when(jnp.logical_and(core == 1, jnp.logical_not(short)))
    def _():
        total_send(st_all.at[pl.ds(0, sends)], v_send)


def finish_kernel(n_piece, z_ref, lse_ref, next_ref, out_ref, sum_ref, row_ref, buf, sems):
    lse = lse_ref[...]
    n = z_ref.shape[0] // n_piece

    def put(j):
        part = pl.ds(j * n, n)
        return pltpu.make_async_copy(buf.at[part, :], out_ref.at[part, :], sems.at[j])

    small = [pltpu.make_async_copy(lse_ref, sum_ref, sems.at[n_piece]),
             pltpu.make_async_copy(next_ref, row_ref, sems.at[n_piece + 1])]
    for copy in small:
        copy.start()
    for j in range(n_piece):
        buf[j * n:(j + 1) * n, :] = z_ref[j * n:(j + 1) * n, :] - lse
        put(j).start()
    for copy in small:
        copy.wait()
    for j in range(n_piece):
        put(j).wait()


def solution(mesh):
    n_vp, n_tp = mesh.shape["vp"], mesh.shape["tp"]

    def per_device(hidden, lnf_gain, lnf_bias, emb_table, next_tok, eln_gain, eln_bias):
        rows, width = hidden.shape
        n_block = emb_table.shape[0] // n_tp
        slab = rows // n_vp
        n_round = n_block // 2 // CHUNK + 1
        small = n_block - 2 * (n_round - 1) * CHUNK
        dma = pltpu.SemaphoreType.DMA
        vmem = pl.BlockSpec(memory_space=pltpu.VMEM)
        logits, lse, next_in = pl.pallas_call(
            functools.partial(head_kernel, n_vp, n_tp, n_block, width * n_tp),
            out_shape=(
                pltpu.VMEM((n_block, rows), F32),
                pltpu.VMEM((1, rows), F32),
                pltpu.VMEM((rows, width), BF16),
            ),
            in_specs=[pl.BlockSpec(memory_space=pl.ANY)] * 7,
            out_specs=(vmem, vmem, vmem),
            scratch_shapes=[
                *[pltpu.VMEM((4, n_block, width), BF16)] * 2,
                *[pltpu.VMEM((4, n_block, width), F32)] * 2,
                *[pltpu.VMEM((n_block, rows), F32)] * 5,
                pltpu.VMEM((2, width, rows + 256), F32),
                pltpu.VMEM((2, width, rows), BF16),
                pltpu.VMEM((8, rows), F32),
                pltpu.VMEM((8, rows), F32),
                pltpu.VMEM((rows, width), F32),
                pltpu.VMEM((n_tp, 1, 2 * rows), F32),
                pltpu.VMEM((n_tp, rows // LANE, LANE), F32),
                pltpu.VMEM((2 * n_vp, rows // LANE, LANE), F32),
                pltpu.VMEM((n_vp, slab, width), F32),
                pltpu.VMEM((n_tp, 1, 256), F32),
                pltpu.VMEM((n_vp, slab, width), F32),
                pltpu.VMEM((n_vp * n_tp, rows // LANE, LANE), F32),
                pltpu.VMEM((small, width), F32),
                pltpu.VMEM((2, small // 16 * 8, width), F32),
                pltpu.VMEM((2, small - small // 16 * 8, width), F32),
                pltpu.VMEM((width // (n_vp // 2), rows), F32),
                pltpu.VMEM((2, width, rows), F32),
                pltpu.VMEM((2, width, rows), F32),
                pltpu.VMEM((2, 2, width, rows), BF16),
                dma((7,)), dma, dma((5,)), dma, dma,
                dma, dma((n_round,)), dma, dma, dma((n_round,)),
                dma, dma((3,)), dma, dma((4,)), dma, dma((2,)), dma((2,)), dma, dma,
                pltpu.SemaphoreType.REGULAR((N_HOP,)),
                pltpu.VMEM((rows, width), BF16),
                pltpu.VMEM((1, rows), jnp.int32),
                pltpu.VMEM((4, 1, width), F32),
                dma((3,)),
            ],
            compiler_params=pltpu.CompilerParams(
                collective_id=0, has_side_effects=True, vmem_limit_bytes=57 * 1024 * 1024),
            cost_estimate=pl.CostEstimate(
                flops=4 * rows * n_block * n_tp * width, bytes_accessed=16 * n_block * n_tp * width, transcendentals=rows * n_block),
        )(hidden, lnf_gain[None, :], lnf_bias[None, :], emb_table, next_tok[None, :], eln_gain[None, :], eln_bias[None, :])
        n_piece = 5
        logprobs_t, log_sum, next_bf = pl.pallas_call(
            functools.partial(finish_kernel, n_piece),
            out_shape=(
                jax.ShapeDtypeStruct((n_block, rows), F32),
                jax.ShapeDtypeStruct((1, rows), F32),
                jax.ShapeDtypeStruct((rows, width), BF16),
            ),
            in_specs=[vmem, vmem, vmem],
            out_specs=(pl.BlockSpec(memory_space=pl.ANY),) * 3,
            scratch_shapes=[pltpu.VMEM((n_block, rows), F32), dma((n_piece + 2,))],
            compiler_params=pltpu.CompilerParams(vmem_limit_bytes=16 * 1024 * 1024),
        )(logits, lse, next_in)
        return logprobs_t.T, log_sum[0], next_bf

    return jax.shard_map(
        per_device,
        mesh=mesh,
        in_specs=(P("dp", "tp"), P("tp"), P("tp"), P("vp", "tp"), P("dp"), P("tp"), P("tp")),
        out_specs=(P("dp", ("vp", "tp")), P("dp"), P("dp", "tp")),
        check_vma=False,
    )
```

```python
import functools

import jax
import jax.numpy as jnp
from jax import lax
from jax.experimental import pallas as pl
from jax.experimental.pallas import tpu as pltpu
from jax.sharding import PartitionSpec as P

NORM_EPS = 1e-5
MESH = pl.DeviceIdType.MESH
CHUNK = 144
LANE = 128
F32 = jnp.float32
BF16 = jnp.bfloat16

OPP, LEFT, RIGHT, OWN = 0, 1, 2, 3
SIDE = 4
N_HOP = 5
FIRST = 2
STEP_OF_SLOT = (2, 3, 1, 0)


def head_kernel(n_vp, n_tp, n_block, full_width,
                hid_hbm, g_hbm, b_hbm, emb_ref, tok_hbm, eg_hbm, eb_hbm,
                logits_ref, lse_ref, next_ref,
                e_own, e_oth, e_out, e_in, send_f, recv_f, send_n, recv_l, recv_r,
                hx, xn, m_acc, s_acc, pick, st_ln, st_lse, st_all, rs_buf, row_st, ag_buf, st_dir,
                raw_src, raw_l, raw_r, slab_src, nb, nb_par, xnb,
                ld_sem, ex_send, ex_recv, hx_send, hx_recv,
                f_send, f_recv, n_send, r_send, in_recv,
                t_send, t_recv, v_send, v_recv, raw_send, raw_recv, sx_recv, nb_recv, d_recv, hop,
                hid_ref, tok_ref, vec_ref, in_sem):
    vp = lax.axis_index("vp")
    tp = lax.axis_index("tp")
    core = lax.rem(tp, 2)
    chip = tp // 2
    n_chip = n_tp // 2
    rows, width = hid_hbm.shape
    slab = rows // n_vp
    xslab = width // (n_vp // 2)
    left_chip = lax.rem(chip + n_chip - 1, n_chip)
    right_chip = lax.rem(chip + 1, n_chip)
    left = {"tp": left_chip * 2 + core}
    right = {"tp": right_chip * 2 + core}
    partner = {"tp": chip * 2 + 1 - core}
    y = lax.rem(vp, SIDE)
    z = vp // SIDE
    n_z = n_vp // SIDE
    near_by = ((y > 0, {"vp": lax.rem(vp + n_vp - 1, n_vp)}), (y < SIDE - 1, {"vp": lax.rem(vp + 1, n_vp)}),
               (z > 0, {"vp": lax.rem(vp + n_vp - SIDE, n_vp)}), (z < n_z - 1, {"vp": lax.rem(vp + SIDE, n_vp)}))
    n_near = sum(jnp.where(there, 1, 0) for there, _ in near_by)

    def tell_near(sem):
        for there, peer in near_by:
            @pl.when(there)
            def _(peer=peer):
                pl.semaphore_signal(sem, inc=1, device_id=peer, device_id_type=MESH)

    def hear_near(step):
        pl.semaphore_wait(hop.at[step], n_near)
        if step + 1 < N_HOP:
            tell_near(hop.at[step + 1])

    n_carry = n_vp // 2
    carries = vp < n_carry
    half = (n_block // 2) // CHUNK
    n_round = half + 1
    small = n_block - 2 * half * CHUNK
    small1 = (small // 16) * 8
    small2 = small - small1
    tail0 = 2 * half * CHUNK

    def piece(h, i):
        if isinstance(i, int) and i == 0:
            return (tail0, small1) if h == 0 else (tail0 + small1, small2)
        off = h * half * CHUNK + (i - 1) * CHUNK
        return (off if isinstance(i, int) else pl.multiple_of(off, 16)), CHUNK

    barrier = pltpu.get_barrier_semaphore()
    for peer in (left, right, partner):
        pl.semaphore_signal(barrier, inc=1, device_id=peer, device_id_type=MESH)
    tell_near(barrier)

    parts = ((tail0, small), (0, tail0), (0, n_block))

    def load(slot, other, q, sem):
        blk = lax.rem(chip + STEP_OF_SLOT[slot], n_chip) * 2 + (1 - core if other else core)
        off, n = parts[q]
        src = emb_ref.at[pl.ds(pl.multiple_of(blk * n_block + off, 8), n), :]
        dst = (e_oth if other else e_own).at[slot, pl.ds(off, n), :]
        return pltpu.make_async_copy(src, dst, ld_sem.at[sem])

    hid_copy = pltpu.make_async_copy(hid_hbm, hid_ref, in_sem.at[0])
    tok_copy = pltpu.make_async_copy(tok_hbm, tok_ref, in_sem.at[1])
    hid_copy.start()
    for k, src in enumerate((g_hbm, b_hbm, eg_hbm, eb_hbm)):
        pltpu.make_async_copy(src, vec_ref.at[k], in_sem.at[2]).start()
    for slot in (RIGHT, LEFT):
        load(slot, True, 0, 0).start()
        load(slot, False, 0, 0).start()

    def total_load(ref, sem):
        pltpu.make_async_copy(ref, ref, sem).wait()

    def total_recv(ref, sem):
        pltpu.make_async_remote_copy(src_ref=ref, dst_ref=ref, send_sem=sem, recv_sem=sem,
                                     device_id=partner, device_id_type=MESH).wait_recv()

    def total_send(ref, sem):
        pltpu.make_async_remote_copy(src_ref=ref, dst_ref=ref, send_sem=sem, recv_sem=sem,
                                     device_id=partner, device_id_type=MESH).wait_send()

    hid_copy.wait()
    h_t = hid_ref[...].astype(F32).T
    hx[0, :, 0:rows] = h_t
    st_ln[core, :, 0:rows] = jnp.sum(h_t, axis=0, keepdims=True)
    st_ln[core, :, rows:2 * rows] = jnp.sum(h_t * h_t, axis=0, keepdims=True)

    def convert(slot, q):
        off, n = parts[q]
        e_out[slot, off:off + n, :] = e_oth[slot, off:off + n, :].astype(F32)

    total_load(e_own.at[0, pl.ds(0, 4 * small), :], ld_sem.at[0])
    for slot, q, sem in ((OPP, 2, 1), (LEFT, 1, 3), (RIGHT, 1, 3), (OWN, 2, 4)):
        load(slot, True, q, sem).start()
        if slot == OPP:
            load(slot, False, q, 2).start()
    for slot, q, sem in ((LEFT, 1, 5), (RIGHT, 1, 5), (OWN, 2, 6)):
        load(slot, False, q, sem).start()
    tok_copy.start()
    for slot in (RIGHT, LEFT):
        convert(slot, 0)
        off, n = piece(0 if slot == RIGHT else 1, 0)
        raw_src[off - tail0:off - tail0 + n, :] = e_own[slot, off:off + n, :].astype(F32)

    def raw_copy(slot, other):
        off, n = piece(0 if slot == RIGHT else 1, 0)
        src = e_out.at[slot, pl.ds(off, n), :] if other else raw_src.at[pl.ds(off - tail0, n), :]
        to = (right_chip if slot == RIGHT else left_chip) * 2 + (1 - core if other else core)
        return pltpu.make_async_remote_copy(
            src_ref=src, dst_ref=(raw_l if slot == RIGHT else raw_r).at[int(other)],
            send_sem=raw_send, recv_sem=raw_recv.at[int(slot == LEFT)],
            device_id={"tp": to}, device_id_type=MESH)

    pl.semaphore_wait(barrier, 3 + n_near)

    def tp_start(buf, stage):
        for j in range(1, n_tp):
            pltpu.make_async_remote_copy(
                src_ref=buf.at[tp], dst_ref=buf.at[tp], send_sem=t_send, recv_sem=t_recv.at[stage],
                device_id={"tp": lax.rem(tp + j, n_tp)}, device_id_type=MESH).start()

    def tp_wait(buf, stage):
        total_recv(buf.at[pl.ds(0, n_tp - 1)], t_recv.at[stage])

    def tp_drain(buf):
        total_send(buf.at[pl.ds(0, n_tp - 1)], t_send)

    def stat_copy(slot, to, sem):
        return pltpu.make_async_remote_copy(
            src_ref=st_ln.at[slot], dst_ref=st_ln.at[slot], send_sem=t_send, recv_sem=t_recv.at[sem],
            device_id=to, device_id_type=MESH)

    stat_copy(core, partner, 3).start()
    for slot in (RIGHT, LEFT):
        raw_copy(slot, False).start()
    for peer in (left, right, partner):
        pl.semaphore_signal(hop.at[N_HOP], inc=1, device_id=peer, device_id_type=MESH)

    total_load(vec_ref, in_sem.at[2])
    hx[0, :, rows:rows + LANE] = jnp.broadcast_to(vec_ref[0], (LANE, width)).T
    hx[0, :, rows + LANE:rows + 256] = jnp.broadcast_to(vec_ref[1], (LANE, width)).T
    hx_copy = pltpu.make_async_remote_copy(
        src_ref=hx.at[0], dst_ref=hx.at[1], send_sem=hx_send, recv_sem=hx_recv,
        device_id=partner, device_id_type=MESH)
    hx_copy.start()
    tell_near(hop.at[0])

    def ex_copy(slot, q, sem):
        off, n = parts[q]
        return pltpu.make_async_remote_copy(
            src_ref=e_out.at[slot, pl.ds(off, n), :], dst_ref=e_in.at[slot, pl.ds(off, n), :],
            send_sem=ex_send, recv_sem=ex_recv.at[sem], device_id=partner, device_id_type=MESH)

    load(OPP, True, 2, 1).wait()
    for q in range(2):
        convert(OPP, q)
        ex_copy(OPP, q, q).start()

    pl.semaphore_wait(hop.at[N_HOP], 3)
    total_recv(st_ln.at[0], t_recv.at[3])
    mine_at = n_chip + chip
    st_ln[mine_at] = st_ln[0] + st_ln[1]
    for peer in (left, right, {"tp": lax.rem(tp + n_chip, n_tp)}):
        stat_copy(mine_at, peer, 0).start()
    for slot in (RIGHT, LEFT):
        raw_copy(slot, True).start()

    for slot in (LEFT, RIGHT):
        ex_copy(slot, 0, 2).start()
    sides = e_oth.at[pl.ds(LEFT, 2), pl.ds(0, tail0), :]
    total_load(sides, ld_sem.at[3])
    for slot in (LEFT, RIGHT):
        convert(slot, 1)
        ex_copy(slot, 1, 3).start()
    load(OWN, True, 2, 4).wait()
    convert(OWN, 2)
    ex_copy(OWN, 2, 4).start()

    total_recv(st_ln.at[pl.ds(0, 3)], t_recv.at[0])
    total = st_ln[n_chip]
    for j in range(1, n_chip):
        total = total + st_ln[n_chip + j]
    mean = total[:, 0:rows] / full_width
    rstd = lax.rsqrt(total[:, rows:2 * rows] / full_width - mean * mean + NORM_EPS)

    def norm(which):
        gain = hx[which, :, rows:rows + LANE]
        bias = hx[which, :, rows + LANE:rows + 256]
        for c in range(rows // LANE):
            cols = slice(c * LANE, c * LANE + LANE)
            xn[which, :, cols] = ((hx[which, :, cols] - mean[:, cols]) * rstd[:, cols] * gain + bias).astype(BF16)

    def slab_copy(d):
        return pltpu.make_async_remote_copy(
            src_ref=slab_src, dst_ref=nb.at[d, pl.ds(pl.multiple_of(vp * xslab, 8), xslab), :],
            send_sem=hx_send, recv_sem=sx_recv.at[d], device_id=right if d == 0 else left, device_id_type=MESH)

    norm(0)
    hx_copy.wait_send()

    @pl.when(carries)
    def _():
        slab_src[...] = xn[0, pl.ds(pl.multiple_of(vp * xslab, 32), xslab), :].astype(F32)
        for d in range(2):
            slab_copy(d).start()

    hx_copy.wait_recv()
    norm(1)

    def part_sum(slot, off, n):
        mine = e_own[slot, pl.ds(off, n), :]
        theirs = e_in[slot, pl.ds(off, n), :].astype(BF16)
        return (jnp.dot(mine, xn[0], preferred_element_type=F32)
                + jnp.dot(theirs, xn[1], preferred_element_type=F32))

    def f_copy(h, i):
        off, n = piece(h, i)
        return pltpu.make_async_remote_copy(
            src_ref=send_f.at[pl.ds(off, n), :], dst_ref=recv_f.at[pl.ds(off, n), :],
            send_sem=f_send, recv_sem=f_recv.at[i],
            device_id=left if h == 0 else right, device_id_type=MESH)

    def r_copy(h, i):
        off, n = piece(h, i)
        dst = (recv_r if h == 0 else recv_l).at[pl.ds(off, n), :]
        return pltpu.make_async_remote_copy(
            src_ref=recv_f.at[pl.ds(off, n), :], dst_ref=dst,
            send_sem=r_send, recv_sem=in_recv.at[i],
            device_id=left if h == 0 else right, device_id_type=MESH)

    def n_copy(h, i):
        off, n = piece(h, i)
        dst = (recv_l if h == 0 else recv_r).at[pl.ds(off, n), :]
        return pltpu.make_async_remote_copy(
            src_ref=send_n.at[pl.ds(off, n), :], dst_ref=dst,
            send_sem=n_send, recv_sem=in_recv.at[i],
            device_id=right if h == 0 else left, device_id_type=MESH)

    def far(i):
        for h in range(2):
            off, n = piece(h, i)
            send_f[pl.ds(off, n), :] = part_sum(OPP, off, n)
            f_copy(h, i).start()

    def near(i):
        for h in range(2):
            off, n = piece(h, i)
            send_n[pl.ds(off, n), :] = part_sum(RIGHT if h == 0 else LEFT, off, n)
            n_copy(h, i).start()

    def relay(i):
        mine = [part_sum(LEFT if h == 0 else RIGHT, *piece(h, i)) for h in range(2)]
        total_recv(recv_f.at[pl.ds(0, small if isinstance(i, int) else 2 * CHUNK), :], f_recv.at[i])
        for h in range(2):
            off, n = piece(h, i)
            recv_f[pl.ds(off, n), :] = recv_f[pl.ds(off, n), :] + mine[h]
            r_copy(h, i).start()

    def account(z):
        zr = z.reshape(z.shape[0] // 8, 8, rows)
        old = m_acc[...]
        new = jnp.maximum(old, jnp.max(zr, axis=0))
        m_acc[...] = new
        s_acc[...] = s_acc[...] * jnp.exp(old - new) + jnp.sum(jnp.exp(zr - new[None]), axis=0)

    def settle_raw():
        for h in range(2):
            off, n = piece(h, 0)
            raw = raw_l if h == 0 else raw_r
            if h == 0:
                total_recv(recv_l.at[pl.ds(0, small), :], in_recv.at[0])
            mine = part_sum(OWN, off, n)
            total_recv(raw, raw_recv.at[h])
            for other in range(2):
                mine = mine + jnp.dot(raw[other].astype(BF16), xnb[h, other], preferred_element_type=F32)
            z = mine + (recv_r if h == 0 else recv_l)[off:off + n, :]
            account(z)
            logits_ref[off:off + n, :] = z

    def settle(i):
        mine = [part_sum(OWN, *piece(h, i)) for h in range(2)]
        total_recv(recv_l.at[pl.ds(0, 4 * CHUNK), :], in_recv.at[i])
        for h in range(2):
            off, n = piece(h, i)
            z = mine[h] + recv_l[pl.ds(off, n), :] + recv_r[pl.ds(off, n), :]
            account(z)
            logits_ref[pl.ds(off, n), :] = z

    tok_copy.wait()
    tok = jnp.broadcast_to(tok_ref[...], (LANE, rows)).T

    def gather(step):
        for other in range(2):
            blk_chip = lax.rem(chip + jnp.where(step == 0, STEP_OF_SLOT[0], jnp.where(
                step == 1, STEP_OF_SLOT[1], jnp.where(step == 2, STEP_OF_SLOT[2], STEP_OF_SLOT[3]))), n_chip)
            blk = blk_chip * 2 + (1 - core if other else core)
            base = vp * (n_tp * n_block) + blk * n_block
            ref = e_oth if other else e_own
            acc = pick[...]
            for off in range(0, n_block, 512):
                n = min(512, n_block - off)
                for o, k in ((off, n // LANE * LANE), (off + n // LANE * LANE, n % LANE)):
                    if k == 0:
                        continue
                    lane = lax.broadcasted_iota(jnp.int32, (rows, k), 1) + (base + o)
                    if k % LANE == 0:
                        want = jnp.concatenate([tok] * (k // LANE), axis=1) if k > LANE else tok
                    else:
                        want = tok[:, :k]
                    hot = jnp.where(want == lane, 1.0, 0.0).astype(BF16)
                    acc = acc + jnp.dot(hot, ref[step, o:o + k, :], preferred_element_type=F32)
            pick[...] = acc

    def v_copy(src, dst, stage, j):
        return pltpu.make_async_remote_copy(
            src_ref=src, dst_ref=dst, send_sem=v_send, recv_sem=v_recv.at[stage],
            device_id={"vp": lax.rem(vp + j, n_vp)}, device_id_type=MESH)

    def vp_start(buf, stage):
        for j in range(1, n_vp):
            v_copy(buf.at[vp], buf.at[vp], stage, j).start()

    def vp_wait(buf, stage):
        total_recv(buf.at[pl.ds(0, n_vp - 1)], v_recv.at[stage])

    def vp_drain(buf):
        total_send(buf.at[pl.ds(0, n_vp - 1)], v_send)

    def slabs_forward():
        hear_near(N_HOP - 1)

        @pl.when(carries)
        def _():
            own = pl.ds(pl.multiple_of(vp * xslab, 8), xslab)
            for d in range(2):
                slab_copy(d).wait_recv()
                for j in range(1, n_vp):
                    v_copy(nb.at[d, own, :], nb.at[d, own, :], 3, j).start()

    nb_copy = pltpu.make_async_remote_copy(
        src_ref=nb, dst_ref=nb_par, send_sem=hx_send, recv_sem=nb_recv, device_id=partner, device_id_type=MESH)

    def slabs_swap():
        @pl.when(carries)
        def _():
            total_send(nb.at[0, pl.ds(0, 2 * xslab), :], hx_send)
            total_recv(nb.at[:, pl.ds(0, width - xslab), :], v_recv.at[3])

        @pl.when(jnp.logical_not(carries))
        def _():
            total_recv(nb, v_recv.at[3])

        nb_copy.start()
        for d in range(2):
            xnb[d, 0] = nb[d].astype(BF16)

    def slabs_done():
        nb_copy.wait_recv()
        for d in range(2):
            xnb[d, 1] = nb_par[d].astype(BF16)

    def rows_scatter():
        @pl.when(carries)
        def _():
            total_send(send_f.at[pl.ds(0, 2 * (n_vp - 1) * xslab), :], v_send)

        for j in range(1, n_vp):
            peer = lax.rem(vp + j, n_vp)
            v_copy(pick.at[pl.ds(pl.multiple_of(peer * slab, 8), slab), :], rs_buf.at[vp], 0, j).start()
        rs_buf[vp] = pick[pl.ds(pl.multiple_of(vp * slab, 8), slab), :]

    def rows_stats():
        vp_wait(rs_buf, 0)
        tot = rs_buf[0]
        for j in range(1, n_vp):
            tot = tot + rs_buf[j]
        ag_buf[vp] = tot
        lane = lax.broadcasted_iota(jnp.int32, (slab, LANE), 1)
        both = jnp.where(lane == 0, jnp.sum(tot, axis=1, keepdims=True), jnp.sum(tot * tot, axis=1, keepdims=True)).T
        total_send(st_ln.at[pl.ds(0, 4)], t_send)
        row_st[tp] = jnp.zeros((1, 256), F32)
        row_st[tp, :, 0:slab] = both[0:1]
        row_st[tp, :, LANE:LANE + slab] = both[1:2]
        tp_start(row_st, 1)

    def rows_norm():
        tp_wait(row_st, 1)
        tp_drain(row_st)
        tot = row_st[0]
        for j in range(1, n_tp):
            tot = tot + row_st[j]
        mu = tot[:, 0:LANE] / full_width
        rs = lax.rsqrt(tot[:, LANE:256] / full_width - mu * mu + NORM_EPS)
        mu = jnp.broadcast_to(mu, (LANE, LANE)).T[0:slab, 0:1]
        rs = jnp.broadcast_to(rs, (LANE, LANE)).T[0:slab, 0:1]
        out = ((ag_buf[vp] - mu) * rs * vec_ref[2] + vec_ref[3]).astype(BF16)
        ag_buf[vp] = out.astype(F32)
        vp_drain(rs_buf)
        vp_start(ag_buf, 1)

    def rows_out():
        vp_wait(ag_buf, 1)
        for j in range(n_vp):
            next_ref[j * slab:(j + 1) * slab, :] = ag_buf[j].astype(BF16)

    pick[...] = jnp.zeros_like(pick)
    m_acc[...] = jnp.full_like(m_acc, -jnp.inf)
    s_acc[...] = jnp.zeros_like(s_acc)

    load(OPP, False, 2, 2).wait()
    for q in range(2):
        ex_copy(OPP, q, q).wait_recv()
        far(q)
        hear_near(q)
    total_recv(e_in.at[pl.ds(LEFT, 2), pl.ds(tail0, small), :], ex_recv.at[2])
    far(2)
    hear_near(2)
    relay(0)
    hear_near(3)
    total_load(sides, ld_sem.at[5])
    total_recv(e_in.at[pl.ds(LEFT, 2), pl.ds(0, tail0), :], ex_recv.at[3])
    load(OWN, False, 2, 6).wait()
    ex_copy(OWN, 2, 4).wait_recv()

    def raw_drain():
        total_send(e_in.at[0, pl.ds(0, 2 * small), :], raw_send)

    def at(i, when, *steps):
        @pl.when(i == when)
        def _():
            for step in steps:
                step()

    def round_body(i, carry):
        near(i)

        @pl.when(i + 2 < n_round)
        def _():
            far(i + 2)

        relay(i)
        at(i, 1, slabs_forward, raw_drain)

        @pl.when(i <= 2)
        def _():
            gather(2 * i - 2)
            gather(2 * i - 1)

        at(i, 3, rows_scatter)
        at(i, 4, slabs_swap, rows_stats)
        at(i, 5, slabs_done, settle_raw)
        at(i, 6, rows_norm)

        @pl.when(i >= 3)
        def _():
            settle(i - 2)

        return carry

    lax.fori_loop(1, n_round, round_body, 0)

    def last_body(i, carry):
        settle(i)
        return carry

    lax.fori_loop(n_round - 2, n_round, last_body, 0)

    def merge(buf, n):
        sums = buf[0:n]
        top = jnp.max(sums, axis=0)
        return top + jnp.log(jnp.sum(jnp.exp(sums - top[None]), axis=0))

    def put(dst, at, value):
        for k in range(rows // LANE):
            dst[at, k:k + 1, :] = value[:, k * LANE:k * LANE + LANE]

    m8 = m_acc[...]
    top = jnp.max(m8, axis=0, keepdims=True)
    put(st_lse, tp, top + jnp.log(jnp.sum(s_acc[...] * jnp.exp(m8 - top), axis=0, keepdims=True)))

    me = vp * n_tp + tp
    is_first = me < FIRST
    for first in range(FIRST):
        @pl.when(me != first)
        def _(first=first):
            pltpu.make_async_remote_copy(
                src_ref=st_lse.at[tp], dst_ref=st_dir.at[me], send_sem=raw_send, recv_sem=d_recv,
                device_id={"vp": 0, "tp": first}, device_id_type=MESH).start()

    def collect(to_chip):
        return pltpu.make_async_remote_copy(
            src_ref=st_lse.at[tp], dst_ref=st_lse.at[tp], send_sem=t_send, recv_sem=t_recv.at[2],
            device_id={"tp": to_chip * 2 + 1}, device_id_type=MESH)

    for to in range(n_chip):
        @pl.when(jnp.logical_or(chip != to, core == 0))
        def _(to=to):
            collect(to).start()

    rows_out()
    nb_copy.wait_send()
    total_send(e_out, ex_send)
    total_send(send_f, f_send)
    total_send(recv_f, r_send)
    total_send(send_n.at[pl.ds(0, tail0), :], n_send)
    vp_drain(ag_buf)

    def spread(to, to_core):
        return pltpu.make_async_remote_copy(
            src_ref=st_all.at[vp], dst_ref=st_all.at[vp], send_sem=v_send, recv_sem=v_recv.at[2],
            device_id={"vp": to, "tp": chip * 2 + to_core}, device_id_type=MESH)

    @pl.when(core == 1)
    def _():
        total_recv(st_lse.at[pl.ds(0, n_tp - 1)], t_recv.at[2])
        st_all[vp] = merge(st_lse, n_tp)
        for to in range(n_vp):
            @pl.when(jnp.logical_and(vp != to, jnp.logical_or(chip != 0, to != 0)))
            def _(to=to):
                spread(to, 1).start()
        for to in range(n_vp):
            @pl.when(jnp.logical_or(chip != 0, to != 0))
            def _(to=to):
                spread(to, 0).start()
        total_send(st_lse.at[pl.ds(0, n_chip - 1)], t_send)

        @pl.when(jnp.logical_not(is_first))
        def _():
            total_recv(st_all.at[pl.ds(0, n_vp - 1)], v_recv.at[2])

    @pl.when(core == 0)
    def _():
        total_send(st_lse.at[pl.ds(0, n_chip)], t_send)

        @pl.when(jnp.logical_not(is_first))
        def _():
            total_recv(st_all.at[pl.ds(0, n_vp)], v_recv.at[2])

    def result(value):
        for k in range(rows // LANE):
            lse_ref[:, k * LANE:k * LANE + LANE] = value[k:k + 1, :]

    @pl.when(is_first)
    def _():
        put_row = st_lse[tp]
        st_dir[me] = put_row
        total_recv(st_dir.at[pl.ds(0, n_vp * n_tp - 1)], d_recv)
        result(merge(st_dir, n_vp * n_tp))
        total_send(st_lse.at[pl.ds(0, FIRST - 1)], raw_send)

    @pl.when(jnp.logical_not(is_first))
    def _():
        result(merge(st_all, n_vp))
        total_send(st_lse.at[pl.ds(0, FIRST)], raw_send)

    sends = 2 * n_vp - 1
    for there, fewer in ((chip != 0, 0), (jnp.logical_and(chip == 0, vp == 0), 1), (jnp.logical_and(chip == 0, vp != 0), 2)):
        @pl.when(jnp.logical_and(core == 1, there))
        def _(fewer=fewer):
            total_send(st_all.at[pl.ds(0, sends - fewer)], v_send)


def finish_kernel(n_piece, z_ref, lse_ref, next_ref, out_ref, sum_ref, row_ref, buf, sems):
    lse = lse_ref[...]
    n = z_ref.shape[0] // n_piece

    def put(j):
        part = pl.ds(j * n, n)
        return pltpu.make_async_copy(buf.at[part, :], out_ref.at[part, :], sems.at[j])

    small = [pltpu.make_async_copy(lse_ref, sum_ref, sems.at[n_piece]),
             pltpu.make_async_copy(next_ref, row_ref, sems.at[n_piece + 1])]
    for copy in small:
        copy.start()
    for j in range(n_piece):
        buf[j * n:(j + 1) * n, :] = z_ref[j * n:(j + 1) * n, :] - lse
        put(j).start()
    for copy in small:
        copy.wait()
    for j in range(n_piece):
        put(j).wait()


def solution(mesh):
    n_vp, n_tp = mesh.shape["vp"], mesh.shape["tp"]

    def per_device(hidden, lnf_gain, lnf_bias, emb_table, next_tok, eln_gain, eln_bias):
        rows, width = hidden.shape
        n_block = emb_table.shape[0] // n_tp
        slab = rows // n_vp
        n_round = n_block // 2 // CHUNK + 1
        small = n_block - 2 * (n_round - 1) * CHUNK
        dma = pltpu.SemaphoreType.DMA
        vmem = pl.BlockSpec(memory_space=pltpu.VMEM)
        logits, lse, next_in = pl.pallas_call(
            functools.partial(head_kernel, n_vp, n_tp, n_block, width * n_tp),
            out_shape=(
                pltpu.VMEM((n_block, rows), F32),
                pltpu.VMEM((1, rows), F32),
                pltpu.VMEM((rows, width), BF16),
            ),
            in_specs=[pl.BlockSpec(memory_space=pl.ANY)] * 7,
            out_specs=(vmem, vmem, vmem),
            scratch_shapes=[
                *[pltpu.VMEM((4, n_block, width), BF16)] * 2,
                *[pltpu.VMEM((4, n_block, width), F32)] * 2,
                *[pltpu.VMEM((n_block, rows), F32)] * 5,
                pltpu.VMEM((2, width, rows + 256), F32),
                pltpu.VMEM((2, width, rows), BF16),
                pltpu.VMEM((8, rows), F32),
                pltpu.VMEM((8, rows), F32),
                pltpu.VMEM((rows, width), F32),
                pltpu.VMEM((n_tp, 1, 2 * rows), F32),
                pltpu.VMEM((n_tp, rows // LANE, LANE), F32),
                pltpu.VMEM((2 * n_vp, rows // LANE, LANE), F32),
                pltpu.VMEM((n_vp, slab, width), F32),
                pltpu.VMEM((n_tp, 1, 256), F32),
                pltpu.VMEM((n_vp, slab, width), F32),
                pltpu.VMEM((n_vp * n_tp, rows // LANE, LANE), F32),
                pltpu.VMEM((small, width), F32),
                pltpu.VMEM((2, small // 16 * 8, width), F32),
                pltpu.VMEM((2, small - small // 16 * 8, width), F32),
                pltpu.VMEM((width // (n_vp // 2), rows), F32),
                pltpu.VMEM((2, width, rows), F32),
                pltpu.VMEM((2, width, rows), F32),
                pltpu.VMEM((2, 2, width, rows), BF16),
                dma((7,)), dma, dma((5,)), dma, dma,
                dma, dma((n_round,)), dma, dma, dma((n_round,)),
                dma, dma((4,)), dma, dma((4,)), dma, dma((2,)), dma((2,)), dma, dma,
                pltpu.SemaphoreType.REGULAR((N_HOP + 1,)),
                pltpu.VMEM((rows, width), BF16),
                pltpu.VMEM((1, rows), jnp.int32),
                pltpu.VMEM((4, 1, width), F32),
                dma((3,)),
            ],
            compiler_params=pltpu.CompilerParams(
                collective_id=0, has_side_effects=True, vmem_limit_bytes=57 * 1024 * 1024),
            cost_estimate=pl.CostEstimate(
                flops=4 * rows * n_block * n_tp * width, bytes_accessed=16 * n_block * n_tp * width, transcendentals=rows * n_block),
        )(hidden, lnf_gain[None, :], lnf_bias[None, :], emb_table, next_tok[None, :], eln_gain[None, :], eln_bias[None, :])
        n_piece = 5
        logprobs_t, log_sum, next_bf = pl.pallas_call(
            functools.partial(finish_kernel, n_piece),
            out_shape=(
                jax.ShapeDtypeStruct((n_block, rows), F32),
                jax.ShapeDtypeStruct((1, rows), F32),
                jax.ShapeDtypeStruct((rows, width), BF16),
            ),
            in_specs=[vmem, vmem, vmem],
            out_specs=(pl.BlockSpec(memory_space=pl.ANY),) * 3,
            scratch_shapes=[pltpu.VMEM((n_block, rows), F32), dma((n_piece + 2,))],
            compiler_params=pltpu.CompilerParams(vmem_limit_bytes=16 * 1024 * 1024),
        )(logits, lse, next_in)
        return logprobs_t.T, log_sum[0], next_bf

    return jax.shard_map(
        per_device,
        mesh=mesh,
        in_specs=(P("dp", "tp"), P("tp"), P("tp"), P("vp", "tp"), P("dp"), P("tp"), P("tp")),
        out_specs=(P("dp", ("vp", "tp")), P("dp"), P("dp", "tp")),
        check_vma=False,
    )
```

```python
import functools

import jax
import jax.numpy as jnp
from jax import lax
from jax.experimental import pallas as pl
from jax.experimental.pallas import tpu as pltpu
from jax.sharding import PartitionSpec as P

NORM_EPS = 1e-5
MESH = pl.DeviceIdType.MESH
CHUNK = 144
LANE = 128
F32 = jnp.float32
BF16 = jnp.bfloat16

OPP, LEFT, RIGHT, OWN = 0, 1, 2, 3
SIDE = 4
N_HOP = 5
FIRST = 2
STEP_OF_SLOT = (2, 3, 1, 0)


def head_kernel(n_vp, n_tp, n_block, full_width,
                hid_hbm, g_hbm, b_hbm, emb_ref, tok_hbm, eg_hbm, eb_hbm,
                logits_ref, lse_ref, next_ref,
                e_own, e_oth, e_out, e_in, send_f, recv_f, send_n, recv_l, recv_r,
                hx, xn, m_acc, s_acc, pick, st_ln, st_lse, st_all, rs_buf, row_st, ag_buf, st_dir,
                raw_src, raw_l, raw_r, slab_src, nb, nb_par, xnb,
                ld_sem, ex_send, ex_recv, hx_send, hx_recv,
                f_send, f_recv, n_send, r_send, in_recv,
                t_send, t_recv, v_send, v_recv, raw_send, raw_recv, sx_recv, nb_recv, d_recv, hop,
                hid_ref, tok_ref, vec_ref, in_sem):
    vp = lax.axis_index("vp")
    tp = lax.axis_index("tp")
    core = lax.rem(tp, 2)
    chip = tp // 2
    n_chip = n_tp // 2
    rows, width = hid_hbm.shape
    slab = rows // n_vp
    xslab = width // (n_vp // 2)
    left_chip = lax.rem(chip + n_chip - 1, n_chip)
    right_chip = lax.rem(chip + 1, n_chip)
    left = {"tp": left_chip * 2 + core}
    right = {"tp": right_chip * 2 + core}
    partner = {"tp": chip * 2 + 1 - core}
    y = lax.rem(vp, SIDE)
    z = vp // SIDE
    n_z = n_vp // SIDE
    near_by = ((y > 0, {"vp": lax.rem(vp + n_vp - 1, n_vp)}), (y < SIDE - 1, {"vp": lax.rem(vp + 1, n_vp)}),
               (z > 0, {"vp": lax.rem(vp + n_vp - SIDE, n_vp)}), (z < n_z - 1, {"vp": lax.rem(vp + SIDE, n_vp)}))
    n_near = sum(jnp.where(there, 1, 0) for there, _ in near_by)

    def tell_near(sem):
        for there, peer in near_by:
            @pl.when(there)
            def _(peer=peer):
                pl.semaphore_signal(sem, inc=1, device_id=peer, device_id_type=MESH)

    def hear_near(step):
        pl.semaphore_wait(hop.at[step], n_near)
        if step + 1 < N_HOP:
            tell_near(hop.at[step + 1])

    n_carry = n_vp // 2
    carries = jnp.logical_or(vp < n_carry - 1, vp == n_carry)
    own_slab = pl.ds(pl.multiple_of(lax.min(vp, n_carry - 1) * xslab, 32), xslab)
    half = (n_block // 2) // CHUNK
    n_round = half + 1
    small = n_block - 2 * half * CHUNK
    small1 = (small // 16) * 8
    small2 = small - small1
    tail0 = 2 * half * CHUNK

    def piece(h, i):
        if isinstance(i, int) and i == 0:
            return (tail0, small1) if h == 0 else (tail0 + small1, small2)
        off = h * half * CHUNK + (i - 1) * CHUNK
        return (off if isinstance(i, int) else pl.multiple_of(off, 16)), CHUNK

    barrier = pltpu.get_barrier_semaphore()
    for peer in (left, right, partner):
        pl.semaphore_signal(barrier, inc=1, device_id=peer, device_id_type=MESH)
    tell_near(barrier)

    parts = ((tail0, small), (0, tail0), (0, n_block))

    def load(slot, other, q, sem):
        blk = lax.rem(chip + STEP_OF_SLOT[slot], n_chip) * 2 + (1 - core if other else core)
        off, n = parts[q]
        src = emb_ref.at[pl.ds(pl.multiple_of(blk * n_block + off, 8), n), :]
        dst = (e_oth if other else e_own).at[slot, pl.ds(off, n), :]
        return pltpu.make_async_copy(src, dst, ld_sem.at[sem])

    hid_copy = pltpu.make_async_copy(hid_hbm, hid_ref, in_sem.at[0])
    tok_copy = pltpu.make_async_copy(tok_hbm, tok_ref, in_sem.at[1])
    hid_copy.start()
    for k, src in enumerate((g_hbm, b_hbm, eg_hbm, eb_hbm)):
        pltpu.make_async_copy(src, vec_ref.at[k], in_sem.at[2]).start()
    for slot in (RIGHT, LEFT):
        load(slot, True, 0, 0).start()
        load(slot, False, 0, 0).start()

    def total_load(ref, sem):
        pltpu.make_async_copy(ref, ref, sem).wait()

    def total_recv(ref, sem):
        pltpu.make_async_remote_copy(src_ref=ref, dst_ref=ref, send_sem=sem, recv_sem=sem,
                                     device_id=partner, device_id_type=MESH).wait_recv()

    def total_send(ref, sem):
        pltpu.make_async_remote_copy(src_ref=ref, dst_ref=ref, send_sem=sem, recv_sem=sem,
                                     device_id=partner, device_id_type=MESH).wait_send()

    hid_copy.wait()
    h_t = hid_ref[...].astype(F32).T
    hx[0, :, 0:rows] = h_t
    st_ln[core, :, 0:rows] = jnp.sum(h_t, axis=0, keepdims=True)
    st_ln[core, :, rows:2 * rows] = jnp.sum(h_t * h_t, axis=0, keepdims=True)

    def convert(slot, q):
        off, n = parts[q]
        e_out[slot, off:off + n, :] = e_oth[slot, off:off + n, :].astype(F32)

    total_load(e_own.at[0, pl.ds(0, 4 * small), :], ld_sem.at[0])
    for slot, q, sem in ((OPP, 2, 1), (LEFT, 1, 3), (RIGHT, 1, 3), (OWN, 2, 4)):
        load(slot, True, q, sem).start()
        if slot == OPP:
            load(slot, False, q, 2).start()
    for slot, q, sem in ((LEFT, 1, 5), (RIGHT, 1, 5), (OWN, 2, 6)):
        load(slot, False, q, sem).start()
    tok_copy.start()
    for slot in (RIGHT, LEFT):
        convert(slot, 0)
        off, n = piece(0 if slot == RIGHT else 1, 0)
        raw_src[off - tail0:off - tail0 + n, :] = e_own[slot, off:off + n, :].astype(F32)

    def raw_copy(slot, other):
        off, n = piece(0 if slot == RIGHT else 1, 0)
        src = e_out.at[slot, pl.ds(off, n), :] if other else raw_src.at[pl.ds(off - tail0, n), :]
        to = (right_chip if slot == RIGHT else left_chip) * 2 + (1 - core if other else core)
        return pltpu.make_async_remote_copy(
            src_ref=src, dst_ref=(raw_l if slot == RIGHT else raw_r).at[int(other)],
            send_sem=raw_send, recv_sem=raw_recv.at[int(slot == LEFT)],
            device_id={"tp": to}, device_id_type=MESH)

    pl.semaphore_wait(barrier, 3 + n_near)

    def tp_start(buf, stage):
        for j in range(1, n_tp):
            pltpu.make_async_remote_copy(
                src_ref=buf.at[tp], dst_ref=buf.at[tp], send_sem=t_send, recv_sem=t_recv.at[stage],
                device_id={"tp": lax.rem(tp + j, n_tp)}, device_id_type=MESH).start()

    def tp_wait(buf, stage):
        total_recv(buf.at[pl.ds(0, n_tp - 1)], t_recv.at[stage])

    def tp_drain(buf):
        total_send(buf.at[pl.ds(0, n_tp - 1)], t_send)

    def stat_copy(slot, to, sem):
        return pltpu.make_async_remote_copy(
            src_ref=st_ln.at[slot], dst_ref=st_ln.at[slot], send_sem=t_send, recv_sem=t_recv.at[sem],
            device_id=to, device_id_type=MESH)

    stat_copy(core, partner, 3).start()
    for slot in (RIGHT, LEFT):
        raw_copy(slot, False).start()
    for peer in (left, right, partner):
        pl.semaphore_signal(hop.at[N_HOP], inc=1, device_id=peer, device_id_type=MESH)

    total_load(vec_ref, in_sem.at[2])
    hx[0, :, rows:rows + LANE] = jnp.broadcast_to(vec_ref[0], (LANE, width)).T
    hx[0, :, rows + LANE:rows + 256] = jnp.broadcast_to(vec_ref[1], (LANE, width)).T
    hx_copy = pltpu.make_async_remote_copy(
        src_ref=hx.at[0], dst_ref=hx.at[1], send_sem=hx_send, recv_sem=hx_recv,
        device_id=partner, device_id_type=MESH)
    hx_copy.start()
    tell_near(hop.at[0])

    def ex_copy(slot, q, sem):
        off, n = parts[q]
        return pltpu.make_async_remote_copy(
            src_ref=e_out.at[slot, pl.ds(off, n), :], dst_ref=e_in.at[slot, pl.ds(off, n), :],
            send_sem=ex_send, recv_sem=ex_recv.at[sem], device_id=partner, device_id_type=MESH)

    load(OPP, True, 2, 1).wait()
    for q in range(2):
        convert(OPP, q)
        ex_copy(OPP, q, q).start()

    pl.semaphore_wait(hop.at[N_HOP], 3)
    total_recv(st_ln.at[0], t_recv.at[3])
    mine_at = n_chip + chip
    st_ln[mine_at] = st_ln[0] + st_ln[1]
    for peer in (left, right, {"tp": lax.rem(tp + n_chip, n_tp)}):
        stat_copy(mine_at, peer, 0).start()
    for slot in (RIGHT, LEFT):
        raw_copy(slot, True).start()

    for slot in (LEFT, RIGHT):
        ex_copy(slot, 0, 2).start()
    sides = e_oth.at[pl.ds(LEFT, 2), pl.ds(0, tail0), :]
    total_load(sides, ld_sem.at[3])
    for slot in (LEFT, RIGHT):
        convert(slot, 1)
        ex_copy(slot, 1, 3).start()
    load(OWN, True, 2, 4).wait()
    convert(OWN, 2)
    ex_copy(OWN, 2, 4).start()

    total_recv(st_ln.at[pl.ds(0, 3)], t_recv.at[0])
    total = st_ln[n_chip]
    for j in range(1, n_chip):
        total = total + st_ln[n_chip + j]
    mean = total[:, 0:rows] / full_width
    rstd = lax.rsqrt(total[:, rows:2 * rows] / full_width - mean * mean + NORM_EPS)

    def norm(which):
        gain = hx[which, :, rows:rows + LANE]
        bias = hx[which, :, rows + LANE:rows + 256]
        for c in range(rows // LANE):
            cols = slice(c * LANE, c * LANE + LANE)
            xn[which, :, cols] = ((hx[which, :, cols] - mean[:, cols]) * rstd[:, cols] * gain + bias).astype(BF16)

    def slab_copy(d):
        return pltpu.make_async_remote_copy(
            src_ref=slab_src, dst_ref=nb.at[d, own_slab, :],
            send_sem=hx_send, recv_sem=sx_recv.at[d], device_id=right if d == 0 else left, device_id_type=MESH)

    norm(0)
    hx_copy.wait_send()

    @pl.when(carries)
    def _():
        slab_src[...] = xn[0, own_slab, :].astype(F32)
        for d in range(2):
            slab_copy(d).start()

    hx_copy.wait_recv()
    norm(1)

    def part_sum(slot, off, n):
        mine = e_own[slot, pl.ds(off, n), :]
        theirs = e_in[slot, pl.ds(off, n), :].astype(BF16)
        return (jnp.dot(mine, xn[0], preferred_element_type=F32)
                + jnp.dot(theirs, xn[1], preferred_element_type=F32))

    def f_copy(h, i):
        off, n = piece(h, i)
        return pltpu.make_async_remote_copy(
            src_ref=send_f.at[pl.ds(off, n), :], dst_ref=recv_f.at[pl.ds(off, n), :],
            send_sem=f_send, recv_sem=f_recv.at[i],
            device_id=left if h == 0 else right, device_id_type=MESH)

    def r_copy(h, i):
        off, n = piece(h, i)
        dst = (recv_r if h == 0 else recv_l).at[pl.ds(off, n), :]
        return pltpu.make_async_remote_copy(
            src_ref=recv_f.at[pl.ds(off, n), :], dst_ref=dst,
            send_sem=r_send, recv_sem=in_recv.at[i],
            device_id=left if h == 0 else right, device_id_type=MESH)

    def n_copy(h, i):
        off, n = piece(h, i)
        dst = (recv_l if h == 0 else recv_r).at[pl.ds(off, n), :]
        return pltpu.make_async_remote_copy(
            src_ref=send_n.at[pl.ds(off, n), :], dst_ref=dst,
            send_sem=n_send, recv_sem=in_recv.at[i],
            device_id=right if h == 0 else left, device_id_type=MESH)

    def far(i):
        for h in range(2):
            off, n = piece(h, i)
            send_f[pl.ds(off, n), :] = part_sum(OPP, off, n)
            f_copy(h, i).start()

    def near(i):
        for h in range(2):
            off, n = piece(h, i)
            send_n[pl.ds(off, n), :] = part_sum(RIGHT if h == 0 else LEFT, off, n)
            n_copy(h, i).start()

    def relay(i):
        mine = [part_sum(LEFT if h == 0 else RIGHT, *piece(h, i)) for h in range(2)]
        total_recv(recv_f.at[pl.ds(0, small if isinstance(i, int) else 2 * CHUNK), :], f_recv.at[i])
        for h in range(2):
            off, n = piece(h, i)
            recv_f[pl.ds(off, n), :] = recv_f[pl.ds(off, n), :] + mine[h]
            r_copy(h, i).start()

    def account(z):
        zr = z.reshape(z.shape[0] // 8, 8, rows)
        old = m_acc[...]
        new = jnp.maximum(old, jnp.max(zr, axis=0))
        m_acc[...] = new
        s_acc[...] = s_acc[...] * jnp.exp(old - new) + jnp.sum(jnp.exp(zr - new[None]), axis=0)

    def settle_raw():
        for h in range(2):
            off, n = piece(h, 0)
            raw = raw_l if h == 0 else raw_r
            if h == 0:
                total_recv(recv_l.at[pl.ds(0, small), :], in_recv.at[0])
            mine = part_sum(OWN, off, n)
            total_recv(raw, raw_recv.at[h])
            for other in range(2):
                mine = mine + jnp.dot(raw[other].astype(BF16), xnb[h, other], preferred_element_type=F32)
            z = mine + (recv_r if h == 0 else recv_l)[off:off + n, :]
            account(z)
            logits_ref[off:off + n, :] = z

    def settle(i):
        mine = [part_sum(OWN, *piece(h, i)) for h in range(2)]
        total_recv(recv_l.at[pl.ds(0, 4 * CHUNK), :], in_recv.at[i])
        for h in range(2):
            off, n = piece(h, i)
            z = mine[h] + recv_l[pl.ds(off, n), :] + recv_r[pl.ds(off, n), :]
            account(z)
            logits_ref[pl.ds(off, n), :] = z

    tok_copy.wait()
    tok = jnp.broadcast_to(tok_ref[...], (LANE, rows)).T

    def gather(step):
        for other in range(2):
            blk_chip = lax.rem(chip + jnp.where(step == 0, STEP_OF_SLOT[0], jnp.where(
                step == 1, STEP_OF_SLOT[1], jnp.where(step == 2, STEP_OF_SLOT[2], STEP_OF_SLOT[3]))), n_chip)
            blk = blk_chip * 2 + (1 - core if other else core)
            base = vp * (n_tp * n_block) + blk * n_block
            ref = e_oth if other else e_own
            acc = pick[...]
            for off in range(0, n_block, 512):
                n = min(512, n_block - off)
                for o, k in ((off, n // LANE * LANE), (off + n // LANE * LANE, n % LANE)):
                    if k == 0:
                        continue
                    lane = lax.broadcasted_iota(jnp.int32, (rows, k), 1) + (base + o)
                    if k % LANE == 0:
                        want = jnp.concatenate([tok] * (k // LANE), axis=1) if k > LANE else tok
                    else:
                        want = tok[:, :k]
                    hot = jnp.where(want == lane, 1.0, 0.0).astype(BF16)
                    acc = acc + jnp.dot(hot, ref[step, o:o + k, :], preferred_element_type=F32)
            pick[...] = acc

    def v_copy(src, dst, stage, j):
        return pltpu.make_async_remote_copy(
            src_ref=src, dst_ref=dst, send_sem=v_send, recv_sem=v_recv.at[stage],
            device_id={"vp": lax.rem(vp + j, n_vp)}, device_id_type=MESH)

    def vp_start(buf, stage):
        for j in range(1, n_vp):
            v_copy(buf.at[vp], buf.at[vp], stage, j).start()

    def vp_wait(buf, stage):
        total_recv(buf.at[pl.ds(0, n_vp - 1)], v_recv.at[stage])

    def vp_drain(buf):
        total_send(buf.at[pl.ds(0, n_vp - 1)], v_send)

    def slabs_forward():
        hear_near(N_HOP - 1)

        @pl.when(carries)
        def _():
            for d in range(2):
                slab_copy(d).wait_recv()
                for j in range(1, n_vp):
                    v_copy(nb.at[d, own_slab, :], nb.at[d, own_slab, :], 3, j).start()

    nb_copy = pltpu.make_async_remote_copy(
        src_ref=nb, dst_ref=nb_par, send_sem=hx_send, recv_sem=nb_recv, device_id=partner, device_id_type=MESH)

    def slabs_swap():
        @pl.when(carries)
        def _():
            total_send(nb.at[0, pl.ds(0, 2 * xslab), :], hx_send)
            total_recv(nb.at[:, pl.ds(0, width - xslab), :], v_recv.at[3])

        @pl.when(jnp.logical_not(carries))
        def _():
            total_recv(nb, v_recv.at[3])

        nb_copy.start()
        for d in range(2):
            xnb[d, 0] = nb[d].astype(BF16)

    def slabs_done():
        nb_copy.wait_recv()
        for d in range(2):
            xnb[d, 1] = nb_par[d].astype(BF16)

    def rows_scatter():
        @pl.when(carries)
        def _():
            total_send(send_f.at[pl.ds(0, 2 * (n_vp - 1) * xslab), :], v_send)

        for j in range(1, n_vp):
            peer = lax.rem(vp + j, n_vp)
            v_copy(pick.at[pl.ds(pl.multiple_of(peer * slab, 8), slab), :], rs_buf.at[vp], 0, j).start()
        rs_buf[vp] = pick[pl.ds(pl.multiple_of(vp * slab, 8), slab), :]

    def rows_stats():
        vp_wait(rs_buf, 0)
        tot = rs_buf[0]
        for j in range(1, n_vp):
            tot = tot + rs_buf[j]
        ag_buf[vp] = tot
        lane = lax.broadcasted_iota(jnp.int32, (slab, LANE), 1)
        both = jnp.where(lane == 0, jnp.sum(tot, axis=1, keepdims=True), jnp.sum(tot * tot, axis=1, keepdims=True)).T
        total_send(st_ln.at[pl.ds(0, 4)], t_send)
        row_st[tp] = jnp.zeros((1, 256), F32)
        row_st[tp, :, 0:slab] = both[0:1]
        row_st[tp, :, LANE:LANE + slab] = both[1:2]
        tp_start(row_st, 1)

    def rows_norm():
        tp_wait(row_st, 1)
        tp_drain(row_st)
        tot = row_st[0]
        for j in range(1, n_tp):
            tot = tot + row_st[j]
        mu = tot[:, 0:LANE] / full_width
        rs = lax.rsqrt(tot[:, LANE:256] / full_width - mu * mu + NORM_EPS)
        mu = jnp.broadcast_to(mu, (LANE, LANE)).T[0:slab, 0:1]
        rs = jnp.broadcast_to(rs, (LANE, LANE)).T[0:slab, 0:1]
        out = ((ag_buf[vp] - mu) * rs * vec_ref[2] + vec_ref[3]).astype(BF16)
        ag_buf[vp] = out.astype(F32)
        vp_drain(rs_buf)
        vp_start(ag_buf, 1)

    def rows_out():
        vp_wait(ag_buf, 1)
        for j in range(n_vp):
            next_ref[j * slab:(j + 1) * slab, :] = ag_buf[j].astype(BF16)

    pick[...] = jnp.zeros_like(pick)
    m_acc[...] = jnp.full_like(m_acc, -jnp.inf)
    s_acc[...] = jnp.zeros_like(s_acc)

    load(OPP, False, 2, 2).wait()
    for q in range(2):
        ex_copy(OPP, q, q).wait_recv()
        far(q)
        hear_near(q)
    total_recv(e_in.at[pl.ds(LEFT, 2), pl.ds(tail0, small), :], ex_recv.at[2])
    far(2)
    hear_near(2)
    relay(0)
    hear_near(3)
    total_load(sides, ld_sem.at[5])
    total_recv(e_in.at[pl.ds(LEFT, 2), pl.ds(0, tail0), :], ex_recv.at[3])
    load(OWN, False, 2, 6).wait()
    ex_copy(OWN, 2, 4).wait_recv()

    def raw_drain():
        total_send(e_in.at[0, pl.ds(0, 2 * small), :], raw_send)

    def at(i, when, *steps):
        @pl.when(i == when)
        def _():
            for step in steps:
                step()

    def round_body(i, carry):
        near(i)

        @pl.when(i + 2 < n_round)
        def _():
            far(i + 2)

        relay(i)
        at(i, 1, slabs_forward, raw_drain)

        @pl.when(i <= 2)
        def _():
            gather(2 * i - 2)
            gather(2 * i - 1)

        at(i, 3, rows_scatter)
        at(i, 4, slabs_swap, rows_stats)
        at(i, 5, slabs_done, settle_raw)
        at(i, 6, rows_norm)

        @pl.when(i >= 3)
        def _():
            settle(i - 2)

        return carry

    lax.fori_loop(1, n_round, round_body, 0)

    def last_body(i, carry):
        settle(i)
        return carry

    lax.fori_loop(n_round - 2, n_round, last_body, 0)

    def merge(buf, n):
        sums = buf[0:n]
        top = jnp.max(sums, axis=0)
        return top + jnp.log(jnp.sum(jnp.exp(sums - top[None]), axis=0))

    def put(dst, at, value):
        for k in range(rows // LANE):
            dst[at, k:k + 1, :] = value[:, k * LANE:k * LANE + LANE]

    m8 = m_acc[...]
    top = jnp.max(m8, axis=0, keepdims=True)
    put(st_lse, tp, top + jnp.log(jnp.sum(s_acc[...] * jnp.exp(m8 - top), axis=0, keepdims=True)))

    me = vp * n_tp + tp
    is_first = me < FIRST
    for first in reversed(range(FIRST)):
        @pl.when(me != first)
        def _(first=first):
            pltpu.make_async_remote_copy(
                src_ref=st_lse.at[tp], dst_ref=st_dir.at[me], send_sem=raw_send, recv_sem=d_recv,
                device_id={"vp": 0, "tp": first}, device_id_type=MESH).start()

    def collect(to_chip):
        return pltpu.make_async_remote_copy(
            src_ref=st_lse.at[tp], dst_ref=st_lse.at[tp], send_sem=t_send, recv_sem=t_recv.at[2],
            device_id={"tp": to_chip * 2 + 1}, device_id_type=MESH)

    for to in range(n_chip):
        @pl.when(jnp.logical_or(chip != to, core == 0))
        def _(to=to):
            collect(to).start()

    rows_out()
    nb_copy.wait_send()
    total_send(e_out, ex_send)
    total_send(send_f, f_send)
    total_send(recv_f, r_send)
    total_send(send_n.at[pl.ds(0, tail0), :], n_send)
    vp_drain(ag_buf)

    def spread(to, to_core):
        return pltpu.make_async_remote_copy(
            src_ref=st_all.at[vp], dst_ref=st_all.at[vp], send_sem=v_send, recv_sem=v_recv.at[2],
            device_id={"vp": to, "tp": chip * 2 + to_core}, device_id_type=MESH)

    @pl.when(core == 1)
    def _():
        total_recv(st_lse.at[pl.ds(0, n_tp - 1)], t_recv.at[2])
        st_all[vp] = merge(st_lse, n_tp)
        for to in range(n_vp):
            @pl.when(jnp.logical_and(vp != to, jnp.logical_or(chip != 0, to != 0)))
            def _(to=to):
                spread(to, 1).start()
        for to in range(n_vp):
            @pl.when(jnp.logical_or(chip != 0, to != 0))
            def _(to=to):
                spread(to, 0).start()
        total_send(st_lse.at[pl.ds(0, n_chip - 1)], t_send)

        @pl.when(jnp.logical_not(is_first))
        def _():
            total_recv(st_all.at[pl.ds(0, n_vp - 1)], v_recv.at[2])

    @pl.when(core == 0)
    def _():
        total_send(st_lse.at[pl.ds(0, n_chip)], t_send)

        @pl.when(jnp.logical_not(is_first))
        def _():
            total_recv(st_all.at[pl.ds(0, n_vp)], v_recv.at[2])

    def result(value):
        for k in range(rows // LANE):
            lse_ref[:, k * LANE:k * LANE + LANE] = value[k:k + 1, :]

    @pl.when(is_first)
    def _():
        put_row = st_lse[tp]
        st_dir[me] = put_row
        total_recv(st_dir.at[pl.ds(0, n_vp * n_tp - 1)], d_recv)
        result(merge(st_dir, n_vp * n_tp))
        total_send(st_lse.at[pl.ds(0, FIRST - 1)], raw_send)

    @pl.when(jnp.logical_not(is_first))
    def _():
        result(merge(st_all, n_vp))
        total_send(st_lse.at[pl.ds(0, FIRST)], raw_send)

    sends = 2 * n_vp - 1
    for there, fewer in ((chip != 0, 0), (jnp.logical_and(chip == 0, vp == 0), 1), (jnp.logical_and(chip == 0, vp != 0), 2)):
        @pl.when(jnp.logical_and(core == 1, there))
        def _(fewer=fewer):
            total_send(st_all.at[pl.ds(0, sends - fewer)], v_send)


def finish_kernel(n_piece, z_ref, lse_ref, next_ref, out_ref, sum_ref, row_ref, buf, sems):
    lse = lse_ref[...]
    n = z_ref.shape[0] // n_piece

    def put(j):
        part = pl.ds(j * n, n)
        return pltpu.make_async_copy(buf.at[part, :], out_ref.at[part, :], sems.at[j])

    small = [pltpu.make_async_copy(lse_ref, sum_ref, sems.at[n_piece]),
             pltpu.make_async_copy(next_ref, row_ref, sems.at[n_piece + 1])]
    for copy in small:
        copy.start()
    for j in range(n_piece):
        buf[j * n:(j + 1) * n, :] = z_ref[j * n:(j + 1) * n, :] - lse
        put(j).start()
    for copy in small:
        copy.wait()
    for j in range(n_piece):
        put(j).wait()


def solution(mesh):
    n_vp, n_tp = mesh.shape["vp"], mesh.shape["tp"]

    def per_device(hidden, lnf_gain, lnf_bias, emb_table, next_tok, eln_gain, eln_bias):
        rows, width = hidden.shape
        n_block = emb_table.shape[0] // n_tp
        slab = rows // n_vp
        n_round = n_block // 2 // CHUNK + 1
        small = n_block - 2 * (n_round - 1) * CHUNK
        dma = pltpu.SemaphoreType.DMA
        vmem = pl.BlockSpec(memory_space=pltpu.VMEM)
        logits, lse, next_in = pl.pallas_call(
            functools.partial(head_kernel, n_vp, n_tp, n_block, width * n_tp),
            out_shape=(
                pltpu.VMEM((n_block, rows), F32),
                pltpu.VMEM((1, rows), F32),
                pltpu.VMEM((rows, width), BF16),
            ),
            in_specs=[pl.BlockSpec(memory_space=pl.ANY)] * 7,
            out_specs=(vmem, vmem, vmem),
            scratch_shapes=[
                *[pltpu.VMEM((4, n_block, width), BF16)] * 2,
                *[pltpu.VMEM((4, n_block, width), F32)] * 2,
                *[pltpu.VMEM((n_block, rows), F32)] * 5,
                pltpu.VMEM((2, width, rows + 256), F32),
                pltpu.VMEM((2, width, rows), BF16),
                pltpu.VMEM((8, rows), F32),
                pltpu.VMEM((8, rows), F32),
                pltpu.VMEM((rows, width), F32),
                pltpu.VMEM((n_tp, 1, 2 * rows), F32),
                pltpu.VMEM((n_tp, rows // LANE, LANE), F32),
                pltpu.VMEM((2 * n_vp, rows // LANE, LANE), F32),
                pltpu.VMEM((n_vp, slab, width), F32),
                pltpu.VMEM((n_tp, 1, 256), F32),
                pltpu.VMEM((n_vp, slab, width), F32),
                pltpu.VMEM((n_vp * n_tp, rows // LANE, LANE), F32),
                pltpu.VMEM((small, width), F32),
                pltpu.VMEM((2, small // 16 * 8, width), F32),
                pltpu.VMEM((2, small - small // 16 * 8, width), F32),
                pltpu.VMEM((width // (n_vp // 2), rows), F32),
                pltpu.VMEM((2, width, rows), F32),
                pltpu.VMEM((2, width, rows), F32),
                pltpu.VMEM((2, 2, width, rows), BF16),
                dma((7,)), dma, dma((5,)), dma, dma,
                dma, dma((n_round,)), dma, dma, dma((n_round,)),
                dma, dma((4,)), dma, dma((4,)), dma, dma((2,)), dma((2,)), dma, dma,
                pltpu.SemaphoreType.REGULAR((N_HOP + 1,)),
                pltpu.VMEM((rows, width), BF16),
                pltpu.VMEM((1, rows), jnp.int32),
                pltpu.VMEM((4, 1, width), F32),
                dma((3,)),
            ],
            compiler_params=pltpu.CompilerParams(
                collective_id=0, has_side_effects=True, vmem_limit_bytes=57 * 1024 * 1024),
            cost_estimate=pl.CostEstimate(
                flops=4 * rows * n_block * n_tp * width, bytes_accessed=16 * n_block * n_tp * width, transcendentals=rows * n_block),
        )(hidden, lnf_gain[None, :], lnf_bias[None, :], emb_table, next_tok[None, :], eln_gain[None, :], eln_bias[None, :])
        n_piece = 5
        logprobs_t, log_sum, next_bf = pl.pallas_call(
            functools.partial(finish_kernel, n_piece),
            out_shape=(
                jax.ShapeDtypeStruct((n_block, rows), F32),
                jax.ShapeDtypeStruct((1, rows), F32),
                jax.ShapeDtypeStruct((rows, width), BF16),
            ),
            in_specs=[vmem, vmem, vmem],
            out_specs=(pl.BlockSpec(memory_space=pl.ANY),) * 3,
            scratch_shapes=[pltpu.VMEM((n_block, rows), F32), dma((n_piece + 2,))],
            compiler_params=pltpu.CompilerParams(vmem_limit_bytes=16 * 1024 * 1024),
        )(logits, lse, next_in)
        return logprobs_t.T, log_sum[0], next_bf

    return jax.shard_map(
        per_device,
        mesh=mesh,
        in_specs=(P("dp", "tp"), P("tp"), P("tp"), P("vp", "tp"), P("dp"), P("tp"), P("tp")),
        out_specs=(P("dp", ("vp", "tp")), P("dp"), P("dp", "tp")),
        check_vma=False,
    )
```

```python
import functools

import jax
import jax.numpy as jnp
from jax import lax
from jax.experimental import pallas as pl
from jax.experimental.pallas import tpu as pltpu
from jax.sharding import PartitionSpec as P

NORM_EPS = 1e-5
MESH = pl.DeviceIdType.MESH
CHUNK = 144
LANE = 128
F32 = jnp.float32
BF16 = jnp.bfloat16

OPP, LEFT, RIGHT, OWN = 0, 1, 2, 3
SIDE = 4
N_HOP = 5
FIRST = 2
STEP_OF_SLOT = (2, 3, 1, 0)


def head_kernel(n_vp, n_tp, n_block, full_width,
                hid_hbm, g_hbm, b_hbm, emb_ref, tok_hbm, eg_hbm, eb_hbm,
                logits_ref, lse_ref, next_ref,
                e_own, e_oth, e_out, e_in, send_f, recv_f, send_n, recv_l, recv_r,
                hx, xn, m_acc, s_acc, pick, st_ln, st_lse, st_all, rs_buf, row_st, ag_buf, st_dir,
                raw_src, raw_l, raw_r, slab_src, nb, nb_par, xnb,
                ld_sem, ex_send, ex_recv, hx_send, hx_recv,
                f_send, f_recv, n_send, r_send, in_recv,
                t_send, t_recv, v_send, v_recv, raw_send, raw_recv, sx_recv, nb_recv, d_recv, hop,
                hid_ref, tok_ref, vec_ref, in_sem):
    vp = lax.axis_index("vp")
    tp = lax.axis_index("tp")
    core = lax.rem(tp, 2)
    chip = tp // 2
    n_chip = n_tp // 2
    rows, width = hid_hbm.shape
    slab = rows // n_vp
    xslab = width // (n_vp // 2)
    left_chip = lax.rem(chip + n_chip - 1, n_chip)
    right_chip = lax.rem(chip + 1, n_chip)
    left = {"tp": left_chip * 2 + core}
    right = {"tp": right_chip * 2 + core}
    partner = {"tp": chip * 2 + 1 - core}
    y = lax.rem(vp, SIDE)
    z = vp // SIDE
    n_z = n_vp // SIDE
    near_by = ((y > 0, {"vp": lax.rem(vp + n_vp - 1, n_vp)}), (y < SIDE - 1, {"vp": lax.rem(vp + 1, n_vp)}),
               (z > 0, {"vp": lax.rem(vp + n_vp - SIDE, n_vp)}), (z < n_z - 1, {"vp": lax.rem(vp + SIDE, n_vp)}))
    n_near = sum(jnp.where(there, 1, 0) for there, _ in near_by)

    def tell_near(sem):
        for there, peer in near_by:
            @pl.when(there)
            def _(peer=peer):
                pl.semaphore_signal(sem, inc=1, device_id=peer, device_id_type=MESH)

    def hear_near(step):
        pl.semaphore_wait(hop.at[step], n_near)
        if step + 1 < N_HOP:
            tell_near(hop.at[step + 1])

    n_carry = n_vp // 2
    carries = jnp.logical_or(vp < n_carry - 1, vp == n_carry)
    own_slab = pl.ds(pl.multiple_of(lax.min(vp, n_carry - 1) * xslab, 32), xslab)
    half = (n_block // 2) // CHUNK
    n_round = half + 1
    small = n_block - 2 * half * CHUNK
    small1 = (small // 16) * 8
    small2 = small - small1
    tail0 = 2 * half * CHUNK

    def piece(h, i):
        if isinstance(i, int) and i == 0:
            return (tail0, small1) if h == 0 else (tail0 + small1, small2)
        off = h * half * CHUNK + (i - 1) * CHUNK
        return (off if isinstance(i, int) else pl.multiple_of(off, 16)), CHUNK

    barrier = pltpu.get_barrier_semaphore()
    for peer in (left, right, partner):
        pl.semaphore_signal(barrier, inc=1, device_id=peer, device_id_type=MESH)
    tell_near(barrier)

    parts = ((tail0, small), (0, tail0), (0, n_block))

    def load(slot, other, q, sem):
        blk = lax.rem(chip + STEP_OF_SLOT[slot], n_chip) * 2 + (1 - core if other else core)
        off, n = parts[q]
        src = emb_ref.at[pl.ds(pl.multiple_of(blk * n_block + off, 8), n), :]
        dst = (e_oth if other else e_own).at[slot, pl.ds(off, n), :]
        return pltpu.make_async_copy(src, dst, ld_sem.at[sem])

    hid_copy = pltpu.make_async_copy(hid_hbm, hid_ref, in_sem.at[0])
    tok_copy = pltpu.make_async_copy(tok_hbm, tok_ref, in_sem.at[1])
    for slot in (RIGHT, LEFT):
        load(slot, True, 0, 0).start()
        load(slot, False, 0, 0).start()
    hid_copy.start()
    for k, src in enumerate((g_hbm, b_hbm, eg_hbm, eb_hbm)):
        pltpu.make_async_copy(src, vec_ref.at[k], in_sem.at[2]).start()

    def total_load(ref, sem):
        pltpu.make_async_copy(ref, ref, sem).wait()

    def total_recv(ref, sem):
        pltpu.make_async_remote_copy(src_ref=ref, dst_ref=ref, send_sem=sem, recv_sem=sem,
                                     device_id=partner, device_id_type=MESH).wait_recv()

    def total_send(ref, sem):
        pltpu.make_async_remote_copy(src_ref=ref, dst_ref=ref, send_sem=sem, recv_sem=sem,
                                     device_id=partner, device_id_type=MESH).wait_send()

    def convert(slot, q):
        off, n = parts[q]
        e_out[slot, off:off + n, :] = e_oth[slot, off:off + n, :].astype(F32)

    total_load(e_own.at[0, pl.ds(0, 4 * small), :], ld_sem.at[0])
    for slot, q, sem in ((OPP, 2, 1), (LEFT, 1, 3), (RIGHT, 1, 3), (OWN, 2, 4)):
        load(slot, True, q, sem).start()
        if slot == OPP:
            load(slot, False, q, 2).start()
    for slot, q, sem in ((LEFT, 1, 5), (RIGHT, 1, 5), (OWN, 2, 6)):
        load(slot, False, q, sem).start()
    tok_copy.start()
    for slot in (RIGHT, LEFT):
        convert(slot, 0)
        off, n = piece(0 if slot == RIGHT else 1, 0)
        raw_src[off - tail0:off - tail0 + n, :] = e_own[slot, off:off + n, :].astype(F32)

    def raw_copy(slot, other):
        off, n = piece(0 if slot == RIGHT else 1, 0)
        src = e_out.at[slot, pl.ds(off, n), :] if other else raw_src.at[pl.ds(off - tail0, n), :]
        to = (right_chip if slot == RIGHT else left_chip) * 2 + (1 - core if other else core)
        return pltpu.make_async_remote_copy(
            src_ref=src, dst_ref=(raw_l if slot == RIGHT else raw_r).at[int(other)],
            send_sem=raw_send, recv_sem=raw_recv.at[int(slot == LEFT)],
            device_id={"tp": to}, device_id_type=MESH)

    pl.semaphore_wait(barrier, 3 + n_near)

    def tp_start(buf, stage):
        for j in range(1, n_tp):
            pltpu.make_async_remote_copy(
                src_ref=buf.at[tp], dst_ref=buf.at[tp], send_sem=t_send, recv_sem=t_recv.at[stage],
                device_id={"tp": lax.rem(tp + j, n_tp)}, device_id_type=MESH).start()

    def tp_wait(buf, stage):
        total_recv(buf.at[pl.ds(0, n_tp - 1)], t_recv.at[stage])

    def tp_drain(buf):
        total_send(buf.at[pl.ds(0, n_tp - 1)], t_send)

    def stat_copy(slot, to, sem):
        return pltpu.make_async_remote_copy(
            src_ref=st_ln.at[slot], dst_ref=st_ln.at[slot], send_sem=t_send, recv_sem=t_recv.at[sem],
            device_id=to, device_id_type=MESH)

    for slot in (RIGHT, LEFT):
        raw_copy(slot, False).start()
    for peer in (left, right, partner):
        pl.semaphore_signal(hop.at[N_HOP], inc=1, device_id=peer, device_id_type=MESH)

    hid_copy.wait()
    h_t = hid_ref[...].astype(F32).T
    hx[0, :, 0:rows] = h_t
    st_ln[core, :, 0:rows] = jnp.sum(h_t, axis=0, keepdims=True)
    st_ln[core, :, rows:2 * rows] = jnp.sum(h_t * h_t, axis=0, keepdims=True)

    stat_copy(core, partner, 3).start()
    total_load(vec_ref, in_sem.at[2])
    hx[0, :, rows:rows + LANE] = jnp.broadcast_to(vec_ref[0], (LANE, width)).T
    hx[0, :, rows + LANE:rows + 256] = jnp.broadcast_to(vec_ref[1], (LANE, width)).T
    hx_copy = pltpu.make_async_remote_copy(
        src_ref=hx.at[0], dst_ref=hx.at[1], send_sem=hx_send, recv_sem=hx_recv,
        device_id=partner, device_id_type=MESH)
    hx_copy.start()
    tell_near(hop.at[0])

    def ex_copy(slot, q, sem):
        off, n = parts[q]
        return pltpu.make_async_remote_copy(
            src_ref=e_out.at[slot, pl.ds(off, n), :], dst_ref=e_in.at[slot, pl.ds(off, n), :],
            send_sem=ex_send, recv_sem=ex_recv.at[sem], device_id=partner, device_id_type=MESH)

    load(OPP, True, 2, 1).wait()
    for q in range(2):
        convert(OPP, q)
        ex_copy(OPP, q, q).start()

    pl.semaphore_wait(hop.at[N_HOP], 3)
    total_recv(st_ln.at[0], t_recv.at[3])
    mine_at = n_chip + chip
    st_ln[mine_at] = st_ln[0] + st_ln[1]
    for peer in (left, right, {"tp": lax.rem(tp + n_chip, n_tp)}):
        stat_copy(mine_at, peer, 0).start()
    for slot in (RIGHT, LEFT):
        raw_copy(slot, True).start()

    for slot in (LEFT, RIGHT):
        ex_copy(slot, 0, 2).start()
    sides = e_oth.at[pl.ds(LEFT, 2), pl.ds(0, tail0), :]
    total_load(sides, ld_sem.at[3])
    for slot in (LEFT, RIGHT):
        convert(slot, 1)
        ex_copy(slot, 1, 3).start()
    load(OWN, True, 2, 4).wait()
    convert(OWN, 2)
    ex_copy(OWN, 2, 4).start()

    total_recv(st_ln.at[pl.ds(0, 3)], t_recv.at[0])
    total = st_ln[n_chip]
    for j in range(1, n_chip):
        total = total + st_ln[n_chip + j]
    mean = total[:, 0:rows] / full_width
    rstd = lax.rsqrt(total[:, rows:2 * rows] / full_width - mean * mean + NORM_EPS)

    def norm(which):
        gain = hx[which, :, rows:rows + LANE]
        bias = hx[which, :, rows + LANE:rows + 256]
        for c in range(rows // LANE):
            cols = slice(c * LANE, c * LANE + LANE)
            xn[which, :, cols] = ((hx[which, :, cols] - mean[:, cols]) * rstd[:, cols] * gain + bias).astype(BF16)

    def slab_copy(d):
        return pltpu.make_async_remote_copy(
            src_ref=slab_src, dst_ref=nb.at[d, own_slab, :],
            send_sem=hx_send, recv_sem=sx_recv.at[d], device_id=right if d == 0 else left, device_id_type=MESH)

    norm(0)
    hx_copy.wait_send()

    @pl.when(carries)
    def _():
        slab_src[...] = xn[0, own_slab, :].astype(F32)
        for d in range(2):
            slab_copy(d).start()

    hx_copy.wait_recv()
    norm(1)

    def part_sum(slot, off, n):
        mine = e_own[slot, pl.ds(off, n), :]
        theirs = e_in[slot, pl.ds(off, n), :].astype(BF16)
        return (jnp.dot(mine, xn[0], preferred_element_type=F32)
                + jnp.dot(theirs, xn[1], preferred_element_type=F32))

    def f_copy(h, i):
        off, n = piece(h, i)
        return pltpu.make_async_remote_copy(
            src_ref=send_f.at[pl.ds(off, n), :], dst_ref=recv_f.at[pl.ds(off, n), :],
            send_sem=f_send, recv_sem=f_recv.at[i],
            device_id=left if h == 0 else right, device_id_type=MESH)

    def r_copy(h, i):
        off, n = piece(h, i)
        dst = (recv_r if h == 0 else recv_l).at[pl.ds(off, n), :]
        return pltpu.make_async_remote_copy(
            src_ref=recv_f.at[pl.ds(off, n), :], dst_ref=dst,
            send_sem=r_send, recv_sem=in_recv.at[i],
            device_id=left if h == 0 else right, device_id_type=MESH)

    def n_copy(h, i):
        off, n = piece(h, i)
        dst = (recv_l if h == 0 else recv_r).at[pl.ds(off, n), :]
        return pltpu.make_async_remote_copy(
            src_ref=send_n.at[pl.ds(off, n), :], dst_ref=dst,
            send_sem=n_send, recv_sem=in_recv.at[i],
            device_id=right if h == 0 else left, device_id_type=MESH)

    def far(i):
        for h in range(2):
            off, n = piece(h, i)
            send_f[pl.ds(off, n), :] = part_sum(OPP, off, n)
            f_copy(h, i).start()

    def near(i):
        for h in range(2):
            off, n = piece(h, i)
            send_n[pl.ds(off, n), :] = part_sum(RIGHT if h == 0 else LEFT, off, n)
            n_copy(h, i).start()

    def relay(i):
        mine = [part_sum(LEFT if h == 0 else RIGHT, *piece(h, i)) for h in range(2)]
        total_recv(recv_f.at[pl.ds(0, small if isinstance(i, int) else 2 * CHUNK), :], f_recv.at[i])
        for h in range(2):
            off, n = piece(h, i)
            recv_f[pl.ds(off, n), :] = recv_f[pl.ds(off, n), :] + mine[h]
            r_copy(h, i).start()

    def account(z):
        zr = z.reshape(z.shape[0] // 8, 8, rows)
        old = m_acc[...]
        new = jnp.maximum(old, jnp.max(zr, axis=0))
        m_acc[...] = new
        s_acc[...] = s_acc[...] * jnp.exp(old - new) + jnp.sum(jnp.exp(zr - new[None]), axis=0)

    def settle_raw():
        for h in range(2):
            off, n = piece(h, 0)
            raw = raw_l if h == 0 else raw_r
            if h == 0:
                total_recv(recv_l.at[pl.ds(0, small), :], in_recv.at[0])
            mine = part_sum(OWN, off, n)
            total_recv(raw, raw_recv.at[h])
            for other in range(2):
                mine = mine + jnp.dot(raw[other].astype(BF16), xnb[h, other], preferred_element_type=F32)
            z = mine + (recv_r if h == 0 else recv_l)[off:off + n, :]
            account(z)
            logits_ref[off:off + n, :] = z

    def settle(i):
        mine = [part_sum(OWN, *piece(h, i)) for h in range(2)]
        total_recv(recv_l.at[pl.ds(0, 4 * CHUNK), :], in_recv.at[i])
        for h in range(2):
            off, n = piece(h, i)
            z = mine[h] + recv_l[pl.ds(off, n), :] + recv_r[pl.ds(off, n), :]
            account(z)
            logits_ref[pl.ds(off, n), :] = z

    tok_copy.wait()
    tok = jnp.broadcast_to(tok_ref[...], (LANE, rows)).T

    def gather(step):
        for other in range(2):
            blk_chip = lax.rem(chip + jnp.where(step == 0, STEP_OF_SLOT[0], jnp.where(
                step == 1, STEP_OF_SLOT[1], jnp.where(step == 2, STEP_OF_SLOT[2], STEP_OF_SLOT[3]))), n_chip)
            blk = blk_chip * 2 + (1 - core if other else core)
            base = vp * (n_tp * n_block) + blk * n_block
            ref = e_oth if other else e_own
            acc = pick[...]
            for off in range(0, n_block, 512):
                n = min(512, n_block - off)
                for o, k in ((off, n // LANE * LANE), (off + n // LANE * LANE, n % LANE)):
                    if k == 0:
                        continue
                    lane = lax.broadcasted_iota(jnp.int32, (rows, k), 1) + (base + o)
                    if k % LANE == 0:
                        want = jnp.concatenate([tok] * (k // LANE), axis=1) if k > LANE else tok
                    else:
                        want = tok[:, :k]
                    hot = jnp.where(want == lane, 1.0, 0.0).astype(BF16)
                    acc = acc + jnp.dot(hot, ref[step, o:o + k, :], preferred_element_type=F32)
            pick[...] = acc

    def v_copy(src, dst, stage, j):
        return pltpu.make_async_remote_copy(
            src_ref=src, dst_ref=dst, send_sem=v_send, recv_sem=v_recv.at[stage],
            device_id={"vp": lax.rem(vp + j, n_vp)}, device_id_type=MESH)

    def vp_start(buf, stage):
        for j in range(1, n_vp):
            v_copy(buf.at[vp], buf.at[vp], stage, j).start()

    def vp_wait(buf, stage):
        total_recv(buf.at[pl.ds(0, n_vp - 1)], v_recv.at[stage])

    def vp_drain(buf):
        total_send(buf.at[pl.ds(0, n_vp - 1)], v_send)

    def slabs_forward():
        hear_near(N_HOP - 1)

        @pl.when(carries)
        def _():
            for d in range(2):
                slab_copy(d).wait_recv()
                for j in range(1, n_vp):
                    v_copy(nb.at[d, own_slab, :], nb.at[d, own_slab, :], 3, j).start()

    nb_copy = pltpu.make_async_remote_copy(
        src_ref=nb, dst_ref=nb_par, send_sem=hx_send, recv_sem=nb_recv, device_id=partner, device_id_type=MESH)

    def slabs_swap():
        @pl.when(carries)
        def _():
            total_send(nb.at[0, pl.ds(0, 2 * xslab), :], hx_send)
            total_recv(nb.at[:, pl.ds(0, width - xslab), :], v_recv.at[3])

        @pl.when(jnp.logical_not(carries))
        def _():
            total_recv(nb, v_recv.at[3])

        nb_copy.start()
        for d in range(2):
            xnb[d, 0] = nb[d].astype(BF16)

    def slabs_done():
        nb_copy.wait_recv()
        for d in range(2):
            xnb[d, 1] = nb_par[d].astype(BF16)

    def rows_scatter():
        @pl.when(carries)
        def _():
            total_send(send_f.at[pl.ds(0, 2 * (n_vp - 1) * xslab), :], v_send)

        for j in range(1, n_vp):
            peer = lax.rem(vp + j, n_vp)
            v_copy(pick.at[pl.ds(pl.multiple_of(peer * slab, 8), slab), :], rs_buf.at[vp], 0, j).start()
        rs_buf[vp] = pick[pl.ds(pl.multiple_of(vp * slab, 8), slab), :]

    def rows_stats():
        vp_wait(rs_buf, 0)
        tot = rs_buf[0]
        for j in range(1, n_vp):
            tot = tot + rs_buf[j]
        ag_buf[vp] = tot
        lane = lax.broadcasted_iota(jnp.int32, (slab, LANE), 1)
        both = jnp.where(lane == 0, jnp.sum(tot, axis=1, keepdims=True), jnp.sum(tot * tot, axis=1, keepdims=True)).T
        total_send(st_ln.at[pl.ds(0, 4)], t_send)
        row_st[tp] = jnp.zeros((1, 256), F32)
        row_st[tp, :, 0:slab] = both[0:1]
        row_st[tp, :, LANE:LANE + slab] = both[1:2]
        tp_start(row_st, 1)

    def rows_norm():
        tp_wait(row_st, 1)
        tp_drain(row_st)
        tot = row_st[0]
        for j in range(1, n_tp):
            tot = tot + row_st[j]
        mu = tot[:, 0:LANE] / full_width
        rs = lax.rsqrt(tot[:, LANE:256] / full_width - mu * mu + NORM_EPS)
        mu = jnp.broadcast_to(mu, (LANE, LANE)).T[0:slab, 0:1]
        rs = jnp.broadcast_to(rs, (LANE, LANE)).T[0:slab, 0:1]
        out = ((ag_buf[vp] - mu) * rs * vec_ref[2] + vec_ref[3]).astype(BF16)
        ag_buf[vp] = out.astype(F32)
        vp_drain(rs_buf)
        vp_start(ag_buf, 1)

    def rows_out():
        vp_wait(ag_buf, 1)
        for j in range(n_vp):
            next_ref[j * slab:(j + 1) * slab, :] = ag_buf[j].astype(BF16)

    pick[...] = jnp.zeros_like(pick)
    m_acc[...] = jnp.full_like(m_acc, -jnp.inf)
    s_acc[...] = jnp.zeros_like(s_acc)

    load(OPP, False, 2, 2).wait()
    for q in range(2):
        ex_copy(OPP, q, q).wait_recv()
        far(q)
        hear_near(q)
    total_recv(e_in.at[pl.ds(LEFT, 2), pl.ds(tail0, small), :], ex_recv.at[2])
    far(2)
    hear_near(2)
    relay(0)
    hear_near(3)
    total_load(sides, ld_sem.at[5])
    total_recv(e_in.at[pl.ds(LEFT, 2), pl.ds(0, tail0), :], ex_recv.at[3])
    load(OWN, False, 2, 6).wait()
    ex_copy(OWN, 2, 4).wait_recv()

    def raw_drain():
        total_send(e_in.at[0, pl.ds(0, 2 * small), :], raw_send)

    def at(i, when, *steps):
        @pl.when(i == when)
        def _():
            for step in steps:
                step()

    def round_body(i, carry):
        near(i)

        @pl.when(i + 2 < n_round)
        def _():
            far(i + 2)

        relay(i)
        at(i, 1, slabs_forward, raw_drain)

        @pl.when(i <= 2)
        def _():
            gather(2 * i - 2)
            gather(2 * i - 1)

        at(i, 3, rows_scatter)
        at(i, 4, slabs_swap, rows_stats)
        at(i, 5, slabs_done, settle_raw)
        at(i, 6, rows_norm)

        @pl.when(i >= 3)
        def _():
            settle(i - 2)

        return carry

    lax.fori_loop(1, n_round, round_body, 0)

    def last_body(i, carry):
        settle(i)
        return carry

    lax.fori_loop(n_round - 2, n_round, last_body, 0)

    def merge(buf, n):
        sums = buf[0:n]
        top = jnp.max(sums, axis=0)
        return top + jnp.log(jnp.sum(jnp.exp(sums - top[None]), axis=0))

    def put(dst, at, value):
        for k in range(rows // LANE):
            dst[at, k:k + 1, :] = value[:, k * LANE:k * LANE + LANE]

    m8 = m_acc[...]
    top = jnp.max(m8, axis=0, keepdims=True)
    put(st_lse, tp, top + jnp.log(jnp.sum(s_acc[...] * jnp.exp(m8 - top), axis=0, keepdims=True)))

    me = vp * n_tp + tp
    is_first = me < FIRST
    for first in reversed(range(FIRST)):
        @pl.when(me != first)
        def _(first=first):
            pltpu.make_async_remote_copy(
                src_ref=st_lse.at[tp], dst_ref=st_dir.at[me], send_sem=raw_send, recv_sem=d_recv,
                device_id={"vp": 0, "tp": first}, device_id_type=MESH).start()

    def collect(to_chip):
        return pltpu.make_async_remote_copy(
            src_ref=st_lse.at[tp], dst_ref=st_lse.at[tp], send_sem=t_send, recv_sem=t_recv.at[2],
            device_id={"tp": to_chip * 2 + 1}, device_id_type=MESH)

    for to in range(n_chip):
        @pl.when(jnp.logical_or(chip != to, core == 0))
        def _(to=to):
            collect(to).start()

    rows_out()
    nb_copy.wait_send()
    total_send(e_out, ex_send)
    total_send(send_f, f_send)
    total_send(recv_f, r_send)
    total_send(send_n.at[pl.ds(0, tail0), :], n_send)
    vp_drain(ag_buf)

    def spread(to, to_core):
        return pltpu.make_async_remote_copy(
            src_ref=st_all.at[vp], dst_ref=st_all.at[vp], send_sem=v_send, recv_sem=v_recv.at[2],
            device_id={"vp": to, "tp": chip * 2 + to_core}, device_id_type=MESH)

    @pl.when(core == 1)
    def _():
        total_recv(st_lse.at[pl.ds(0, n_tp - 1)], t_recv.at[2])
        st_all[vp] = merge(st_lse, n_tp)
        for to in range(n_vp):
            @pl.when(jnp.logical_and(vp != to, jnp.logical_or(chip != 0, to != 0)))
            def _(to=to):
                spread(to, 1).start()
        for to in range(n_vp):
            @pl.when(jnp.logical_or(chip != 0, to != 0))
            def _(to=to):
                spread(to, 0).start()
        total_send(st_lse.at[pl.ds(0, n_chip - 1)], t_send)

        @pl.when(jnp.logical_not(is_first))
        def _():
            total_recv(st_all.at[pl.ds(0, n_vp - 1)], v_recv.at[2])

    @pl.when(core == 0)
    def _():
        total_send(st_lse.at[pl.ds(0, n_chip)], t_send)

        @pl.when(jnp.logical_not(is_first))
        def _():
            total_recv(st_all.at[pl.ds(0, n_vp)], v_recv.at[2])

    def result(value):
        for k in range(rows // LANE):
            lse_ref[:, k * LANE:k * LANE + LANE] = value[k:k + 1, :]

    @pl.when(is_first)
    def _():
        put_row = st_lse[tp]
        st_dir[me] = put_row
        total_recv(st_dir.at[pl.ds(0, n_vp * n_tp - 1)], d_recv)
        result(merge(st_dir, n_vp * n_tp))
        total_send(st_lse.at[pl.ds(0, FIRST - 1)], raw_send)

    @pl.when(jnp.logical_not(is_first))
    def _():
        result(merge(st_all, n_vp))
        total_send(st_lse.at[pl.ds(0, FIRST)], raw_send)

    sends = 2 * n_vp - 1
    for there, fewer in ((chip != 0, 0), (jnp.logical_and(chip == 0, vp == 0), 1), (jnp.logical_and(chip == 0, vp != 0), 2)):
        @pl.when(jnp.logical_and(core == 1, there))
        def _(fewer=fewer):
            total_send(st_all.at[pl.ds(0, sends - fewer)], v_send)


def finish_kernel(n_piece, z_ref, lse_ref, next_ref, out_ref, sum_ref, row_ref, buf, sems):
    lse = lse_ref[...]
    unit = z_ref.shape[0] // 35
    edges = [unit * k for k in (0, 1, 3, 7, 14, 21, 28, 35)]

    def put(j):
        part = pl.ds(edges[j], edges[j + 1] - edges[j])
        return pltpu.make_async_copy(buf.at[part, :], out_ref.at[part, :], sems.at[j])

    small = [pltpu.make_async_copy(lse_ref, sum_ref, sems.at[n_piece]),
             pltpu.make_async_copy(next_ref, row_ref, sems.at[n_piece + 1])]
    for copy in small:
        copy.start()
    for j in range(n_piece):
        buf[edges[j]:edges[j + 1], :] = z_ref[edges[j]:edges[j + 1], :] - lse
        put(j).start()
    for copy in small:
        copy.wait()
    for j in range(n_piece):
        put(j).wait()


def solution(mesh):
    n_vp, n_tp = mesh.shape["vp"], mesh.shape["tp"]

    def per_device(hidden, lnf_gain, lnf_bias, emb_table, next_tok, eln_gain, eln_bias):
        rows, width = hidden.shape
        n_block = emb_table.shape[0] // n_tp
        slab = rows // n_vp
        n_round = n_block // 2 // CHUNK + 1
        small = n_block - 2 * (n_round - 1) * CHUNK
        dma = pltpu.SemaphoreType.DMA
        vmem = pl.BlockSpec(memory_space=pltpu.VMEM)
        logits, lse, next_in = pl.pallas_call(
            functools.partial(head_kernel, n_vp, n_tp, n_block, width * n_tp),
            out_shape=(
                pltpu.VMEM((n_block, rows), F32),
                pltpu.VMEM((1, rows), F32),
                pltpu.VMEM((rows, width), BF16),
            ),
            in_specs=[pl.BlockSpec(memory_space=pl.ANY)] * 7,
            out_specs=(vmem, vmem, vmem),
            scratch_shapes=[
                *[pltpu.VMEM((4, n_block, width), BF16)] * 2,
                *[pltpu.VMEM((4, n_block, width), F32)] * 2,
                *[pltpu.VMEM((n_block, rows), F32)] * 5,
                pltpu.VMEM((2, width, rows + 256), F32),
                pltpu.VMEM((2, width, rows), BF16),
                pltpu.VMEM((8, rows), F32),
                pltpu.VMEM((8, rows), F32),
                pltpu.VMEM((rows, width), F32),
                pltpu.VMEM((n_tp, 1, 2 * rows), F32),
                pltpu.VMEM((n_tp, rows // LANE, LANE), F32),
                pltpu.VMEM((2 * n_vp, rows // LANE, LANE), F32),
                pltpu.VMEM((n_vp, slab, width), F32),
                pltpu.VMEM((n_tp, 1, 256), F32),
                pltpu.VMEM((n_vp, slab, width), F32),
                pltpu.VMEM((n_vp * n_tp, rows // LANE, LANE), F32),
                pltpu.VMEM((small, width), F32),
                pltpu.VMEM((2, small // 16 * 8, width), F32),
                pltpu.VMEM((2, small - small // 16 * 8, width), F32),
                pltpu.VMEM((width // (n_vp // 2), rows), F32),
                pltpu.VMEM((2, width, rows), F32),
                pltpu.VMEM((2, width, rows), F32),
                pltpu.VMEM((2, 2, width, rows), BF16),
                dma((7,)), dma, dma((5,)), dma, dma,
                dma, dma((n_round,)), dma, dma, dma((n_round,)),
                dma, dma((4,)), dma, dma((4,)), dma, dma((2,)), dma((2,)), dma, dma,
                pltpu.SemaphoreType.REGULAR((N_HOP + 1,)),
                pltpu.VMEM((rows, width), BF16),
                pltpu.VMEM((1, rows), jnp.int32),
                pltpu.VMEM((4, 1, width), F32),
                dma((3,)),
            ],
            compiler_params=pltpu.CompilerParams(
                collective_id=0, has_side_effects=True, vmem_limit_bytes=57 * 1024 * 1024),
            cost_estimate=pl.CostEstimate(
                flops=4 * rows * n_block * n_tp * width, bytes_accessed=16 * n_block * n_tp * width, transcendentals=rows * n_block),
        )(hidden, lnf_gain[None, :], lnf_bias[None, :], emb_table, next_tok[None, :], eln_gain[None, :], eln_bias[None, :])
        n_piece = 7
        logprobs_t, log_sum, next_bf = pl.pallas_call(
            functools.partial(finish_kernel, n_piece),
            out_shape=(
                jax.ShapeDtypeStruct((n_block, rows), F32),
                jax.ShapeDtypeStruct((1, rows), F32),
                jax.ShapeDtypeStruct((rows, width), BF16),
            ),
            in_specs=[vmem, vmem, vmem],
            out_specs=(pl.BlockSpec(memory_space=pl.ANY),) * 3,
            scratch_shapes=[pltpu.VMEM((n_block, rows), F32), dma((n_piece + 2,))],
            compiler_params=pltpu.CompilerParams(vmem_limit_bytes=16 * 1024 * 1024),
        )(logits, lse, next_in)
        return logprobs_t.T, log_sum[0], next_bf

    return jax.shard_map(
        per_device,
        mesh=mesh,
        in_specs=(P("dp", "tp"), P("tp"), P("tp"), P("vp", "tp"), P("dp"), P("tp"), P("tp")),
        out_specs=(P("dp", ("vp", "tp")), P("dp"), P("dp", "tp")),
        check_vma=False,
    )
```

```python
import functools

import jax
import jax.numpy as jnp
from jax import lax
from jax.experimental import pallas as pl
from jax.experimental.pallas import tpu as pltpu
from jax.sharding import PartitionSpec as P

NORM_EPS = 1e-5
MESH = pl.DeviceIdType.MESH
CHUNK = 144
LANE = 128
F32 = jnp.float32
BF16 = jnp.bfloat16

OPP, LEFT, RIGHT, OWN = 0, 1, 2, 3
SIDE = 4
N_HOP = 5
FIRST = 2
STEP_OF_SLOT = (2, 3, 1, 0)


def head_kernel(n_vp, n_tp, n_block, full_width,
                hid_hbm, g_hbm, b_hbm, emb_ref, tok_hbm, eg_hbm, eb_hbm,
                logits_ref, lse_ref, next_ref,
                e_own, e_oth, e_out, e_in, send_f, recv_f, send_n, recv_l, recv_r,
                hx, xn, m_acc, s_acc, pick, st_ln, st_lse, st_all, rs_buf, row_st, ag_buf, st_dir,
                raw_src, raw_l, raw_r, slab_src, nb, nb_par, xnb,
                ld_sem, ex_send, ex_recv, hx_send, hx_recv,
                f_send, f_recv, n_send, r_send, in_recv,
                t_send, t_recv, v_send, v_recv, raw_send, raw_recv, sx_recv, nb_recv, d_recv, hop,
                hid_ref, tok_ref, vec_ref, in_sem):
    vp = lax.axis_index("vp")
    tp = lax.axis_index("tp")
    core = lax.rem(tp, 2)
    chip = tp // 2
    n_chip = n_tp // 2
    rows, width = hid_hbm.shape
    slab = rows // n_vp
    xslab = width // (n_vp // 2)
    left_chip = lax.rem(chip + n_chip - 1, n_chip)
    right_chip = lax.rem(chip + 1, n_chip)
    left = {"tp": left_chip * 2 + core}
    right = {"tp": right_chip * 2 + core}
    partner = {"tp": chip * 2 + 1 - core}
    y = lax.rem(vp, SIDE)
    z = vp // SIDE
    n_z = n_vp // SIDE
    near_by = ((y > 0, {"vp": lax.rem(vp + n_vp - 1, n_vp)}), (y < SIDE - 1, {"vp": lax.rem(vp + 1, n_vp)}),
               (z > 0, {"vp": lax.rem(vp + n_vp - SIDE, n_vp)}), (z < n_z - 1, {"vp": lax.rem(vp + SIDE, n_vp)}))
    n_near = sum(jnp.where(there, 1, 0) for there, _ in near_by)

    def tell_near(sem):
        for there, peer in near_by:
            @pl.when(there)
            def _(peer=peer):
                pl.semaphore_signal(sem, inc=1, device_id=peer, device_id_type=MESH)

    def hear_near(step):
        pl.semaphore_wait(hop.at[step], n_near)
        if step + 1 < N_HOP:
            tell_near(hop.at[step + 1])

    n_carry = n_vp // 2
    carries = jnp.logical_or(vp < n_carry - 1, vp == n_carry)
    own_slab = pl.ds(pl.multiple_of(lax.min(vp, n_carry - 1) * xslab, 32), xslab)
    half = (n_block // 2) // CHUNK
    n_round = half + 1
    small = n_block - 2 * half * CHUNK
    small2 = (small // 16) * 8
    small1 = small - small2
    tail0 = 2 * half * CHUNK

    def piece(h, i):
        if isinstance(i, int) and i == 0:
            return (tail0 + small2, small1) if h == 0 else (tail0, small2)
        off = h * half * CHUNK + (i - 1) * CHUNK
        return (off if isinstance(i, int) else pl.multiple_of(off, 16)), CHUNK

    barrier = pltpu.get_barrier_semaphore()
    for peer in (left, right, partner):
        pl.semaphore_signal(barrier, inc=1, device_id=peer, device_id_type=MESH)
    tell_near(barrier)

    parts = ((tail0, small), (0, tail0), (0, n_block))

    def load(slot, other, q, sem):
        blk = lax.rem(chip + STEP_OF_SLOT[slot], n_chip) * 2 + (1 - core if other else core)
        off, n = parts[q]
        src = emb_ref.at[pl.ds(pl.multiple_of(blk * n_block + off, 8), n), :]
        dst = (e_oth if other else e_own).at[slot, pl.ds(off, n), :]
        return pltpu.make_async_copy(src, dst, ld_sem.at[sem])

    hid_copy = pltpu.make_async_copy(hid_hbm, hid_ref, in_sem.at[0])
    tok_copy = pltpu.make_async_copy(tok_hbm, tok_ref, in_sem.at[1])
    for slot in (RIGHT, LEFT):
        load(slot, True, 0, 0).start()
        load(slot, False, 0, 0).start()
    hid_copy.start()
    for k, src in enumerate((g_hbm, b_hbm, eg_hbm, eb_hbm)):
        pltpu.make_async_copy(src, vec_ref.at[k], in_sem.at[2]).start()

    def total_load(ref, sem):
        pltpu.make_async_copy(ref, ref, sem).wait()

    def total_recv(ref, sem):
        pltpu.make_async_remote_copy(src_ref=ref, dst_ref=ref, send_sem=sem, recv_sem=sem,
                                     device_id=partner, device_id_type=MESH).wait_recv()

    def total_send(ref, sem):
        pltpu.make_async_remote_copy(src_ref=ref, dst_ref=ref, send_sem=sem, recv_sem=sem,
                                     device_id=partner, device_id_type=MESH).wait_send()

    def convert(slot, q):
        off, n = parts[q]
        e_out[slot, off:off + n, :] = e_oth[slot, off:off + n, :].astype(F32)

    total_load(e_own.at[0, pl.ds(0, 4 * small), :], ld_sem.at[0])
    for slot, q, sem in ((OPP, 2, 1), (LEFT, 1, 3), (RIGHT, 1, 3), (OWN, 2, 4)):
        load(slot, True, q, sem).start()
        if slot == OPP:
            load(slot, False, q, 2).start()
    for slot, q, sem in ((LEFT, 1, 5), (RIGHT, 1, 5), (OWN, 2, 6)):
        load(slot, False, q, sem).start()
    tok_copy.start()
    for slot in (RIGHT, LEFT):
        convert(slot, 0)
        off, n = piece(0 if slot == RIGHT else 1, 0)
        raw_src[off - tail0:off - tail0 + n, :] = e_own[slot, off:off + n, :].astype(F32)

    def raw_copy(slot, other):
        off, n = piece(0 if slot == RIGHT else 1, 0)
        src = e_out.at[slot, pl.ds(off, n), :] if other else raw_src.at[pl.ds(off - tail0, n), :]
        to = (right_chip if slot == RIGHT else left_chip) * 2 + (1 - core if other else core)
        return pltpu.make_async_remote_copy(
            src_ref=src, dst_ref=(raw_l if slot == RIGHT else raw_r).at[int(other)],
            send_sem=raw_send, recv_sem=raw_recv.at[int(slot == LEFT)],
            device_id={"tp": to}, device_id_type=MESH)

    pl.semaphore_wait(barrier, 3 + n_near)

    def tp_start(buf, stage):
        for j in range(1, n_tp):
            pltpu.make_async_remote_copy(
                src_ref=buf.at[tp], dst_ref=buf.at[tp], send_sem=t_send, recv_sem=t_recv.at[stage],
                device_id={"tp": lax.rem(tp + j, n_tp)}, device_id_type=MESH).start()

    def tp_wait(buf, stage):
        total_recv(buf.at[pl.ds(0, n_tp - 1)], t_recv.at[stage])

    def tp_drain(buf):
        total_send(buf.at[pl.ds(0, n_tp - 1)], t_send)

    def stat_copy(slot, to, sem):
        return pltpu.make_async_remote_copy(
            src_ref=st_ln.at[slot], dst_ref=st_ln.at[slot], send_sem=t_send, recv_sem=t_recv.at[sem],
            device_id=to, device_id_type=MESH)

    for slot in (RIGHT, LEFT):
        raw_copy(slot, False).start()
    for peer in (left, right, partner):
        pl.semaphore_signal(hop.at[N_HOP], inc=1, device_id=peer, device_id_type=MESH)

    hid_copy.wait()
    h_t = hid_ref[...].astype(F32).T
    hx[0, :, 0:rows] = h_t
    st_ln[core, :, 0:rows] = jnp.sum(h_t, axis=0, keepdims=True)
    st_ln[core, :, rows:2 * rows] = jnp.sum(h_t * h_t, axis=0, keepdims=True)

    stat_copy(core, partner, 3).start()
    total_load(vec_ref, in_sem.at[2])
    hx[0, :, rows:rows + LANE] = jnp.broadcast_to(vec_ref[0], (LANE, width)).T
    hx[0, :, rows + LANE:rows + 256] = jnp.broadcast_to(vec_ref[1], (LANE, width)).T
    hx_copy = pltpu.make_async_remote_copy(
        src_ref=hx.at[0], dst_ref=hx.at[1], send_sem=hx_send, recv_sem=hx_recv,
        device_id=partner, device_id_type=MESH)
    hx_copy.start()
    tell_near(hop.at[0])

    def ex_copy(slot, q, sem):
        off, n = parts[q]
        return pltpu.make_async_remote_copy(
            src_ref=e_out.at[slot, pl.ds(off, n), :], dst_ref=e_in.at[slot, pl.ds(off, n), :],
            send_sem=ex_send, recv_sem=ex_recv.at[sem], device_id=partner, device_id_type=MESH)

    load(OPP, True, 2, 1).wait()
    for q in range(2):
        convert(OPP, q)
        ex_copy(OPP, q, q).start()

    pl.semaphore_wait(hop.at[N_HOP], 3)
    total_recv(st_ln.at[0], t_recv.at[3])
    mine_at = n_chip + chip
    st_ln[mine_at] = st_ln[0] + st_ln[1]
    for peer in (left, right, {"tp": lax.rem(tp + n_chip, n_tp)}):
        stat_copy(mine_at, peer, 0).start()
    for slot in (RIGHT, LEFT):
        raw_copy(slot, True).start()

    for slot in (LEFT, RIGHT):
        ex_copy(slot, 0, 2).start()
    sides = e_oth.at[pl.ds(LEFT, 2), pl.ds(0, tail0), :]
    total_load(sides, ld_sem.at[3])
    for slot in (LEFT, RIGHT):
        convert(slot, 1)
        ex_copy(slot, 1, 3).start()
    load(OWN, True, 2, 4).wait()
    convert(OWN, 2)
    ex_copy(OWN, 2, 4).start()

    total_recv(st_ln.at[pl.ds(0, 3)], t_recv.at[0])
    total = st_ln[n_chip]
    for j in range(1, n_chip):
        total = total + st_ln[n_chip + j]
    mean = total[:, 0:rows] / full_width
    rstd = lax.rsqrt(total[:, rows:2 * rows] / full_width - mean * mean + NORM_EPS)

    def norm(which):
        gain = hx[which, :, rows:rows + LANE]
        bias = hx[which, :, rows + LANE:rows + 256]
        for c in range(rows // LANE):
            cols = slice(c * LANE, c * LANE + LANE)
            xn[which, :, cols] = ((hx[which, :, cols] - mean[:, cols]) * rstd[:, cols] * gain + bias).astype(BF16)

    def slab_copy(d):
        return pltpu.make_async_remote_copy(
            src_ref=slab_src, dst_ref=nb.at[d, own_slab, :],
            send_sem=hx_send, recv_sem=sx_recv.at[d], device_id=right if d == 0 else left, device_id_type=MESH)

    norm(0)
    hx_copy.wait_send()

    @pl.when(carries)
    def _():
        slab_src[...] = xn[0, own_slab, :].astype(F32)
        for d in range(2):
            slab_copy(d).start()

    hx_copy.wait_recv()
    norm(1)

    def part_sum(slot, off, n):
        mine = e_own[slot, pl.ds(off, n), :]
        theirs = e_in[slot, pl.ds(off, n), :].astype(BF16)
        return (jnp.dot(mine, xn[0], preferred_element_type=F32)
                + jnp.dot(theirs, xn[1], preferred_element_type=F32))

    def f_copy(h, i):
        off, n = piece(h, i)
        return pltpu.make_async_remote_copy(
            src_ref=send_f.at[pl.ds(off, n), :], dst_ref=recv_f.at[pl.ds(off, n), :],
            send_sem=f_send, recv_sem=f_recv.at[i],
            device_id=left if h == 0 else right, device_id_type=MESH)

    def r_copy(h, i):
        off, n = piece(h, i)
        dst = (recv_r if h == 0 else recv_l).at[pl.ds(off, n), :]
        return pltpu.make_async_remote_copy(
            src_ref=recv_f.at[pl.ds(off, n), :], dst_ref=dst,
            send_sem=r_send, recv_sem=in_recv.at[i],
            device_id=left if h == 0 else right, device_id_type=MESH)

    def n_copy(h, i):
        off, n = piece(h, i)
        dst = (recv_l if h == 0 else recv_r).at[pl.ds(off, n), :]
        return pltpu.make_async_remote_copy(
            src_ref=send_n.at[pl.ds(off, n), :], dst_ref=dst,
            send_sem=n_send, recv_sem=in_recv.at[i],
            device_id=right if h == 0 else left, device_id_type=MESH)

    def far(i):
        for h in range(2):
            off, n = piece(h, i)
            send_f[pl.ds(off, n), :] = part_sum(OPP, off, n)
            f_copy(h, i).start()

    def near(i):
        for h in range(2):
            off, n = piece(h, i)
            send_n[pl.ds(off, n), :] = part_sum(RIGHT if h == 0 else LEFT, off, n)
            n_copy(h, i).start()

    def relay(i):
        mine = [part_sum(LEFT if h == 0 else RIGHT, *piece(h, i)) for h in range(2)]
        total_recv(recv_f.at[pl.ds(0, small if isinstance(i, int) else 2 * CHUNK), :], f_recv.at[i])
        for h in range(2):
            off, n = piece(h, i)
            recv_f[pl.ds(off, n), :] = recv_f[pl.ds(off, n), :] + mine[h]
            r_copy(h, i).start()

    def account(z):
        zr = z.reshape(z.shape[0] // 8, 8, rows)
        old = m_acc[...]
        new = jnp.maximum(old, jnp.max(zr, axis=0))
        m_acc[...] = new
        s_acc[...] = s_acc[...] * jnp.exp(old - new) + jnp.sum(jnp.exp(zr - new[None]), axis=0)

    def settle_raw():
        for h in range(2):
            off, n = piece(h, 0)
            raw = raw_l if h == 0 else raw_r
            if h == 0:
                total_recv(recv_l.at[pl.ds(0, small), :], in_recv.at[0])
            mine = part_sum(OWN, off, n)
            total_recv(raw, raw_recv.at[h])
            for other in range(2):
                mine = mine + jnp.dot(raw[other].astype(BF16), xnb[h, other], preferred_element_type=F32)
            z = mine + (recv_r if h == 0 else recv_l)[off:off + n, :]
            account(z)
            logits_ref[off:off + n, :] = z

    def settle(i):
        mine = [part_sum(OWN, *piece(h, i)) for h in range(2)]
        total_recv(recv_l.at[pl.ds(0, 4 * CHUNK), :], in_recv.at[i])
        for h in range(2):
            off, n = piece(h, i)
            z = mine[h] + recv_l[pl.ds(off, n), :] + recv_r[pl.ds(off, n), :]
            account(z)
            logits_ref[pl.ds(off, n), :] = z

    tok_copy.wait()
    tok = jnp.broadcast_to(tok_ref[...], (LANE, rows)).T

    def gather(step):
        for other in range(2):
            blk_chip = lax.rem(chip + jnp.where(step == 0, STEP_OF_SLOT[0], jnp.where(
                step == 1, STEP_OF_SLOT[1], jnp.where(step == 2, STEP_OF_SLOT[2], STEP_OF_SLOT[3]))), n_chip)
            blk = blk_chip * 2 + (1 - core if other else core)
            base = vp * (n_tp * n_block) + blk * n_block
            ref = e_oth if other else e_own
            acc = pick[...]
            for off in range(0, n_block, 512):
                n = min(512, n_block - off)
                for o, k in ((off, n // LANE * LANE), (off + n // LANE * LANE, n % LANE)):
                    if k == 0:
                        continue
                    lane = lax.broadcasted_iota(jnp.int32, (rows, k), 1) + (base + o)
                    if k % LANE == 0:
                        want = jnp.concatenate([tok] * (k // LANE), axis=1) if k > LANE else tok
                    else:
                        want = tok[:, :k]
                    hot = jnp.where(want == lane, 1.0, 0.0).astype(BF16)
                    acc = acc + jnp.dot(hot, ref[step, o:o + k, :], preferred_element_type=F32)
            pick[...] = acc

    def v_copy(src, dst, stage, j):
        return pltpu.make_async_remote_copy(
            src_ref=src, dst_ref=dst, send_sem=v_send, recv_sem=v_recv.at[stage],
            device_id={"vp": lax.rem(vp + j, n_vp)}, device_id_type=MESH)

    def vp_start(buf, stage):
        for j in range(1, n_vp):
            v_copy(buf.at[vp], buf.at[vp], stage, j).start()

    def vp_wait(buf, stage):
        total_recv(buf.at[pl.ds(0, n_vp - 1)], v_recv.at[stage])

    def vp_drain(buf):
        total_send(buf.at[pl.ds(0, n_vp - 1)], v_send)

    def slabs_forward():
        hear_near(N_HOP - 1)

        @pl.when(carries)
        def _():
            for d in range(2):
                slab_copy(d).wait_recv()
                for j in range(1, n_vp):
                    v_copy(nb.at[d, own_slab, :], nb.at[d, own_slab, :], 3, j).start()

    nb_copy = pltpu.make_async_remote_copy(
        src_ref=nb, dst_ref=nb_par, send_sem=hx_send, recv_sem=nb_recv, device_id=partner, device_id_type=MESH)

    def slabs_swap():
        @pl.when(carries)
        def _():
            total_send(nb.at[0, pl.ds(0, 2 * xslab), :], hx_send)
            total_recv(nb.at[:, pl.ds(0, width - xslab), :], v_recv.at[3])

        @pl.when(jnp.logical_not(carries))
        def _():
            total_recv(nb, v_recv.at[3])

        nb_copy.start()
        for d in range(2):
            xnb[d, 0] = nb[d].astype(BF16)

    def slabs_done():
        nb_copy.wait_recv()
        for d in range(2):
            xnb[d, 1] = nb_par[d].astype(BF16)

    def rows_scatter():
        @pl.when(carries)
        def _():
            total_send(send_f.at[pl.ds(0, 2 * (n_vp - 1) * xslab), :], v_send)

        for j in range(1, n_vp):
            peer = lax.rem(vp + j, n_vp)
            v_copy(pick.at[pl.ds(pl.multiple_of(peer * slab, 8), slab), :], rs_buf.at[vp], 0, j).start()
        rs_buf[vp] = pick[pl.ds(pl.multiple_of(vp * slab, 8), slab), :]

    def rows_stats():
        vp_wait(rs_buf, 0)
        tot = rs_buf[0]
        for j in range(1, n_vp):
            tot = tot + rs_buf[j]
        ag_buf[vp] = tot
        lane = lax.broadcasted_iota(jnp.int32, (slab, LANE), 1)
        both = jnp.where(lane == 0, jnp.sum(tot, axis=1, keepdims=True), jnp.sum(tot * tot, axis=1, keepdims=True)).T
        total_send(st_ln.at[pl.ds(0, 4)], t_send)
        row_st[tp] = jnp.zeros((1, 256), F32)
        row_st[tp, :, 0:slab] = both[0:1]
        row_st[tp, :, LANE:LANE + slab] = both[1:2]
        tp_start(row_st, 1)

    def rows_norm():
        tp_wait(row_st, 1)
        tp_drain(row_st)
        tot = row_st[0]
        for j in range(1, n_tp):
            tot = tot + row_st[j]
        mu = tot[:, 0:LANE] / full_width
        rs = lax.rsqrt(tot[:, LANE:256] / full_width - mu * mu + NORM_EPS)
        mu = jnp.broadcast_to(mu, (LANE, LANE)).T[0:slab, 0:1]
        rs = jnp.broadcast_to(rs, (LANE, LANE)).T[0:slab, 0:1]
        out = ((ag_buf[vp] - mu) * rs * vec_ref[2] + vec_ref[3]).astype(BF16)
        ag_buf[vp] = out.astype(F32)
        vp_drain(rs_buf)
        vp_start(ag_buf, 1)

    def rows_out():
        vp_wait(ag_buf, 1)
        for j in range(n_vp):
            next_ref[j * slab:(j + 1) * slab, :] = ag_buf[j].astype(BF16)

    pick[...] = jnp.zeros_like(pick)
    m_acc[...] = jnp.full_like(m_acc, -jnp.inf)
    s_acc[...] = jnp.zeros_like(s_acc)

    load(OPP, False, 2, 2).wait()
    for q in range(2):
        ex_copy(OPP, q, q).wait_recv()
        far(q)
        hear_near(q)
    total_recv(e_in.at[pl.ds(LEFT, 2), pl.ds(tail0, small), :], ex_recv.at[2])
    far(2)
    hear_near(2)
    relay(0)
    hear_near(3)
    total_load(sides, ld_sem.at[5])
    total_recv(e_in.at[pl.ds(LEFT, 2), pl.ds(0, tail0), :], ex_recv.at[3])
    load(OWN, False, 2, 6).wait()
    ex_copy(OWN, 2, 4).wait_recv()

    def raw_drain():
        total_send(e_in.at[0, pl.ds(0, 2 * small), :], raw_send)

    def at(i, when, *steps):
        @pl.when(i == when)
        def _():
            for step in steps:
                step()

    def round_body(i, carry):
        near(i)

        @pl.when(i + 2 < n_round)
        def _():
            far(i + 2)

        relay(i)
        at(i, 1, slabs_forward, raw_drain)

        @pl.when(i <= 2)
        def _():
            gather(2 * i - 2)
            gather(2 * i - 1)

        at(i, 3, rows_scatter)
        at(i, 4, slabs_swap, rows_stats)
        at(i, 5, slabs_done, settle_raw)
        at(i, 6, rows_norm)

        @pl.when(i >= 3)
        def _():
            settle(i - 2)

        return carry

    lax.fori_loop(1, n_round, round_body, 0)

    def last_body(i, carry):
        settle(i)
        return carry

    lax.fori_loop(n_round - 2, n_round, last_body, 0)

    def merge(buf, n):
        sums = buf[0:n]
        top = jnp.max(sums, axis=0)
        return top + jnp.log(jnp.sum(jnp.exp(sums - top[None]), axis=0))

    def put(dst, at, value):
        for k in range(rows // LANE):
            dst[at, k:k + 1, :] = value[:, k * LANE:k * LANE + LANE]

    m8 = m_acc[...]
    top = jnp.max(m8, axis=0, keepdims=True)
    put(st_lse, tp, top + jnp.log(jnp.sum(s_acc[...] * jnp.exp(m8 - top), axis=0, keepdims=True)))

    me = vp * n_tp + tp
    is_first = me < FIRST
    for first in reversed(range(FIRST)):
        @pl.when(me != first)
        def _(first=first):
            pltpu.make_async_remote_copy(
                src_ref=st_lse.at[tp], dst_ref=st_dir.at[me], send_sem=raw_send, recv_sem=d_recv,
                device_id={"vp": 0, "tp": first}, device_id_type=MESH).start()

    def collect(to_chip):
        return pltpu.make_async_remote_copy(
            src_ref=st_lse.at[tp], dst_ref=st_lse.at[tp], send_sem=t_send, recv_sem=t_recv.at[2],
            device_id={"tp": to_chip * 2 + 1}, device_id_type=MESH)

    for to in range(n_chip):
        @pl.when(jnp.logical_or(chip != to, core == 0))
        def _(to=to):
            collect(to).start()

    rows_out()
    nb_copy.wait_send()
    total_send(e_out, ex_send)
    total_send(send_f, f_send)
    total_send(recv_f, r_send)
    total_send(send_n.at[pl.ds(0, tail0), :], n_send)
    vp_drain(ag_buf)

    def spread(to, to_core):
        return pltpu.make_async_remote_copy(
            src_ref=st_all.at[vp], dst_ref=st_all.at[vp], send_sem=v_send, recv_sem=v_recv.at[2],
            device_id={"vp": to, "tp": chip * 2 + to_core}, device_id_type=MESH)

    @pl.when(core == 1)
    def _():
        total_recv(st_lse.at[pl.ds(0, n_tp - 1)], t_recv.at[2])
        st_all[vp] = merge(st_lse, n_tp)
        for to in range(n_vp):
            @pl.when(jnp.logical_and(vp != to, jnp.logical_or(chip != 0, to != 0)))
            def _(to=to):
                spread(to, 1).start()
        for to in range(n_vp):
            @pl.when(jnp.logical_or(chip != 0, to != 0))
            def _(to=to):
                spread(to, 0).start()
        total_send(st_lse.at[pl.ds(0, n_chip - 1)], t_send)

        @pl.when(jnp.logical_not(is_first))
        def _():
            total_recv(st_all.at[pl.ds(0, n_vp - 1)], v_recv.at[2])

    @pl.when(core == 0)
    def _():
        total_send(st_lse.at[pl.ds(0, n_chip)], t_send)

        @pl.when(jnp.logical_not(is_first))
        def _():
            total_recv(st_all.at[pl.ds(0, n_vp)], v_recv.at[2])

    def result(value):
        for k in range(rows // LANE):
            lse_ref[:, k * LANE:k * LANE + LANE] = value[k:k + 1, :]

    @pl.when(is_first)
    def _():
        put_row = st_lse[tp]
        st_dir[me] = put_row
        total_recv(st_dir.at[pl.ds(0, n_vp * n_tp - 1)], d_recv)
        result(merge(st_dir, n_vp * n_tp))
        total_send(st_lse.at[pl.ds(0, FIRST - 1)], raw_send)

    @pl.when(jnp.logical_not(is_first))
    def _():
        result(merge(st_all, n_vp))
        total_send(st_lse.at[pl.ds(0, FIRST)], raw_send)

    sends = 2 * n_vp - 1
    for there, fewer in ((chip != 0, 0), (jnp.logical_and(chip == 0, vp == 0), 1), (jnp.logical_and(chip == 0, vp != 0), 2)):
        @pl.when(jnp.logical_and(core == 1, there))
        def _(fewer=fewer):
            total_send(st_all.at[pl.ds(0, sends - fewer)], v_send)


def finish_kernel(n_piece, z_ref, lse_ref, next_ref, out_ref, sum_ref, row_ref, buf, sems):
    lse = lse_ref[...]
    unit = z_ref.shape[0] // 35
    edges = [unit * k for k in (0, 1, 3, 7, 14, 21, 28, 35)]

    def put(j):
        part = pl.ds(edges[j], edges[j + 1] - edges[j])
        return pltpu.make_async_copy(buf.at[part, :], out_ref.at[part, :], sems.at[j])

    small = [pltpu.make_async_copy(lse_ref, sum_ref, sems.at[n_piece]),
             pltpu.make_async_copy(next_ref, row_ref, sems.at[n_piece + 1])]
    for copy in small:
        copy.start()
    for j in range(n_piece):
        buf[edges[j]:edges[j + 1], :] = z_ref[edges[j]:edges[j + 1], :] - lse
        put(j).start()
    for copy in small:
        copy.wait()
    for j in range(n_piece):
        put(j).wait()


def solution(mesh):
    n_vp, n_tp = mesh.shape["vp"], mesh.shape["tp"]

    def per_device(hidden, lnf_gain, lnf_bias, emb_table, next_tok, eln_gain, eln_bias):
        rows, width = hidden.shape
        n_block = emb_table.shape[0] // n_tp
        slab = rows // n_vp
        n_round = n_block // 2 // CHUNK + 1
        small = n_block - 2 * (n_round - 1) * CHUNK
        dma = pltpu.SemaphoreType.DMA
        vmem = pl.BlockSpec(memory_space=pltpu.VMEM)
        logits, lse, next_in = pl.pallas_call(
            functools.partial(head_kernel, n_vp, n_tp, n_block, width * n_tp),
            out_shape=(
                pltpu.VMEM((n_block, rows), F32),
                pltpu.VMEM((1, rows), F32),
                pltpu.VMEM((rows, width), BF16),
            ),
            in_specs=[pl.BlockSpec(memory_space=pl.ANY)] * 7,
            out_specs=(vmem, vmem, vmem),
            scratch_shapes=[
                *[pltpu.VMEM((4, n_block, width), BF16)] * 2,
                *[pltpu.VMEM((4, n_block, width), F32)] * 2,
                *[pltpu.VMEM((n_block, rows), F32)] * 5,
                pltpu.VMEM((2, width, rows + 256), F32),
                pltpu.VMEM((2, width, rows), BF16),
                pltpu.VMEM((8, rows), F32),
                pltpu.VMEM((8, rows), F32),
                pltpu.VMEM((rows, width), F32),
                pltpu.VMEM((n_tp, 1, 2 * rows), F32),
                pltpu.VMEM((n_tp, rows // LANE, LANE), F32),
                pltpu.VMEM((2 * n_vp, rows // LANE, LANE), F32),
                pltpu.VMEM((n_vp, slab, width), F32),
                pltpu.VMEM((n_tp, 1, 256), F32),
                pltpu.VMEM((n_vp, slab, width), F32),
                pltpu.VMEM((n_vp * n_tp, rows // LANE, LANE), F32),
                pltpu.VMEM((small, width), F32),
                pltpu.VMEM((2, small - small // 16 * 8, width), F32),
                pltpu.VMEM((2, small // 16 * 8, width), F32),
                pltpu.VMEM((width // (n_vp // 2), rows), F32),
                pltpu.VMEM((2, width, rows), F32),
                pltpu.VMEM((2, width, rows), F32),
                pltpu.VMEM((2, 2, width, rows), BF16),
                dma((7,)), dma, dma((5,)), dma, dma,
                dma, dma((n_round,)), dma, dma, dma((n_round,)),
                dma, dma((4,)), dma, dma((4,)), dma, dma((2,)), dma((2,)), dma, dma,
                pltpu.SemaphoreType.REGULAR((N_HOP + 1,)),
                pltpu.VMEM((rows, width), BF16),
                pltpu.VMEM((1, rows), jnp.int32),
                pltpu.VMEM((4, 1, width), F32),
                dma((3,)),
            ],
            compiler_params=pltpu.CompilerParams(
                collective_id=0, has_side_effects=True, vmem_limit_bytes=57 * 1024 * 1024),
            cost_estimate=pl.CostEstimate(
                flops=4 * rows * n_block * n_tp * width, bytes_accessed=16 * n_block * n_tp * width, transcendentals=rows * n_block),
        )(hidden, lnf_gain[None, :], lnf_bias[None, :], emb_table, next_tok[None, :], eln_gain[None, :], eln_bias[None, :])
        n_piece = 7
        logprobs_t, log_sum, next_bf = pl.pallas_call(
            functools.partial(finish_kernel, n_piece),
            out_shape=(
                jax.ShapeDtypeStruct((n_block, rows), F32),
                jax.ShapeDtypeStruct((1, rows), F32),
                jax.ShapeDtypeStruct((rows, width), BF16),
            ),
            in_specs=[vmem, vmem, vmem],
            out_specs=(pl.BlockSpec(memory_space=pl.ANY),) * 3,
            scratch_shapes=[pltpu.VMEM((n_block, rows), F32), dma((n_piece + 2,))],
            compiler_params=pltpu.CompilerParams(vmem_limit_bytes=16 * 1024 * 1024),
        )(logits, lse, next_in)
        return logprobs_t.T, log_sum[0], next_bf

    return jax.shard_map(
        per_device,
        mesh=mesh,
        in_specs=(P("dp", "tp"), P("tp"), P("tp"), P("vp", "tp"), P("dp"), P("tp"), P("tp")),
        out_specs=(P("dp", ("vp", "tp")), P("dp"), P("dp", "tp")),
        check_vma=False,
    )
```
